32 devices in a mesh: dp: 4 (over x, core), fsdp: 8 (over z, y).
Axes of the slice: x: 2, y: 2, z: 4, core: 2. Of those that a mesh axis runs over, the one named last changes fastest.
Arguments:
- inputs: bfloat16 [2, 4, 16, 192, 768], P(None, 'dp', 'fsdp'), may hold values from -6 to 6
- space_in: bfloat16 [768, 2304], P('fsdp'), may hold values from -0.21875 to 0.21875
- space_out: bfloat16 [768, 768], P('fsdp'), may hold values from -1.5 to 1.5
- time_in: bfloat16 [768, 2304], P('fsdp'), may hold values from -0.21875 to 0.21875
- time_out: bfloat16 [768, 768], P('fsdp'), may hold values from -0.4375 to 0.4375
- hidden_in: bfloat16 [768, 3072], P('fsdp'), may hold values from -0.21875 to 0.21875
- hidden_out: bfloat16 [3072, 768], P('fsdp'), may hold values from -0.109375 to 0.109375
- norm_gains: bfloat16 [3, 768], P(None, 'fsdp'), may hold values from 0.5 to 1.5
- cotangent: bfloat16 [2, 4, 16, 192, 768], P(None, 'dp', 'fsdp'), may hold values from -6 to 6
Outputs:
- result: float32 [2, 4, 16, 192, 768], P(None, 'dp', 'fsdp')
- input_grad: float32 [2, 4, 16, 192, 768], P(None, 'dp', 'fsdp')
- grad_space_in: float32 [768, 2304], P('fsdp')
- grad_space_out: float32 [768, 768], P('fsdp')
- grad_time_in: float32 [768, 2304], P('fsdp')
- grad_time_out: float32 [768, 768], P('fsdp')
- grad_hidden_in: float32 [768, 3072], P('fsdp')
- grad_hidden_out: float32 [3072, 768], P('fsdp')
- grad_norm_gains: float32 [3, 768], P(None, 'fsdp')
The draws below stay inside these ranges and needn't reach their ends.
All inputs are finite; a program needn't handle non-finite values.
Results may differ from the reference program's by a relative error of at most 0.025.
Values may be sent and summed in bfloat16 or wider, within the bound.
A program may use at most 192 MiB of HBM per device.

```python
import jax
import jax.numpy as jnp
from jax import lax

D = 768
HEADS = 12
HEAD_DIM = 64
FF = 3072
FRAMES = 16
PLACES = 192
MICRO = 2
CLIPS = 4


def level_of(own_key, extent, pieces, low, largest):
    def one(dim, blocks):
        heights = jax.random.uniform(jax.random.fold_in(jax.random.fold_in(own_key, 6), dim), (blocks,), jnp.float32, low / len(pieces), largest / len(pieces))
        return jnp.repeat(jnp.exp(heights), extent[dim] // blocks).reshape((-1,) + (1,) * (len(extent) - dim - 1))

    loudness = one(*pieces[0])
    for cut in pieces[1:]:
        loudness = loudness * one(*cut)
    return loudness


def normal_values(key, shape, scale, reach, shards=(), held_as=jnp.bfloat16):
    entries = scale * jax.random.normal(key, shape, jnp.float32)
    if shards:
        entries = entries * level_of(key, shape, shards, -0.22, 0.18)
    return jnp.clip(entries, -reach, reach).astype(held_as)


def setup_inputs(seed: int = 0) -> dict:
    arg_keys = jax.random.split(jax.random.key(seed), 10)
    inputs = normal_values(arg_keys[0], (MICRO, CLIPS, FRAMES, PLACES, D), 1.0, 6.0, ((1, 4), (2, 8)))
    space_in = normal_values(arg_keys[1], (D, 3 * D), D ** -0.5, 0.21875, ((0, 8),))
    space_out = normal_values(arg_keys[2], (D, D), (max(D * 4 // PLACES, 1)) ** -0.5, 1.5, ((0, 8),))
    time_in = normal_values(arg_keys[3], (D, 3 * D), D ** -0.5, 0.21875, ((0, 8),))
    time_out = normal_values(arg_keys[4], (D, D), (max(D * 4 // FRAMES, 1)) ** -0.5, 0.4375, ((0, 8),))
    hidden_in = normal_values(arg_keys[5], (D, FF), D ** -0.5, 0.21875, ((0, 8),))
    hidden_out = normal_values(arg_keys[6], (FF, D), FF ** -0.5, 0.109375, ((0, 8),))
    norm_gains = jnp.clip(1.0 + 0.1 * jax.random.normal(arg_keys[7], (3, D), jnp.float32), 0.5, 1.5).astype(jnp.bfloat16)
    cotangent = normal_values(arg_keys[8], (MICRO, CLIPS, FRAMES, PLACES, D), 1.0, 6.0, ((1, 4), (2, 8)))
    return {"inputs": inputs, "space_in": space_in, "space_out": space_out, "time_in": time_in, "time_out": time_out, "hidden_in": hidden_in, "hidden_out": hidden_out, "norm_gains": norm_gains, "cotangent": cotangent}


EPS = 1e-06

@jax.custom_vjp
def low(v):
    return lax.optimization_barrier(v.astype(jnp.bfloat16)).astype(jnp.float32)

@jax.custom_vjp
def low_back(v):
    return v

def low_keep(v):
    return (low(v), None)

def low_pass(kept, grad):
    return (grad,)

def back_keep(v):
    return (v, None)

def back_low(kept, grad):
    return (low(grad),)
low.defvjp(low_keep, low_pass)
low_back.defvjp(back_keep, back_low)

def matmul(left, right):
    return jnp.matmul(left, right, precision=lax.Precision.HIGHEST)

def layer_norm(values, scales):
    average = lax.optimization_barrier(jnp.mean(values, axis=-1, keepdims=True))
    centred = values - average
    spread = lax.optimization_barrier(jnp.mean(centred * centred, axis=-1, keepdims=True))
    return centred * lax.rsqrt(spread + EPS) * scales

def attention(normed, weight_in, weight_out):
    leading = normed.shape[:2]
    joined = low_back(low(matmul(normed, weight_in)))
    split_heads = joined.reshape(leading + (3, HEADS, HEAD_DIM))
    queries = split_heads[:, :, 0]
    keyset = split_heads[:, :, 1]
    valueset = split_heads[:, :, 2]
    scores = jnp.einsum('glhd,gmhd->ghlm', queries, keyset, precision=lax.Precision.HIGHEST)
    scores = low_back(scores * HEAD_DIM ** (-0.5))
    weighting = low_back(low(jax.nn.softmax(scores, axis=-1)))
    context = jnp.einsum('ghlm,gmhd->glhd', weighting, valueset, precision=lax.Precision.HIGHEST)
    context = low_back(low(context.reshape(leading + (D,))))
    return low_back(matmul(context, weight_out))

def clip_forward(one_clip, weights):
    space_in, space_out, time_in, time_out, hidden_in, hidden_out, norm_gains = weights
    normed_one = low_back(low(layer_norm(one_clip, norm_gains[0])))
    mixed_one = one_clip + attention(normed_one, space_in, space_out)
    normed_two = low_back(low(layer_norm(mixed_one, norm_gains[1])))
    across = attention(jnp.swapaxes(normed_two, 0, 1), time_in, time_out)
    mixed_two = mixed_one + jnp.swapaxes(across, 0, 1)
    normed_three = low_back(low(layer_norm(mixed_two, norm_gains[2])))
    hidden = low_back(matmul(normed_three, hidden_in))
    activated = low_back(low(jax.nn.gelu(hidden, approximate=False)))
    return mixed_two + low_back(matmul(activated, hidden_out))

def reference(inputs, space_in, space_out, time_in, time_out, hidden_in, hidden_out, norm_gains, cotangent):
    weights = tuple((item.astype(jnp.float32) for item in (space_in, space_out, time_in, time_out, hidden_in, hidden_out, norm_gains)))
    clip_count = MICRO * CLIPS
    clips = inputs.astype(jnp.float32).reshape(clip_count, FRAMES, PLACES, D)
    cotangents = cotangent.astype(jnp.float32).reshape(clip_count, FRAMES, PLACES, D)
    single = jax.checkpoint(clip_forward)

    def forward(clip_stack, params):
        return lax.map(lambda one_clip: single(one_clip, params), clip_stack)
    outputs, pullback = jax.vjp(forward, clips, weights)
    grad_clips, grad_weights = pullback(cotangents)
    full_shape = inputs.shape
    return (outputs.reshape(full_shape), grad_clips.reshape(full_shape), grad_weights[0], grad_weights[1], grad_weights[2], grad_weights[3], grad_weights[4], grad_weights[5], grad_weights[6])
```

```python
from functools import partial

import jax
import jax.numpy as jnp
from jax import lax
from jax.sharding import Mesh
from jax.sharding import PartitionSpec as P

D = 768
HEADS = 12
HEAD_DIM = 64
GAIN_COLS = 128

EPS = 1e-06

MEMBERS = ("fsdp", "core")


def layer_norm(values, scales):
    average = jnp.mean(values, axis=-1, keepdims=True)
    centred = values - average
    spread = jnp.mean(centred * centred, axis=-1, keepdims=True)
    return centred * lax.rsqrt(spread + EPS) * scales


def norm_back(values, scales, incoming):
    unused, pullback = jax.vjp(layer_norm, values, scales)
    return pullback(incoming)


def flat_dot(left, right):
    flat = left.reshape(-1, left.shape[-1])
    product = jnp.dot(flat, right, preferred_element_type=jnp.float32)
    return product.reshape(left.shape[:-1] + (right.shape[1],))


def back_dot(left, right):
    flat = left.reshape(-1, left.shape[-1])
    product = lax.dot_general(
        flat, right, (((1,), (1,)), ((), ())), preferred_element_type=jnp.float32
    )
    return product.reshape(left.shape[:-1] + (right.shape[0],))


def token_sum(left, right):
    left_rows = left.reshape(-1, left.shape[-1])
    right_rows = right.reshape(-1, right.shape[-1])
    return lax.dot_general(
        left_rows, right_rows, (((0,), (0,)), ((), ())), preferred_element_type=jnp.float32
    )


def split_join(joined):
    split_heads = joined.reshape(joined.shape[:-1] + (3, HEADS, HEAD_DIM))
    return (split_heads[..., 0, :, :], split_heads[..., 1, :, :], split_heads[..., 2, :, :])


def attend_core(normed, weight_in, token_form, key_form, score_form):
    joined = flat_dot(normed, weight_in).astype(jnp.bfloat16)
    queries, keyset, valueset = split_join(joined)
    factor = HEAD_DIM ** (-0.5)
    scores = (
        jnp.einsum(
            token_form + "hd," + key_form + "hd->" + score_form,
            queries,
            keyset,
            preferred_element_type=jnp.float32,
        )
        * factor
    )
    totals = jax.nn.logsumexp(scores, axis=-1, keepdims=True)
    weighting = jnp.exp(scores - totals).astype(jnp.bfloat16)
    context = jnp.einsum(
        score_form + "," + key_form + "hd->" + token_form + "hd",
        weighting,
        valueset,
        preferred_element_type=jnp.float32,
    )
    context = context.reshape(normed.shape[:-1] + (D,)).astype(jnp.bfloat16)
    return (joined, totals, context)


def attend_back(joined, totals, back_context, token_form, key_form, score_form):
    queries, keyset, valueset = split_join(joined)
    back_heads = back_context.reshape(back_context.shape[:-1] + (HEADS, HEAD_DIM))
    factor = HEAD_DIM ** (-0.5)
    scores = (
        jnp.einsum(
            token_form + "hd," + key_form + "hd->" + score_form,
            queries,
            keyset,
            preferred_element_type=jnp.float32,
        )
        * factor
    )
    weighting = jnp.exp(scores - totals)
    back_weight = jnp.einsum(
        token_form + "hd," + key_form + "hd->" + score_form,
        back_heads,
        valueset,
        preferred_element_type=jnp.float32,
    )
    back_weight = back_weight.astype(jnp.bfloat16).astype(jnp.float32)
    inner_sum = jnp.sum(weighting * back_weight, axis=-1, keepdims=True)
    back_scores = (weighting * (back_weight - inner_sum)).astype(jnp.bfloat16)
    back_query = (
        jnp.einsum(
            score_form + "," + key_form + "hd->" + token_form + "hd",
            back_scores,
            keyset,
            preferred_element_type=jnp.float32,
        )
        * factor
    )
    back_keys = (
        jnp.einsum(
            score_form + "," + token_form + "hd->" + key_form + "hd",
            back_scores,
            queries,
            preferred_element_type=jnp.float32,
        )
        * factor
    )
    back_values = jnp.einsum(
        score_form + "," + token_form + "hd->" + key_form + "hd",
        weighting.astype(jnp.bfloat16),
        back_heads,
        preferred_element_type=jnp.float32,
    )
    stacked = jnp.stack((back_query, back_keys, back_values), axis=-3)
    return stacked.reshape(back_context.shape[:-1] + (3 * D,)).astype(jnp.bfloat16)


def member_block(weights, gains, part, half):
    pieces = [lax.dynamic_slice_in_dim(w, part * half, half, axis=0) for w in weights[:5]]
    out_rows = lax.dynamic_slice_in_dim(weights[5], part * 4 * half, 4 * half, axis=0)
    pieces.append(jnp.concatenate([out_rows[q * half:(q + 1) * half] for q in range(4)], axis=1))
    gain_part = lax.dynamic_slice_in_dim(gains, part * half, half, axis=1).T
    pieces.append(jnp.pad(gain_part, ((0, 0), (0, GAIN_COLS - gain_part.shape[1]))))
    return jnp.concatenate(pieces, axis=1)


def unpack_rows(block, widths, half):
    members = block.shape[0] // half
    offsets = [0]
    for width in widths:
        offsets.append(offsets[-1] + width)
    outs = [block[:, offsets[i]:offsets[i + 1]] for i in range(5)]
    grouped = block[:, offsets[5]:offsets[6]].reshape(members, half, 4 * D)
    outs.append(
        jnp.concatenate([grouped[:, :, q * D:(q + 1) * D] for q in range(4)], axis=1).reshape(
            members * 4 * half, D
        )
    )
    outs.append(block[:, offsets[6]:offsets[6] + 3].T)
    return outs


def pack_grads(grads, gain_grads, members, half):
    pieces = [g.astype(jnp.bfloat16) for g in grads[:5]]
    grouped = grads[5].astype(jnp.bfloat16).reshape(members, 4 * half, D)
    pieces.append(
        jnp.concatenate([grouped[:, q * half:(q + 1) * half, :] for q in range(4)], axis=2).reshape(
            members * half, 4 * D
        )
    )
    gain_cols = gain_grads.T.astype(jnp.bfloat16)
    pieces.append(jnp.pad(gain_cols, ((0, 0), (0, GAIN_COLS - gain_cols.shape[1]))))
    return jnp.concatenate(pieces, axis=1)


def shards(
    inputs, space_in, space_out, time_in, time_out, hidden_in, hidden_out, norm_gains, cotangent
):
    weights = (space_in, space_out, time_in, time_out, hidden_in, hidden_out)
    widths = [w.shape[1] for w in weights[:5]] + [4 * D]
    fsdp_size = lax.axis_size("fsdp")
    core_size = lax.axis_size("core")
    members = fsdp_size * core_size
    half = space_in.shape[0] // core_size
    core = lax.axis_index("core")

    block = member_block(weights, norm_gains, core, half)
    gathered = lax.all_gather(block, MEMBERS, axis=0, tiled=True)
    s_in, s_out, t_in, t_out, h_in, h_out, gains = unpack_rows(gathered, widths, half)
    gain_rows = gains.astype(jnp.float32)

    micro, _, frames, places, _ = inputs.shape
    spatial = ("gl", "gm", "ghlm")
    temporal = ("blg", "bmg", "bghlm")

    frames_in = inputs[:, 0].astype(jnp.float32)
    normed_one = layer_norm(frames_in, gain_rows[0]).astype(jnp.bfloat16)
    join_space, total_space, context_space = attend_core(
        normed_one.reshape(micro * frames, places, D), s_in, *spatial
    )
    context_space = context_space.reshape(micro, frames, places, D)
    mixed_one = frames_in + flat_dot(context_space, s_out)
    normed_two = layer_norm(mixed_one, gain_rows[1]).astype(jnp.bfloat16)
    placed = lax.all_to_all(normed_two, "fsdp", split_axis=2, concat_axis=1, tiled=True)
    join_time, total_time, context_placed = attend_core(placed, t_in, *temporal)
    context_time = lax.all_to_all(context_placed, "fsdp", split_axis=1, concat_axis=2, tiled=True)
    mixed_two = mixed_one + flat_dot(context_time, t_out)
    normed_three = layer_norm(mixed_two, gain_rows[2]).astype(jnp.bfloat16)
    hidden = flat_dot(normed_three, h_in)
    activated = jax.nn.gelu(hidden, approximate=False).astype(jnp.bfloat16)
    result = mixed_two + flat_dot(activated, h_out)

    upstream = cotangent[:, 0].astype(jnp.float32)
    rounded = upstream.astype(jnp.bfloat16)
    grad_hidden_out = token_sum(activated, rounded)
    back_active = back_dot(rounded, h_out).astype(jnp.bfloat16)
    unused, gelu_pull = jax.vjp(partial(jax.nn.gelu, approximate=False), hidden)
    back_hidden = gelu_pull(back_active.astype(jnp.float32))[0].astype(jnp.bfloat16)
    grad_hidden_in = token_sum(normed_three, back_hidden)
    back_three = back_dot(back_hidden, h_in).astype(jnp.bfloat16)
    back_mixed, gain_grad_two = norm_back(mixed_two, gain_rows[2], back_three.astype(jnp.float32))
    upstream = upstream + back_mixed
    rounded = upstream.astype(jnp.bfloat16)
    grad_time_out = token_sum(context_time, rounded)
    back_context = back_dot(rounded, t_out).astype(jnp.bfloat16)
    back_placed = lax.all_to_all(back_context, "fsdp", split_axis=2, concat_axis=1, tiled=True)
    back_join = attend_back(join_time, total_time, back_placed, *temporal)
    grad_time_in = token_sum(placed, back_join)
    back_two_placed = back_dot(back_join, t_in).astype(jnp.bfloat16)
    back_two = lax.all_to_all(back_two_placed, "fsdp", split_axis=1, concat_axis=2, tiled=True)
    back_mixed, gain_grad_one = norm_back(mixed_one, gain_rows[1], back_two.astype(jnp.float32))
    upstream = upstream + back_mixed
    rounded = upstream.astype(jnp.bfloat16)
    grad_space_out = token_sum(context_space, rounded)
    back_context = back_dot(rounded, s_out).astype(jnp.bfloat16)
    back_join = attend_back(
        join_space, total_space, back_context.reshape(micro * frames, places, D), *spatial
    )
    grad_space_in = token_sum(normed_one, back_join)
    back_one = back_dot(back_join, s_in).astype(jnp.bfloat16).reshape(micro, frames, places, D)
    back_mixed, gain_grad_zero = norm_back(frames_in, gain_rows[0], back_one.astype(jnp.float32))
    input_grad = upstream + back_mixed

    grads = (grad_space_in, grad_space_out, grad_time_in, grad_time_out, grad_hidden_in, grad_hidden_out)
    gain_grads = jnp.stack((gain_grad_zero, gain_grad_one, gain_grad_two))
    packed = pack_grads(grads, gain_grads, members, half)
    owned = lax.psum_scatter(packed, MEMBERS, scatter_dimension=0, tiled=True)
    owned = lax.psum(owned, "dpo")
    owned = lax.all_gather(owned, "core", axis=0, tiled=True)
    outs = unpack_rows(owned, widths, half)
    outs = [part.astype(jnp.float32) for part in outs]
    return (result[:, None], input_grad[:, None], *outs)


def solution(mesh):
    dp_size, fsdp_size = mesh.devices.shape
    split = Mesh(mesh.devices.reshape(dp_size // 2, 2, fsdp_size), ("dpo", "core", "fsdp"))
    tokens = P(None, ("dpo", "core"), "fsdp", None, None)
    rows = P("fsdp", None)
    return jax.shard_map(
        shards,
        mesh=split,
        in_specs=(tokens, rows, rows, rows, rows, rows, rows, P(None, "fsdp"), tokens),
        out_specs=(tokens, tokens, rows, rows, rows, rows, rows, rows, P(None, "fsdp")),
        check_vma=False,
    )
```

```python
from functools import partial

import jax
import jax.numpy as jnp
from jax import lax
from jax.sharding import Mesh
from jax.sharding import PartitionSpec as P


D = 768
HEADS = 12
HEAD_DIM = 64
GAIN_COLS = 128

EPS = 1e-06

MEMBERS = ("fsdp", "core")


def layer_norm(values, scales):
    average = jnp.mean(values, axis=-1, keepdims=True)
    centred = values - average
    spread = jnp.mean(centred * centred, axis=-1, keepdims=True)
    return centred * lax.rsqrt(spread + EPS) * scales


def norm_back(values, scales, incoming):
    _, pullback = jax.vjp(layer_norm, values, scales)
    return pullback(incoming)


def flat_dot(left, right):
    flat = left.reshape(-1, left.shape[-1])
    product = jnp.dot(flat, right, preferred_element_type=jnp.float32)
    return product.reshape(left.shape[:-1] + (right.shape[1],))


def back_dot(left, right):
    flat = left.reshape(-1, left.shape[-1])
    product = lax.dot_general(
        flat, right, (((1,), (1,)), ((), ())), preferred_element_type=jnp.float32
    )
    return product.reshape(left.shape[:-1] + (right.shape[0],))


def token_sum(left, right):
    left_rows = left.reshape(-1, left.shape[-1])
    right_rows = right.reshape(-1, right.shape[-1])
    return lax.dot_general(
        left_rows, right_rows, (((0,), (0,)), ((), ())), preferred_element_type=jnp.float32
    )


def split_join(joined):
    split_heads = joined.reshape(joined.shape[:-1] + (3, HEADS, HEAD_DIM))
    return (split_heads[..., 0, :, :], split_heads[..., 1, :, :], split_heads[..., 2, :, :])


def attend_core(normed, weight_in, token_form, key_form, score_form):
    joined = flat_dot(normed, weight_in).astype(jnp.bfloat16)
    queries, keyset, valueset = split_join(joined)
    factor = HEAD_DIM ** (-0.5)
    scores = (
        jnp.einsum(
            token_form + "hd," + key_form + "hd->" + score_form,
            queries,
            keyset,
            preferred_element_type=jnp.float32,
        )
        * factor
    )
    totals = jax.nn.logsumexp(scores, axis=-1, keepdims=True)
    weighting = jnp.exp(scores - totals).astype(jnp.bfloat16)
    context = jnp.einsum(
        score_form + "," + key_form + "hd->" + token_form + "hd",
        weighting,
        valueset,
        preferred_element_type=jnp.float32,
    )
    context = context.reshape(normed.shape[:-1] + (D,)).astype(jnp.bfloat16)
    return (joined, totals, context)


def attend_back(joined, totals, back_context, token_form, key_form, score_form):
    queries, keyset, valueset = split_join(joined)
    back_heads = back_context.reshape(back_context.shape[:-1] + (HEADS, HEAD_DIM))
    factor = HEAD_DIM ** (-0.5)
    scores = (
        jnp.einsum(
            token_form + "hd," + key_form + "hd->" + score_form,
            queries,
            keyset,
            preferred_element_type=jnp.float32,
        )
        * factor
    )
    weighting = jnp.exp(scores - totals)
    back_weight = jnp.einsum(
        token_form + "hd," + key_form + "hd->" + score_form,
        back_heads,
        valueset,
        preferred_element_type=jnp.float32,
    )
    back_weight = back_weight.astype(jnp.bfloat16).astype(jnp.float32)
    inner_sum = jnp.sum(weighting * back_weight, axis=-1, keepdims=True)
    back_scores = (weighting * (back_weight - inner_sum)).astype(jnp.bfloat16)
    back_query = (
        jnp.einsum(
            score_form + "," + key_form + "hd->" + token_form + "hd",
            back_scores,
            keyset,
            preferred_element_type=jnp.float32,
        )
        * factor
    )
    back_keys = (
        jnp.einsum(
            score_form + "," + token_form + "hd->" + key_form + "hd",
            back_scores,
            queries,
            preferred_element_type=jnp.float32,
        )
        * factor
    )
    back_values = jnp.einsum(
        score_form + "," + token_form + "hd->" + key_form + "hd",
        weighting.astype(jnp.bfloat16),
        back_heads,
        preferred_element_type=jnp.float32,
    )
    stacked = jnp.stack((back_query, back_keys, back_values), axis=-3)
    return stacked.reshape(back_context.shape[:-1] + (3 * D,)).astype(jnp.bfloat16)


def to_member(array, kind, part, half):
    if kind == "gains":
        gain_part = lax.dynamic_slice_in_dim(array, part * half, half, axis=1).T
        return jnp.pad(gain_part, ((0, 0), (0, GAIN_COLS - gain_part.shape[1])))
    if kind == "grouped":
        rows = lax.dynamic_slice_in_dim(array, part * 4 * half, 4 * half, axis=0)
        return jnp.concatenate([rows[q * half:(q + 1) * half] for q in range(4)], axis=1)
    return lax.dynamic_slice_in_dim(array, part * half, half, axis=0)


def width_of(array, kind):
    return {"gains": GAIN_COLS, "grouped": 4 * D}.get(kind, array.shape[-1])


def from_members(block, kinds, widths, half):
    members = block.shape[0] // half
    outs = []
    offset = 0
    for kind, width in zip(kinds, widths):
        part = block[:, offset:offset + width]
        offset += width
        if kind == "gains":
            outs.append(part[:, :3].T)
        elif kind == "grouped":
            grouped = part.reshape(members, half, 4 * D)
            outs.append(
                jnp.concatenate([grouped[:, :, q * D:(q + 1) * D] for q in range(4)], axis=1).reshape(
                    members * 4 * half, D
                )
            )
        else:
            outs.append(part)
    return outs


def to_members_full(array, kind, members, half):
    array = array.astype(jnp.bfloat16)
    if kind == "gains":
        cols = array.T
        return jnp.pad(cols, ((0, 0), (0, GAIN_COLS - cols.shape[1])))
    if kind == "grouped":
        grouped = array.reshape(members, 4 * half, D)
        return jnp.concatenate(
            [grouped[:, q * half:(q + 1) * half, :] for q in range(4)], axis=2
        ).reshape(members * half, 4 * D)
    return array


def gather_group(arrays, kinds, part, half):
    block = jnp.concatenate([to_member(a, k, part, half) for a, k in zip(arrays, kinds)], axis=1)
    widths = [width_of(a, k) for a, k in zip(arrays, kinds)]
    gathered = lax.all_gather(block, MEMBERS, axis=0, tiled=True)
    return from_members(gathered, kinds, widths, half)


def pair_sum(values, axis):
    if lax.axis_size(axis) == 2:
        return values + lax.ppermute(values, axis, [(0, 1), (1, 0)])
    return lax.psum(values, axis)


def core_gather(values):
    if lax.axis_size("core") == 2:
        other = lax.ppermute(values, "core", [(0, 1), (1, 0)])
        first = lax.axis_index("core") == 0
        return jnp.concatenate(
            [jnp.where(first, values, other), jnp.where(first, other, values)], axis=0
        )
    return lax.all_gather(values, "core", axis=0, tiled=True)


def pack_group(grads, kinds, members, half):
    return jnp.concatenate(
        [to_members_full(g, k, members, half) for g, k in zip(grads, kinds)], axis=1
    )


def reduce_group(packed, grads, kinds, half):
    widths = [width_of(g, k) for g, k in zip(grads, kinds)]
    owned = lax.psum_scatter(packed, MEMBERS, scatter_dimension=0, tiled=True)
    owned = core_gather(pair_sum(owned, "dpo"))
    return [part.astype(jnp.float32) for part in from_members(owned, kinds, widths, half)]


def layer(
    inputs, space_in, space_out, time_in, time_out, hidden_in, hidden_out, norm_gains, cotangent
):
    fsdp_size = lax.axis_size("fsdp")
    core_size = lax.axis_size("core")
    members = fsdp_size * core_size
    half = space_in.shape[0] // core_size
    core = lax.axis_index("core")

    s_in, s_out, gains = gather_group(
        (space_in, space_out, norm_gains), ("plain", "plain", "gains"), core, half
    )
    t_in, t_out, h_in, h_out = gather_group(
        (time_in, time_out, hidden_in, hidden_out),
        ("plain", "plain", "plain", "grouped"),
        core,
        half,
    )
    gain_rows = gains.astype(jnp.float32)

    micro, _, frames, places, _ = inputs.shape
    spatial = ("gl", "gm", "ghlm")
    temporal = ("blg", "bmg", "bghlm")

    frames_in = inputs[:, 0].astype(jnp.float32)
    normed_one = layer_norm(frames_in, gain_rows[0]).astype(jnp.bfloat16)
    join_space, total_space, context_space = attend_core(
        normed_one.reshape(micro * frames, places, D), s_in, *spatial
    )
    context_space = context_space.reshape(micro, frames, places, D)
    mixed_one = frames_in + flat_dot(context_space, s_out)
    normed_two = layer_norm(mixed_one, gain_rows[1]).astype(jnp.bfloat16)
    placed = lax.all_to_all(normed_two, "fsdp", split_axis=2, concat_axis=1, tiled=True)
    join_time, total_time, context_placed = attend_core(placed, t_in, *temporal)
    context_time = lax.all_to_all(context_placed, "fsdp", split_axis=1, concat_axis=2, tiled=True)
    mixed_two = mixed_one + flat_dot(context_time, t_out)
    normed_three = layer_norm(mixed_two, gain_rows[2]).astype(jnp.bfloat16)
    hidden = flat_dot(normed_three, h_in)
    activated = jax.nn.gelu(hidden, approximate=False).astype(jnp.bfloat16)
    result = mixed_two + flat_dot(activated, h_out)

    upstream = cotangent[:, 0].astype(jnp.float32)
    rounded = upstream.astype(jnp.bfloat16)
    grad_hidden_out = token_sum(activated, rounded)
    back_active = back_dot(rounded, h_out).astype(jnp.bfloat16)
    _, gelu_pull = jax.vjp(partial(jax.nn.gelu, approximate=False), hidden)
    back_hidden = gelu_pull(back_active.astype(jnp.float32))[0].astype(jnp.bfloat16)
    grad_hidden_in = token_sum(normed_three, back_hidden)
    back_three = back_dot(back_hidden, h_in).astype(jnp.bfloat16)
    ffn_grads = (grad_hidden_in, grad_hidden_out)
    ffn_kinds = ("plain", "grouped")
    packed_ffn, back_three = lax.optimization_barrier(
        (pack_group(ffn_grads, ffn_kinds, members, half), back_three)
    )
    grad_ffn = reduce_group(packed_ffn, ffn_grads, ffn_kinds, half)
    back_mixed, gain_grad_two = norm_back(mixed_two, gain_rows[2], back_three.astype(jnp.float32))
    upstream = upstream + back_mixed
    rounded = upstream.astype(jnp.bfloat16)
    grad_time_out = token_sum(context_time, rounded)
    back_context = back_dot(rounded, t_out).astype(jnp.bfloat16)
    back_placed = lax.all_to_all(back_context, "fsdp", split_axis=2, concat_axis=1, tiled=True)
    back_join = attend_back(join_time, total_time, back_placed, *temporal)
    grad_time_in = token_sum(placed, back_join)
    back_two_placed = back_dot(back_join, t_in).astype(jnp.bfloat16)
    time_grads = (grad_time_in, grad_time_out)
    time_kinds = ("plain", "plain")
    packed_time, back_two_placed = lax.optimization_barrier(
        (pack_group(time_grads, time_kinds, members, half), back_two_placed)
    )
    grad_time = reduce_group(packed_time, time_grads, time_kinds, half)
    back_two = lax.all_to_all(back_two_placed, "fsdp", split_axis=1, concat_axis=2, tiled=True)
    back_mixed, gain_grad_one = norm_back(mixed_one, gain_rows[1], back_two.astype(jnp.float32))
    upstream = upstream + back_mixed
    rounded = upstream.astype(jnp.bfloat16)
    grad_space_out = token_sum(context_space, rounded)
    back_context = back_dot(rounded, s_out).astype(jnp.bfloat16)
    back_join = attend_back(
        join_space, total_space, back_context.reshape(micro * frames, places, D), *spatial
    )
    grad_space_in = token_sum(normed_one, back_join)
    back_one = back_dot(back_join, s_in).astype(jnp.bfloat16).reshape(micro, frames, places, D)
    back_mixed, gain_grad_zero = norm_back(frames_in, gain_rows[0], back_one.astype(jnp.float32))
    input_grad = upstream + back_mixed

    gain_grads = jnp.stack((gain_grad_zero, gain_grad_one, gain_grad_two))
    space_grads = (grad_space_in, grad_space_out, gain_grads)
    space_kinds = ("plain", "plain", "gains")
    grad_space = reduce_group(
        pack_group(space_grads, space_kinds, members, half), space_grads, space_kinds, half
    )
    return (
        result[:, None],
        input_grad[:, None],
        grad_space[0],
        grad_space[1],
        grad_time[0],
        grad_time[1],
        grad_ffn[0],
        grad_ffn[1],
        grad_space[2],
    )


def solution(mesh):
    dp_size, fsdp_size = mesh.devices.shape
    split = Mesh(mesh.devices.reshape(dp_size // 2, 2, fsdp_size), ("dpo", "core", "fsdp"))
    tokens = P(None, ("dpo", "core"), "fsdp", None, None)
    rows = P("fsdp", None)
    return jax.shard_map(
        layer,
        mesh=split,
        in_specs=(tokens, rows, rows, rows, rows, rows, rows, P(None, "fsdp"), tokens),
        out_specs=(tokens, tokens, rows, rows, rows, rows, rows, rows, P(None, "fsdp")),
        check_vma=False,
    )
```

```python
from functools import partial

import jax
import jax.numpy as jnp
from jax import lax
from jax.sharding import Mesh
from jax.sharding import PartitionSpec as P


D = 768
HEADS = 12
HEAD_DIM = 64
GAIN_COLS = 128

EPS = 1e-06

MEMBERS = ("fsdp", "core")


def layer_norm(values, scales):
    average = jnp.mean(values, axis=-1, keepdims=True)
    centred = values - average
    spread = jnp.mean(centred * centred, axis=-1, keepdims=True)
    return centred * lax.rsqrt(spread + EPS) * scales


def norm_back(values, scales, incoming):
    _, pullback = jax.vjp(layer_norm, values, scales)
    return pullback(incoming)


def flat_dot(left, right):
    flat = left.reshape(-1, left.shape[-1])
    product = jnp.dot(flat, right, preferred_element_type=jnp.float32)
    return product.reshape(left.shape[:-1] + (right.shape[1],))


def back_dot(left, right):
    flat = left.reshape(-1, left.shape[-1])
    product = lax.dot_general(
        flat, right, (((1,), (1,)), ((), ())), preferred_element_type=jnp.float32
    )
    return product.reshape(left.shape[:-1] + (right.shape[0],))


def token_sum(left, right):
    left_rows = left.reshape(-1, left.shape[-1])
    right_rows = right.reshape(-1, right.shape[-1])
    return lax.dot_general(
        left_rows, right_rows, (((0,), (0,)), ((), ())), preferred_element_type=jnp.float32
    )


def split_join(joined):
    split_heads = joined.reshape(joined.shape[:-1] + (3, HEADS, HEAD_DIM))
    return (split_heads[..., 0, :, :], split_heads[..., 1, :, :], split_heads[..., 2, :, :])


def attend_core(normed, weight_in, token_form, key_form, score_form):
    joined = flat_dot(normed, weight_in).astype(jnp.bfloat16)
    queries, keyset, valueset = split_join(joined)
    factor = HEAD_DIM ** (-0.5)
    scores = (
        jnp.einsum(
            token_form + "hd," + key_form + "hd->" + score_form,
            queries,
            keyset,
            preferred_element_type=jnp.float32,
        )
        * factor
    )
    totals = jax.nn.logsumexp(scores, axis=-1, keepdims=True)
    weighting = jnp.exp(scores - totals).astype(jnp.bfloat16)
    context = jnp.einsum(
        score_form + "," + key_form + "hd->" + token_form + "hd",
        weighting,
        valueset,
        preferred_element_type=jnp.float32,
    )
    context = context.reshape(normed.shape[:-1] + (D,)).astype(jnp.bfloat16)
    return (joined, totals, context)


def attend_back(joined, totals, back_context, token_form, key_form, score_form):
    queries, keyset, valueset = split_join(joined)
    back_heads = back_context.reshape(back_context.shape[:-1] + (HEADS, HEAD_DIM))
    factor = HEAD_DIM ** (-0.5)
    scores = (
        jnp.einsum(
            token_form + "hd," + key_form + "hd->" + score_form,
            queries,
            keyset,
            preferred_element_type=jnp.float32,
        )
        * factor
    )
    weighting = jnp.exp(scores - totals)
    back_weight = jnp.einsum(
        token_form + "hd," + key_form + "hd->" + score_form,
        back_heads,
        valueset,
        preferred_element_type=jnp.float32,
    )
    back_weight = back_weight.astype(jnp.bfloat16).astype(jnp.float32)
    inner_sum = jnp.sum(weighting * back_weight, axis=-1, keepdims=True)
    back_scores = (weighting * (back_weight - inner_sum)).astype(jnp.bfloat16)
    back_query = (
        jnp.einsum(
            score_form + "," + key_form + "hd->" + token_form + "hd",
            back_scores,
            keyset,
            preferred_element_type=jnp.float32,
        )
        * factor
    )
    back_keys = (
        jnp.einsum(
            score_form + "," + token_form + "hd->" + key_form + "hd",
            back_scores,
            queries,
            preferred_element_type=jnp.float32,
        )
        * factor
    )
    back_values = jnp.einsum(
        score_form + "," + token_form + "hd->" + key_form + "hd",
        weighting.astype(jnp.bfloat16),
        back_heads,
        preferred_element_type=jnp.float32,
    )
    stacked = jnp.stack((back_query, back_keys, back_values), axis=-3)
    return stacked.reshape(back_context.shape[:-1] + (3 * D,)).astype(jnp.bfloat16)


def to_member(array, kind, part, half):
    if kind == "gains":
        gain_part = lax.dynamic_slice_in_dim(array, part * half, half, axis=1).T
        return jnp.pad(gain_part, ((0, 0), (0, GAIN_COLS - gain_part.shape[1])))
    if kind == "grouped":
        rows = lax.dynamic_slice_in_dim(array, part * 4 * half, 4 * half, axis=0)
        return jnp.concatenate([rows[q * half:(q + 1) * half] for q in range(4)], axis=1)
    return lax.dynamic_slice_in_dim(array, part * half, half, axis=0)


def width_of(array, kind):
    return {"gains": GAIN_COLS, "grouped": 4 * D}.get(kind, array.shape[-1])


def from_members(block, kinds, widths, half):
    members = block.shape[0] // half
    outs = []
    offset = 0
    for kind, width in zip(kinds, widths):
        part = block[:, offset:offset + width]
        offset += width
        if kind == "gains":
            outs.append(part[:, :3].T)
        elif kind == "grouped":
            grouped = part.reshape(members, half, 4 * D)
            outs.append(
                jnp.concatenate([grouped[:, :, q * D:(q + 1) * D] for q in range(4)], axis=1).reshape(
                    members * 4 * half, D
                )
            )
        else:
            outs.append(part)
    return outs


def to_members_full(array, kind, members, half):
    array = array.astype(jnp.bfloat16)
    if kind == "gains":
        cols = array.T
        return jnp.pad(cols, ((0, 0), (0, GAIN_COLS - cols.shape[1])))
    if kind == "grouped":
        grouped = array.reshape(members, 4 * half, D)
        return jnp.concatenate(
            [grouped[:, q * half:(q + 1) * half, :] for q in range(4)], axis=2
        ).reshape(members * half, 4 * D)
    return array


def gather_group(arrays, kinds, part, half):
    block = jnp.concatenate([to_member(a, k, part, half) for a, k in zip(arrays, kinds)], axis=1)
    widths = [width_of(a, k) for a, k in zip(arrays, kinds)]
    gathered = lax.all_gather(block, MEMBERS, axis=0, tiled=True)
    return from_members(gathered, kinds, widths, half)


def pair_sum(values, axis):
    if lax.axis_size(axis) == 2:
        return values + lax.ppermute(values, axis, [(0, 1), (1, 0)])
    return lax.psum(values, axis)


def core_gather(values):
    if lax.axis_size("core") == 2:
        other = lax.ppermute(values, "core", [(0, 1), (1, 0)])
        first = lax.axis_index("core") == 0
        return jnp.concatenate(
            [jnp.where(first, values, other), jnp.where(first, other, values)], axis=0
        )
    return lax.all_gather(values, "core", axis=0, tiled=True)


def pack_group(grads, kinds, members, half):
    return jnp.concatenate(
        [to_members_full(g, k, members, half) for g, k in zip(grads, kinds)], axis=1
    )


def reduce_group(packed, grads, kinds, half):
    widths = [width_of(g, k) for g, k in zip(grads, kinds)]
    owned = lax.psum_scatter(packed, MEMBERS, scatter_dimension=0, tiled=True)
    owned = core_gather(pair_sum(owned, "dpo"))
    return [part.astype(jnp.float32) for part in from_members(owned, kinds, widths, half)]


def layer(
    inputs, space_in, space_out, time_in, time_out, hidden_in, hidden_out, norm_gains, cotangent
):
    fsdp_size = lax.axis_size("fsdp")
    core_size = lax.axis_size("core")
    members = fsdp_size * core_size
    half = space_in.shape[0] // core_size
    core = lax.axis_index("core")

    s_in, s_out, gains = gather_group(
        (space_in, space_out, norm_gains), ("plain", "plain", "gains"), core, half
    )
    t_in, t_out = gather_group((time_in, time_out), ("plain", "plain"), core, half)
    h_in, h_out = gather_group((hidden_in, hidden_out), ("plain", "grouped"), core, half)
    gain_rows = gains.astype(jnp.float32)

    micro, _, frames, places, _ = inputs.shape
    spatial = ("gl", "gm", "ghlm")
    temporal = ("blg", "bmg", "bghlm")

    frames_in = inputs[:, 0].astype(jnp.float32)
    normed_one = layer_norm(frames_in, gain_rows[0]).astype(jnp.bfloat16)
    join_space, total_space, context_space = attend_core(
        normed_one.reshape(micro * frames, places, D), s_in, *spatial
    )
    context_space = context_space.reshape(micro, frames, places, D)
    mixed_one = frames_in + flat_dot(context_space, s_out)
    normed_two = layer_norm(mixed_one, gain_rows[1]).astype(jnp.bfloat16)
    placed = lax.all_to_all(normed_two, "fsdp", split_axis=2, concat_axis=1, tiled=True)
    join_time, total_time, context_placed = attend_core(placed, t_in, *temporal)
    context_time = lax.all_to_all(context_placed, "fsdp", split_axis=1, concat_axis=2, tiled=True)
    mixed_two = mixed_one + flat_dot(context_time, t_out)
    normed_three = layer_norm(mixed_two, gain_rows[2]).astype(jnp.bfloat16)
    hidden = flat_dot(normed_three, h_in)
    activated = jax.nn.gelu(hidden, approximate=False).astype(jnp.bfloat16)
    result = mixed_two + flat_dot(activated, h_out)

    upstream = cotangent[:, 0].astype(jnp.float32)
    rounded = upstream.astype(jnp.bfloat16)
    grad_hidden_out = token_sum(activated, rounded)
    back_active = back_dot(rounded, h_out).astype(jnp.bfloat16)
    _, gelu_pull = jax.vjp(partial(jax.nn.gelu, approximate=False), hidden)
    back_hidden = gelu_pull(back_active.astype(jnp.float32))[0].astype(jnp.bfloat16)
    grad_hidden_in = token_sum(normed_three, back_hidden)
    back_three = back_dot(back_hidden, h_in).astype(jnp.bfloat16)
    ffn_grads = (grad_hidden_in, grad_hidden_out)
    ffn_kinds = ("plain", "grouped")
    packed_ffn, back_three = lax.optimization_barrier(
        (pack_group(ffn_grads, ffn_kinds, members, half), back_three)
    )
    grad_ffn = reduce_group(packed_ffn, ffn_grads, ffn_kinds, half)
    back_mixed, gain_grad_two = norm_back(mixed_two, gain_rows[2], back_three.astype(jnp.float32))
    upstream = upstream + back_mixed
    rounded = upstream.astype(jnp.bfloat16)
    grad_time_out = token_sum(context_time, rounded)
    back_context = back_dot(rounded, t_out).astype(jnp.bfloat16)
    back_placed = lax.all_to_all(back_context, "fsdp", split_axis=2, concat_axis=1, tiled=True)
    back_join = attend_back(join_time, total_time, back_placed, *temporal)
    grad_time_in = token_sum(placed, back_join)
    back_two_placed = back_dot(back_join, t_in).astype(jnp.bfloat16)
    time_grads = (grad_time_in, grad_time_out)
    time_kinds = ("plain", "plain")
    packed_time, back_two_placed = lax.optimization_barrier(
        (pack_group(time_grads, time_kinds, members, half), back_two_placed)
    )
    grad_time = reduce_group(packed_time, time_grads, time_kinds, half)
    back_two = lax.all_to_all(back_two_placed, "fsdp", split_axis=1, concat_axis=2, tiled=True)
    back_mixed, gain_grad_one = norm_back(mixed_one, gain_rows[1], back_two.astype(jnp.float32))
    upstream = upstream + back_mixed
    rounded = upstream.astype(jnp.bfloat16)
    grad_space_out = token_sum(context_space, rounded)
    back_context = back_dot(rounded, s_out).astype(jnp.bfloat16)
    back_join = attend_back(
        join_space, total_space, back_context.reshape(micro * frames, places, D), *spatial
    )
    grad_space_in = token_sum(normed_one, back_join)
    back_one = back_dot(back_join, s_in).astype(jnp.bfloat16).reshape(micro, frames, places, D)
    back_mixed, gain_grad_zero = norm_back(frames_in, gain_rows[0], back_one.astype(jnp.float32))
    input_grad = upstream + back_mixed

    gain_grads = jnp.stack((gain_grad_zero, gain_grad_one, gain_grad_two))
    space_grads = (grad_space_in, grad_space_out, gain_grads)
    space_kinds = ("plain", "plain", "gains")
    grad_space = reduce_group(
        pack_group(space_grads, space_kinds, members, half), space_grads, space_kinds, half
    )
    return (
        result[:, None],
        input_grad[:, None],
        grad_space[0],
        grad_space[1],
        grad_time[0],
        grad_time[1],
        grad_ffn[0],
        grad_ffn[1],
        grad_space[2],
    )


def solution(mesh):
    dp_size, fsdp_size = mesh.devices.shape
    split = Mesh(mesh.devices.reshape(dp_size // 2, 2, fsdp_size), ("dpo", "core", "fsdp"))
    tokens = P(None, ("dpo", "core"), "fsdp", None, None)
    rows = P("fsdp", None)
    return jax.shard_map(
        layer,
        mesh=split,
        in_specs=(tokens, rows, rows, rows, rows, rows, rows, P(None, "fsdp"), tokens),
        out_specs=(tokens, tokens, rows, rows, rows, rows, rows, rows, P(None, "fsdp")),
        check_vma=False,
    )
```

```python
import jax
import jax.numpy as jnp
from jax import lax
from jax.sharding import Mesh
from jax.sharding import PartitionSpec as P


D = 768
HEADS = 12
HEAD_DIM = 64
GAIN_COLS = 128

EPS = 1e-06

MEMBERS = ("fsdp", "core")


def layer_norm(values, scales):
    average = jnp.mean(values, axis=-1, keepdims=True)
    centred = values - average
    spread = jnp.mean(centred * centred, axis=-1, keepdims=True)
    return centred * lax.rsqrt(spread + EPS) * scales


def norm_back(values, scales, incoming):
    _, pullback = jax.vjp(layer_norm, values, scales)
    return pullback(incoming)


def flat_dot(left, right):
    flat = left.reshape(-1, left.shape[-1])
    product = jnp.dot(flat, right, preferred_element_type=jnp.float32)
    return product.reshape(left.shape[:-1] + (right.shape[1],))


def back_dot(left, right):
    flat = left.reshape(-1, left.shape[-1])
    product = lax.dot_general(
        flat, right, (((1,), (1,)), ((), ())), preferred_element_type=jnp.float32
    )
    return product.reshape(left.shape[:-1] + (right.shape[0],))


def token_sum(left, right):
    left_rows = left.reshape(-1, left.shape[-1])
    right_rows = right.reshape(-1, right.shape[-1])
    return lax.dot_general(
        left_rows, right_rows, (((0,), (0,)), ((), ())), preferred_element_type=jnp.float32
    )


def split_join(joined):
    split_heads = joined.reshape(joined.shape[:-1] + (3, HEADS, HEAD_DIM))
    return (split_heads[..., 0, :, :], split_heads[..., 1, :, :], split_heads[..., 2, :, :])


def attend_core(normed, weight_in, token_form, key_form, score_form):
    joined = flat_dot(normed, weight_in).astype(jnp.bfloat16)
    queries, keyset, valueset = split_join(joined)
    factor = HEAD_DIM ** (-0.5)
    scores = (
        jnp.einsum(
            token_form + "hd," + key_form + "hd->" + score_form,
            queries,
            keyset,
            preferred_element_type=jnp.float32,
        )
        * factor
    )
    totals = jax.nn.logsumexp(scores, axis=-1, keepdims=True)
    weighting = jnp.exp(scores - totals).astype(jnp.bfloat16)
    context = jnp.einsum(
        score_form + "," + key_form + "hd->" + token_form + "hd",
        weighting,
        valueset,
        preferred_element_type=jnp.float32,
    )
    context = context.reshape(normed.shape[:-1] + (D,)).astype(jnp.bfloat16)
    return (joined, totals, context)


def attend_back(joined, totals, back_context, token_form, key_form, score_form):
    queries, keyset, valueset = split_join(joined)
    back_heads = back_context.reshape(back_context.shape[:-1] + (HEADS, HEAD_DIM))
    factor = HEAD_DIM ** (-0.5)
    scores = (
        jnp.einsum(
            token_form + "hd," + key_form + "hd->" + score_form,
            queries,
            keyset,
            preferred_element_type=jnp.float32,
        )
        * factor
    )
    weighting = jnp.exp(scores - totals)
    back_weight = jnp.einsum(
        token_form + "hd," + key_form + "hd->" + score_form,
        back_heads,
        valueset,
        preferred_element_type=jnp.float32,
    )
    back_weight = back_weight.astype(jnp.bfloat16).astype(jnp.float32)
    inner_sum = jnp.sum(weighting * back_weight, axis=-1, keepdims=True)
    back_scores = (weighting * (back_weight - inner_sum)).astype(jnp.bfloat16)
    back_query = (
        jnp.einsum(
            score_form + "," + key_form + "hd->" + token_form + "hd",
            back_scores,
            keyset,
            preferred_element_type=jnp.float32,
        )
        * factor
    )
    back_keys = (
        jnp.einsum(
            score_form + "," + token_form + "hd->" + key_form + "hd",
            back_scores,
            queries,
            preferred_element_type=jnp.float32,
        )
        * factor
    )
    back_values = jnp.einsum(
        score_form + "," + token_form + "hd->" + key_form + "hd",
        weighting.astype(jnp.bfloat16),
        back_heads,
        preferred_element_type=jnp.float32,
    )
    shape = back_context.shape[:-1] + (D,)
    return tuple(
        part.reshape(shape).astype(jnp.bfloat16) for part in (back_query, back_keys, back_values)
    )


def join_sum(normed, parts):
    return jnp.concatenate([token_sum(normed, part) for part in parts], axis=1)


def join_back(parts, weight_in):
    total = None
    for index, part in enumerate(parts):
        term = back_dot(part, weight_in[:, index * D:(index + 1) * D])
        total = term if total is None else total + term
    return total


SQRT_HALF = 0.5 ** 0.5


def gelu_parts(hidden):
    tail = lax.erfc(-hidden * SQRT_HALF)
    return 0.5 * hidden * tail, tail


def gelu_back(hidden, tail, incoming):
    slope = 0.5 * tail + hidden * (SQRT_HALF / jnp.sqrt(jnp.pi)) * jnp.exp(-0.5 * hidden * hidden)
    return incoming * slope


def to_member(array, kind, part, half):
    if kind == "gains":
        gain_part = lax.dynamic_slice_in_dim(array, part * half, half, axis=1).T
        return jnp.pad(gain_part, ((0, 0), (0, GAIN_COLS - gain_part.shape[1])))
    if kind == "grouped":
        rows = lax.dynamic_slice_in_dim(array, part * 4 * half, 4 * half, axis=0)
        return jnp.concatenate([rows[q * half:(q + 1) * half] for q in range(4)], axis=1)
    return lax.dynamic_slice_in_dim(array, part * half, half, axis=0)


def width_of(array, kind):
    return {"gains": GAIN_COLS, "grouped": 4 * D}.get(kind, array.shape[-1])


def from_members(block, kinds, widths, half):
    members = block.shape[0] // half
    outs = []
    offset = 0
    for kind, width in zip(kinds, widths):
        part = block[:, offset:offset + width]
        offset += width
        if kind == "gains":
            outs.append(part[:, :3].T)
        elif kind == "grouped":
            grouped = part.reshape(members, half, 4 * D)
            outs.append(
                jnp.concatenate([grouped[:, :, q * D:(q + 1) * D] for q in range(4)], axis=1).reshape(
                    members * 4 * half, D
                )
            )
        else:
            outs.append(part)
    return outs


def to_members_full(array, kind, members, half):
    array = array.astype(jnp.bfloat16)
    if kind == "gains":
        cols = array.T
        return jnp.pad(cols, ((0, 0), (0, GAIN_COLS - cols.shape[1])))
    if kind == "grouped":
        grouped = array.reshape(members, 4 * half, D)
        return jnp.concatenate(
            [grouped[:, q * half:(q + 1) * half, :] for q in range(4)], axis=2
        ).reshape(members * half, 4 * D)
    return array


def gather_group(arrays, kinds, part, half):
    block = jnp.concatenate([to_member(a, k, part, half) for a, k in zip(arrays, kinds)], axis=1)
    widths = [width_of(a, k) for a, k in zip(arrays, kinds)]
    gathered = lax.all_gather(block, MEMBERS, axis=0, tiled=True)
    return from_members(gathered, kinds, widths, half)


def pair_sum(values, axis):
    if lax.axis_size(axis) == 2:
        return values + lax.ppermute(values, axis, [(0, 1), (1, 0)])
    return lax.psum(values, axis)


def core_gather(values):
    if lax.axis_size("core") == 2:
        other = lax.ppermute(values, "core", [(0, 1), (1, 0)])
        first = lax.axis_index("core") == 0
        return jnp.concatenate(
            [jnp.where(first, values, other), jnp.where(first, other, values)], axis=0
        )
    return lax.all_gather(values, "core", axis=0, tiled=True)


def pack_group(grads, kinds, members, half):
    return jnp.concatenate(
        [to_members_full(g, k, members, half) for g, k in zip(grads, kinds)], axis=1
    )


def reduce_group(packed, grads, kinds, half):
    widths = [width_of(g, k) for g, k in zip(grads, kinds)]
    owned = lax.psum_scatter(packed, MEMBERS, scatter_dimension=0, tiled=True)
    owned = core_gather(pair_sum(owned, "dpo"))
    return [part.astype(jnp.float32) for part in from_members(owned, kinds, widths, half)]


def layer(
    inputs, space_in, space_out, time_in, time_out, hidden_in, hidden_out, norm_gains, cotangent
):
    fsdp_size = lax.axis_size("fsdp")
    core_size = lax.axis_size("core")
    members = fsdp_size * core_size
    half = space_in.shape[0] // core_size
    core = lax.axis_index("core")

    s_in, s_out, gains = gather_group(
        (space_in, space_out, norm_gains), ("plain", "plain", "gains"), core, half
    )
    t_in, t_out = gather_group((time_in, time_out), ("plain", "plain"), core, half)
    h_in, h_out = gather_group((hidden_in, hidden_out), ("plain", "grouped"), core, half)
    gain_rows = gains.astype(jnp.float32)

    micro = inputs.shape[0]
    spatial = ("gl", "gm", "ghlm")
    temporal = ("lg", "mg", "ghlm")

    saved = []
    results = []
    for index in range(micro):
        frames_in = inputs[index, 0].astype(jnp.float32)
        normed_one = layer_norm(frames_in, gain_rows[0]).astype(jnp.bfloat16)
        join_space, total_space, context_space = attend_core(normed_one, s_in, *spatial)
        mixed_one = frames_in + flat_dot(context_space, s_out)
        normed_two = layer_norm(mixed_one, gain_rows[1]).astype(jnp.bfloat16)
        placed = lax.all_to_all(normed_two, "fsdp", split_axis=1, concat_axis=0, tiled=True)
        join_time, total_time, context_placed = attend_core(placed, t_in, *temporal)
        context_time = lax.all_to_all(
            context_placed, "fsdp", split_axis=0, concat_axis=1, tiled=True
        )
        mixed_two = mixed_one + flat_dot(context_time, t_out)
        normed_three = layer_norm(mixed_two, gain_rows[2]).astype(jnp.bfloat16)
        hidden = flat_dot(normed_three, h_in)
        activated, tail = gelu_parts(hidden)
        activated = activated.astype(jnp.bfloat16)
        results.append(mixed_two + flat_dot(activated, h_out))
        saved.append(
            dict(
                frames_in=frames_in,
                normed_one=normed_one,
                join_space=join_space,
                total_space=total_space,
                context_space=context_space,
                mixed_one=mixed_one,
                placed=placed,
                join_time=join_time,
                total_time=total_time,
                context_time=context_time,
                mixed_two=mixed_two,
                normed_three=normed_three,
                hidden=hidden,
                tail=tail,
                activated=activated,
            )
        )

    def summed(terms):
        total = terms[0]
        for term in terms[1:]:
            total = total + term
        return total

    upstreams = []
    back_threes = []
    gain_two_terms = []
    hidden_out_terms = []
    hidden_in_terms = []
    for index in range(micro):
        s = saved[index]
        upstream = cotangent[index, 0].astype(jnp.float32)
        rounded = upstream.astype(jnp.bfloat16)
        hidden_out_terms.append(token_sum(s["activated"], rounded))
        back_active = back_dot(rounded, h_out).astype(jnp.bfloat16)
        back_hidden = gelu_back(
            s["hidden"], s["tail"], back_active.astype(jnp.float32)
        ).astype(jnp.bfloat16)
        hidden_in_terms.append(token_sum(s["normed_three"], back_hidden))
        back_threes.append(back_dot(back_hidden, h_in).astype(jnp.bfloat16))
        upstreams.append(upstream)
    ffn_grads = (summed(hidden_in_terms), summed(hidden_out_terms))
    ffn_kinds = ("plain", "grouped")
    packed_ffn, back_threes[-1] = lax.optimization_barrier(
        (pack_group(ffn_grads, ffn_kinds, members, half), back_threes[-1])
    )
    grad_ffn = reduce_group(packed_ffn, ffn_grads, ffn_kinds, half)

    back_twos_placed = []
    time_out_terms = []
    time_in_terms = []
    for index in range(micro):
        s = saved[index]
        back_mixed, gain_grad = norm_back(
            s["mixed_two"], gain_rows[2], back_threes[index].astype(jnp.float32)
        )
        gain_two_terms.append(gain_grad)
        upstream = upstreams[index] + back_mixed
        upstreams[index] = upstream
        rounded = upstream.astype(jnp.bfloat16)
        time_out_terms.append(token_sum(s["context_time"], rounded))
        back_context = back_dot(rounded, t_out).astype(jnp.bfloat16)
        back_placed = lax.all_to_all(back_context, "fsdp", split_axis=1, concat_axis=0, tiled=True)
        back_join = attend_back(s["join_time"], s["total_time"], back_placed, *temporal)
        time_in_terms.append(join_sum(s["placed"], back_join))
        back_twos_placed.append(join_back(back_join, t_in).astype(jnp.bfloat16))
    time_grads = (summed(time_in_terms), summed(time_out_terms))
    time_kinds = ("plain", "plain")
    packed_time, back_twos_placed[-1] = lax.optimization_barrier(
        (pack_group(time_grads, time_kinds, members, half), back_twos_placed[-1])
    )
    grad_time = reduce_group(packed_time, time_grads, time_kinds, half)

    input_grads = []
    gain_one_terms = []
    gain_zero_terms = []
    space_out_terms = []
    space_in_terms = []
    for index in range(micro):
        s = saved[index]
        back_two = lax.all_to_all(
            back_twos_placed[index], "fsdp", split_axis=0, concat_axis=1, tiled=True
        )
        back_mixed, gain_grad = norm_back(s["mixed_one"], gain_rows[1], back_two.astype(jnp.float32))
        gain_one_terms.append(gain_grad)
        upstream = upstreams[index] + back_mixed
        rounded = upstream.astype(jnp.bfloat16)
        space_out_terms.append(token_sum(s["context_space"], rounded))
        back_context = back_dot(rounded, s_out).astype(jnp.bfloat16)
        back_join = attend_back(s["join_space"], s["total_space"], back_context, *spatial)
        space_in_terms.append(join_sum(s["normed_one"], back_join))
        back_one = join_back(back_join, s_in).astype(jnp.bfloat16)
        back_mixed, gain_grad = norm_back(
            s["frames_in"], gain_rows[0], back_one.astype(jnp.float32)
        )
        gain_zero_terms.append(gain_grad)
        input_grads.append(upstream + back_mixed)
    grad_space_in = summed(space_in_terms)
    grad_space_out = summed(space_out_terms)
    gain_grad_zero = summed(gain_zero_terms)
    gain_grad_one = summed(gain_one_terms)
    gain_grad_two = summed(gain_two_terms)
    result = jnp.stack(results)
    input_grad = jnp.stack(input_grads)

    gain_grads = jnp.stack((gain_grad_zero, gain_grad_one, gain_grad_two))
    space_grads = (grad_space_in, grad_space_out, gain_grads)
    space_kinds = ("plain", "plain", "gains")
    grad_space = reduce_group(
        pack_group(space_grads, space_kinds, members, half), space_grads, space_kinds, half
    )
    return (
        result[:, None],
        input_grad[:, None],
        grad_space[0],
        grad_space[1],
        grad_time[0],
        grad_time[1],
        grad_ffn[0],
        grad_ffn[1],
        grad_space[2],
    )


def solution(mesh):
    dp_size, fsdp_size = mesh.devices.shape
    split = Mesh(mesh.devices.reshape(dp_size // 2, 2, fsdp_size), ("dpo", "core", "fsdp"))
    tokens = P(None, ("dpo", "core"), "fsdp", None, None)
    rows = P("fsdp", None)
    return jax.shard_map(
        layer,
        mesh=split,
        in_specs=(tokens, rows, rows, rows, rows, rows, rows, P(None, "fsdp"), tokens),
        out_specs=(tokens, tokens, rows, rows, rows, rows, rows, rows, P(None, "fsdp")),
        check_vma=False,
    )
```

```python
from functools import partial

import jax
import jax.numpy as jnp
from jax import lax
from jax.sharding import Mesh
from jax.sharding import PartitionSpec as P


D = 768
HEADS = 12
HEAD_DIM = 64
GAIN_COLS = 128

EPS = 1e-06

MEMBERS = ("fsdp", "core")


def layer_norm(values, scales):
    average = jnp.mean(values, axis=-1, keepdims=True)
    centred = values - average
    spread = jnp.mean(centred * centred, axis=-1, keepdims=True)
    return centred * lax.rsqrt(spread + EPS) * scales


def norm_back(values, scales, incoming):
    _, pullback = jax.vjp(layer_norm, values, scales)
    return pullback(incoming)


def flat_dot(left, right):
    flat = left.reshape(-1, left.shape[-1])
    product = jnp.dot(flat, right, preferred_element_type=jnp.float32)
    return product.reshape(left.shape[:-1] + (right.shape[1],))


def back_dot(left, right):
    flat = left.reshape(-1, left.shape[-1])
    product = lax.dot_general(
        flat, right, (((1,), (1,)), ((), ())), preferred_element_type=jnp.float32
    )
    return product.reshape(left.shape[:-1] + (right.shape[0],))


def token_sum(left, right):
    left_rows = left.reshape(-1, left.shape[-1])
    right_rows = right.reshape(-1, right.shape[-1])
    return lax.dot_general(
        left_rows, right_rows, (((0,), (0,)), ((), ())), preferred_element_type=jnp.float32
    )


def split_join(joined):
    split_heads = joined.reshape(joined.shape[:-1] + (3, HEADS, HEAD_DIM))
    return (split_heads[..., 0, :, :], split_heads[..., 1, :, :], split_heads[..., 2, :, :])


def attend_core(normed, weight_in, token_form, key_form, score_form):
    joined = flat_dot(normed, weight_in).astype(jnp.bfloat16)
    queries, keyset, valueset = split_join(joined)
    factor = HEAD_DIM ** (-0.5)
    scores = (
        jnp.einsum(
            token_form + "hd," + key_form + "hd->" + score_form,
            queries,
            keyset,
            preferred_element_type=jnp.float32,
        )
        * factor
    )
    totals = jax.nn.logsumexp(scores, axis=-1, keepdims=True)
    weighting = jnp.exp(scores - totals).astype(jnp.bfloat16)
    context = jnp.einsum(
        score_form + "," + key_form + "hd->" + token_form + "hd",
        weighting,
        valueset,
        preferred_element_type=jnp.float32,
    )
    context = context.reshape(normed.shape[:-1] + (D,)).astype(jnp.bfloat16)
    return (joined, totals, context)


def attend_back(joined, totals, back_context, token_form, key_form, score_form):
    queries, keyset, valueset = split_join(joined)
    back_heads = back_context.reshape(back_context.shape[:-1] + (HEADS, HEAD_DIM))
    factor = HEAD_DIM ** (-0.5)
    scores = (
        jnp.einsum(
            token_form + "hd," + key_form + "hd->" + score_form,
            queries,
            keyset,
            preferred_element_type=jnp.float32,
        )
        * factor
    )
    weighting = jnp.exp(scores - totals)
    back_weight = jnp.einsum(
        token_form + "hd," + key_form + "hd->" + score_form,
        back_heads,
        valueset,
        preferred_element_type=jnp.float32,
    )
    back_weight = back_weight.astype(jnp.bfloat16).astype(jnp.float32)
    inner_sum = jnp.sum(weighting * back_weight, axis=-1, keepdims=True)
    back_scores = (weighting * (back_weight - inner_sum)).astype(jnp.bfloat16)
    back_query = (
        jnp.einsum(
            score_form + "," + key_form + "hd->" + token_form + "hd",
            back_scores,
            keyset,
            preferred_element_type=jnp.float32,
        )
        * factor
    )
    back_keys = (
        jnp.einsum(
            score_form + "," + token_form + "hd->" + key_form + "hd",
            back_scores,
            queries,
            preferred_element_type=jnp.float32,
        )
        * factor
    )
    back_values = jnp.einsum(
        score_form + "," + token_form + "hd->" + key_form + "hd",
        weighting.astype(jnp.bfloat16),
        back_heads,
        preferred_element_type=jnp.float32,
    )
    stacked = jnp.stack((back_query, back_keys, back_values), axis=-3)
    return stacked.reshape(back_context.shape[:-1] + (3 * D,)).astype(jnp.bfloat16)


def to_member(array, kind, part, half):
    if kind == "gains":
        gain_part = lax.dynamic_slice_in_dim(array, part * half, half, axis=1).T
        return jnp.pad(gain_part, ((0, 0), (0, GAIN_COLS - gain_part.shape[1])))
    if kind == "grouped":
        rows = lax.dynamic_slice_in_dim(array, part * 4 * half, 4 * half, axis=0)
        return jnp.concatenate([rows[q * half:(q + 1) * half] for q in range(4)], axis=1)
    return lax.dynamic_slice_in_dim(array, part * half, half, axis=0)


def width_of(array, kind):
    return {"gains": GAIN_COLS, "grouped": 4 * D}.get(kind, array.shape[-1])


def from_members(block, kinds, widths, half):
    members = block.shape[0] // half
    outs = []
    offset = 0
    for kind, width in zip(kinds, widths):
        part = block[:, offset:offset + width]
        offset += width
        if kind == "gains":
            outs.append(part[:, :3].T)
        elif kind == "grouped":
            grouped = part.reshape(members, half, 4 * D)
            outs.append(
                jnp.concatenate([grouped[:, :, q * D:(q + 1) * D] for q in range(4)], axis=1).reshape(
                    members * 4 * half, D
                )
            )
        else:
            outs.append(part)
    return outs


def to_members_full(array, kind, members, half):
    array = array.astype(jnp.bfloat16)
    if kind == "gains":
        cols = array.T
        return jnp.pad(cols, ((0, 0), (0, GAIN_COLS - cols.shape[1])))
    if kind == "grouped":
        grouped = array.reshape(members, 4 * half, D)
        return jnp.concatenate(
            [grouped[:, q * half:(q + 1) * half, :] for q in range(4)], axis=2
        ).reshape(members * half, 4 * D)
    return array


def gather_group(arrays, kinds, part, half):
    block = jnp.concatenate([to_member(a, k, part, half) for a, k in zip(arrays, kinds)], axis=1)
    widths = [width_of(a, k) for a, k in zip(arrays, kinds)]
    gathered = lax.all_gather(block, MEMBERS, axis=0, tiled=True)
    return from_members(gathered, kinds, widths, half)


def pair_sum(values, axis):
    if lax.axis_size(axis) == 2:
        return values + lax.ppermute(values, axis, [(0, 1), (1, 0)])
    return lax.psum(values, axis)


def core_gather(values):
    if lax.axis_size("core") == 2:
        other = lax.ppermute(values, "core", [(0, 1), (1, 0)])
        first = lax.axis_index("core") == 0
        return jnp.concatenate(
            [jnp.where(first, values, other), jnp.where(first, other, values)], axis=0
        )
    return lax.all_gather(values, "core", axis=0, tiled=True)


def pack_group(grads, kinds, members, half):
    return jnp.concatenate(
        [to_members_full(g, k, members, half) for g, k in zip(grads, kinds)], axis=1
    )


def reduce_group(packed, grads, kinds, half):
    widths = [width_of(g, k) for g, k in zip(grads, kinds)]
    owned = lax.psum_scatter(packed, MEMBERS, scatter_dimension=0, tiled=True)
    owned = core_gather(pair_sum(owned, "dpo"))
    return [part.astype(jnp.float32) for part in from_members(owned, kinds, widths, half)]


def layer(
    inputs, space_in, space_out, time_in, time_out, hidden_in, hidden_out, norm_gains, cotangent
):
    fsdp_size = lax.axis_size("fsdp")
    core_size = lax.axis_size("core")
    members = fsdp_size * core_size
    half = space_in.shape[0] // core_size
    core = lax.axis_index("core")

    s_in, s_out, gains = gather_group(
        (space_in, space_out, norm_gains), ("plain", "plain", "gains"), core, half
    )
    t_in, t_out = gather_group((time_in, time_out), ("plain", "plain"), core, half)
    h_in, h_out = gather_group((hidden_in, hidden_out), ("plain", "grouped"), core, half)
    gain_rows = gains.astype(jnp.float32)

    micro = inputs.shape[0]
    spatial = ("gl", "gm", "ghlm")
    temporal = ("lg", "mg", "ghlm")

    saved = []
    results = []
    for index in range(micro):
        frames_in = inputs[index, 0].astype(jnp.float32)
        normed_one = layer_norm(frames_in, gain_rows[0]).astype(jnp.bfloat16)
        join_space, total_space, context_space = attend_core(normed_one, s_in, *spatial)
        mixed_one = frames_in + flat_dot(context_space, s_out)
        normed_two = layer_norm(mixed_one, gain_rows[1]).astype(jnp.bfloat16)
        placed = lax.all_to_all(normed_two, "fsdp", split_axis=1, concat_axis=0, tiled=True)
        join_time, total_time, context_placed = attend_core(placed, t_in, *temporal)
        context_time = lax.all_to_all(
            context_placed, "fsdp", split_axis=0, concat_axis=1, tiled=True
        )
        mixed_two = mixed_one + flat_dot(context_time, t_out)
        normed_three = layer_norm(mixed_two, gain_rows[2]).astype(jnp.bfloat16)
        hidden = flat_dot(normed_three, h_in)
        activated = jax.nn.gelu(hidden, approximate=False).astype(jnp.bfloat16)
        results.append(mixed_two + flat_dot(activated, h_out))
        saved.append(
            dict(
                frames_in=frames_in,
                normed_one=normed_one,
                join_space=join_space,
                total_space=total_space,
                context_space=context_space,
                mixed_one=mixed_one,
                placed=placed,
                join_time=join_time,
                total_time=total_time,
                context_time=context_time,
                mixed_two=mixed_two,
                normed_three=normed_three,
                hidden=hidden,
                activated=activated,
            )
        )

    def summed(terms):
        total = terms[0]
        for term in terms[1:]:
            total = total + term
        return total

    upstreams = []
    back_threes = []
    gain_two_terms = []
    hidden_out_terms = []
    hidden_in_terms = []
    for index in range(micro):
        s = saved[index]
        upstream = cotangent[index, 0].astype(jnp.float32)
        rounded = upstream.astype(jnp.bfloat16)
        hidden_out_terms.append(token_sum(s["activated"], rounded))
        back_active = back_dot(rounded, h_out).astype(jnp.bfloat16)
        _, gelu_pull = jax.vjp(partial(jax.nn.gelu, approximate=False), s["hidden"])
        back_hidden = gelu_pull(back_active.astype(jnp.float32))[0].astype(jnp.bfloat16)
        hidden_in_terms.append(token_sum(s["normed_three"], back_hidden))
        back_threes.append(back_dot(back_hidden, h_in).astype(jnp.bfloat16))
        upstreams.append(upstream)
    ffn_grads = (summed(hidden_in_terms), summed(hidden_out_terms))
    ffn_kinds = ("plain", "grouped")
    packed_ffn, back_threes[-1] = lax.optimization_barrier(
        (pack_group(ffn_grads, ffn_kinds, members, half), back_threes[-1])
    )
    grad_ffn = reduce_group(packed_ffn, ffn_grads, ffn_kinds, half)

    back_twos_placed = []
    time_out_terms = []
    time_in_terms = []
    for index in range(micro):
        s = saved[index]
        back_mixed, gain_grad = norm_back(
            s["mixed_two"], gain_rows[2], back_threes[index].astype(jnp.float32)
        )
        gain_two_terms.append(gain_grad)
        upstream = upstreams[index] + back_mixed
        upstreams[index] = upstream
        rounded = upstream.astype(jnp.bfloat16)
        time_out_terms.append(token_sum(s["context_time"], rounded))
        back_context = back_dot(rounded, t_out).astype(jnp.bfloat16)
        back_placed = lax.all_to_all(back_context, "fsdp", split_axis=1, concat_axis=0, tiled=True)
        back_join = attend_back(s["join_time"], s["total_time"], back_placed, *temporal)
        time_in_terms.append(token_sum(s["placed"], back_join))
        back_twos_placed.append(back_dot(back_join, t_in).astype(jnp.bfloat16))
    time_grads = (summed(time_in_terms), summed(time_out_terms))
    time_kinds = ("plain", "plain")
    packed_time, back_twos_placed[-1] = lax.optimization_barrier(
        (pack_group(time_grads, time_kinds, members, half), back_twos_placed[-1])
    )
    grad_time = reduce_group(packed_time, time_grads, time_kinds, half)

    input_grads = []
    gain_one_terms = []
    gain_zero_terms = []
    space_out_terms = []
    space_in_terms = []
    for index in range(micro):
        s = saved[index]
        back_two = lax.all_to_all(
            back_twos_placed[index], "fsdp", split_axis=0, concat_axis=1, tiled=True
        )
        if index == micro - 1:
            back_two, grad_ffn = lax.optimization_barrier((back_two, grad_ffn))
        back_mixed, gain_grad = norm_back(s["mixed_one"], gain_rows[1], back_two.astype(jnp.float32))
        gain_one_terms.append(gain_grad)
        upstream = upstreams[index] + back_mixed
        rounded = upstream.astype(jnp.bfloat16)
        space_out_terms.append(token_sum(s["context_space"], rounded))
        back_context = back_dot(rounded, s_out).astype(jnp.bfloat16)
        back_join = attend_back(s["join_space"], s["total_space"], back_context, *spatial)
        space_in_terms.append(token_sum(s["normed_one"], back_join))
        back_one = back_dot(back_join, s_in).astype(jnp.bfloat16)
        back_mixed, gain_grad = norm_back(
            s["frames_in"], gain_rows[0], back_one.astype(jnp.float32)
        )
        gain_zero_terms.append(gain_grad)
        input_grads.append(upstream + back_mixed)
    grad_space_in = summed(space_in_terms)
    grad_space_out = summed(space_out_terms)
    gain_grad_zero = summed(gain_zero_terms)
    gain_grad_one = summed(gain_one_terms)
    gain_grad_two = summed(gain_two_terms)
    result = jnp.stack(results)
    input_grad = jnp.stack(input_grads)

    gain_grads = jnp.stack((gain_grad_zero, gain_grad_one, gain_grad_two))
    space_grads = (grad_space_in, grad_space_out, gain_grads)
    space_kinds = ("plain", "plain", "gains")
    grad_space = reduce_group(
        pack_group(space_grads, space_kinds, members, half), space_grads, space_kinds, half
    )
    return (
        result[:, None],
        input_grad[:, None],
        grad_space[0],
        grad_space[1],
        grad_time[0],
        grad_time[1],
        grad_ffn[0],
        grad_ffn[1],
        grad_space[2],
    )


def solution(mesh):
    dp_size, fsdp_size = mesh.devices.shape
    split = Mesh(mesh.devices.reshape(dp_size // 2, 2, fsdp_size), ("dpo", "core", "fsdp"))
    tokens = P(None, ("dpo", "core"), "fsdp", None, None)
    rows = P("fsdp", None)
    return jax.shard_map(
        layer,
        mesh=split,
        in_specs=(tokens, rows, rows, rows, rows, rows, rows, P(None, "fsdp"), tokens),
        out_specs=(tokens, tokens, rows, rows, rows, rows, rows, rows, P(None, "fsdp")),
        check_vma=False,
    )
```

```python
import jax
import jax.numpy as jnp
from jax import lax
from jax.sharding import Mesh
from jax.sharding import PartitionSpec as P


D = 768
HEADS = 12
HEAD_DIM = 64
GAIN_COLS = 128

EPS = 1e-06

MEMBERS = ("fsdp", "core")


def layer_norm(values, scales):
    average = jnp.mean(values, axis=-1, keepdims=True)
    centred = values - average
    spread = jnp.mean(centred * centred, axis=-1, keepdims=True)
    return centred * lax.rsqrt(spread + EPS) * scales


def norm_back(values, scales, incoming):
    _, pullback = jax.vjp(layer_norm, values, scales)
    return pullback(incoming)


def flat_dot(left, right):
    flat = left.reshape(-1, left.shape[-1])
    product = jnp.dot(flat, right, preferred_element_type=jnp.float32)
    return product.reshape(left.shape[:-1] + (right.shape[1],))


def back_dot(left, right):
    flat = left.reshape(-1, left.shape[-1])
    product = lax.dot_general(
        flat, right, (((1,), (1,)), ((), ())), preferred_element_type=jnp.float32
    )
    return product.reshape(left.shape[:-1] + (right.shape[0],))


def token_sum(left, right):
    left_rows = left.reshape(-1, left.shape[-1])
    right_rows = right.reshape(-1, right.shape[-1])
    return lax.dot_general(
        left_rows, right_rows, (((0,), (0,)), ((), ())), preferred_element_type=jnp.float32
    )


def split_join(joined):
    split_heads = joined.reshape(joined.shape[:-1] + (3, HEADS, HEAD_DIM))
    return (split_heads[..., 0, :, :], split_heads[..., 1, :, :], split_heads[..., 2, :, :])


def attend_core(normed, weight_in, token_form, key_form, score_form):
    joined = flat_dot(normed, weight_in).astype(jnp.bfloat16)
    queries, keyset, valueset = split_join(joined)
    factor = HEAD_DIM ** (-0.5)
    scores = (
        jnp.einsum(
            token_form + "hd," + key_form + "hd->" + score_form,
            queries,
            keyset,
            preferred_element_type=jnp.float32,
        )
        * factor
    )
    totals = jax.nn.logsumexp(scores, axis=-1, keepdims=True)
    weighting = jnp.exp(scores - totals).astype(jnp.bfloat16)
    context = jnp.einsum(
        score_form + "," + key_form + "hd->" + token_form + "hd",
        weighting,
        valueset,
        preferred_element_type=jnp.float32,
    )
    context = context.reshape(normed.shape[:-1] + (D,)).astype(jnp.bfloat16)
    return (joined, totals, context)


def attend_back(joined, totals, back_context, token_form, key_form, score_form):
    queries, keyset, valueset = split_join(joined)
    back_heads = back_context.reshape(back_context.shape[:-1] + (HEADS, HEAD_DIM))
    factor = HEAD_DIM ** (-0.5)
    scores = (
        jnp.einsum(
            token_form + "hd," + key_form + "hd->" + score_form,
            queries,
            keyset,
            preferred_element_type=jnp.float32,
        )
        * factor
    )
    weighting = jnp.exp(scores - totals)
    back_weight = jnp.einsum(
        token_form + "hd," + key_form + "hd->" + score_form,
        back_heads,
        valueset,
        preferred_element_type=jnp.float32,
    )
    back_weight = back_weight.astype(jnp.bfloat16).astype(jnp.float32)
    inner_sum = jnp.sum(weighting * back_weight, axis=-1, keepdims=True)
    back_scores = (weighting * (back_weight - inner_sum)).astype(jnp.bfloat16)
    back_query = (
        jnp.einsum(
            score_form + "," + key_form + "hd->" + token_form + "hd",
            back_scores,
            keyset,
            preferred_element_type=jnp.float32,
        )
        * factor
    )
    back_keys = (
        jnp.einsum(
            score_form + "," + token_form + "hd->" + key_form + "hd",
            back_scores,
            queries,
            preferred_element_type=jnp.float32,
        )
        * factor
    )
    back_values = jnp.einsum(
        score_form + "," + token_form + "hd->" + key_form + "hd",
        weighting.astype(jnp.bfloat16),
        back_heads,
        preferred_element_type=jnp.float32,
    )
    stacked = jnp.stack((back_query, back_keys, back_values), axis=-3)
    return stacked.reshape(back_context.shape[:-1] + (3 * D,)).astype(jnp.bfloat16)


def gelu(values):
    return 0.5 * values * (1.0 + lax.erf(values * (0.5 ** 0.5)))


def to_member(array, kind, part, half):
    if kind == "gains":
        gain_part = lax.dynamic_slice_in_dim(array, part * half, half, axis=1).T
        return jnp.pad(gain_part, ((0, 0), (0, GAIN_COLS - gain_part.shape[1])))
    if kind == "grouped":
        rows = lax.dynamic_slice_in_dim(array, part * 4 * half, 4 * half, axis=0)
        return jnp.concatenate([rows[q * half:(q + 1) * half] for q in range(4)], axis=1)
    return lax.dynamic_slice_in_dim(array, part * half, half, axis=0)


def width_of(array, kind):
    return {"gains": GAIN_COLS, "grouped": 4 * D}.get(kind, array.shape[-1])


def from_members(block, kinds, widths, half):
    members = block.shape[0] // half
    outs = []
    offset = 0
    for kind, width in zip(kinds, widths):
        part = block[:, offset:offset + width]
        offset += width
        if kind == "gains":
            outs.append(part[:, :3].T)
        elif kind == "grouped":
            grouped = part.reshape(members, half, 4 * D)
            outs.append(
                jnp.concatenate([grouped[:, :, q * D:(q + 1) * D] for q in range(4)], axis=1).reshape(
                    members * 4 * half, D
                )
            )
        else:
            outs.append(part)
    return outs


def to_members_full(array, kind, members, half):
    array = array.astype(jnp.bfloat16)
    if kind == "gains":
        cols = array.T
        return jnp.pad(cols, ((0, 0), (0, GAIN_COLS - cols.shape[1])))
    if kind == "grouped":
        grouped = array.reshape(members, 4 * half, D)
        return jnp.concatenate(
            [grouped[:, q * half:(q + 1) * half, :] for q in range(4)], axis=2
        ).reshape(members * half, 4 * D)
    return array


def gather_group(arrays, kinds, part, half):
    block = jnp.concatenate([to_member(a, k, part, half) for a, k in zip(arrays, kinds)], axis=1)
    widths = [width_of(a, k) for a, k in zip(arrays, kinds)]
    gathered = lax.all_gather(block, MEMBERS, axis=0, tiled=True)
    return from_members(gathered, kinds, widths, half)


def pair_sum(values, axis):
    if lax.axis_size(axis) == 2:
        return values + lax.ppermute(values, axis, [(0, 1), (1, 0)])
    return lax.psum(values, axis)


def core_gather(values):
    if lax.axis_size("core") == 2:
        other = lax.ppermute(values, "core", [(0, 1), (1, 0)])
        first = lax.axis_index("core") == 0
        return jnp.concatenate(
            [jnp.where(first, values, other), jnp.where(first, other, values)], axis=0
        )
    return lax.all_gather(values, "core", axis=0, tiled=True)


def pack_group(grads, kinds, members, half):
    return jnp.concatenate(
        [to_members_full(g, k, members, half) for g, k in zip(grads, kinds)], axis=1
    )


def reduce_group(packed, grads, kinds, half):
    widths = [width_of(g, k) for g, k in zip(grads, kinds)]
    owned = lax.psum_scatter(packed, MEMBERS, scatter_dimension=0, tiled=True)
    owned = core_gather(pair_sum(owned, "dpo"))
    return [part.astype(jnp.float32) for part in from_members(owned, kinds, widths, half)]


def layer(
    inputs, space_in, space_out, time_in, time_out, hidden_in, hidden_out, norm_gains, cotangent
):
    fsdp_size = lax.axis_size("fsdp")
    core_size = lax.axis_size("core")
    members = fsdp_size * core_size
    half = space_in.shape[0] // core_size
    core = lax.axis_index("core")

    s_in, s_out, gains = gather_group(
        (space_in, space_out, norm_gains), ("plain", "plain", "gains"), core, half
    )
    t_in, t_out = gather_group((time_in, time_out), ("plain", "plain"), core, half)
    h_in, h_out = gather_group((hidden_in, hidden_out), ("plain", "grouped"), core, half)
    gain_rows = gains.astype(jnp.float32)

    micro = inputs.shape[0]
    spatial = ("gl", "gm", "ghlm")
    temporal = ("lg", "mg", "ghlm")

    saved = []
    results = []
    for index in range(micro):
        frames_in = inputs[index, 0].astype(jnp.float32)
        normed_one = layer_norm(frames_in, gain_rows[0]).astype(jnp.bfloat16)
        join_space, total_space, context_space = attend_core(normed_one, s_in, *spatial)
        mixed_one = frames_in + flat_dot(context_space, s_out)
        normed_two = layer_norm(mixed_one, gain_rows[1]).astype(jnp.bfloat16)
        placed = lax.all_to_all(normed_two, "fsdp", split_axis=1, concat_axis=0, tiled=True)
        join_time, total_time, context_placed = attend_core(placed, t_in, *temporal)
        context_time = lax.all_to_all(
            context_placed, "fsdp", split_axis=0, concat_axis=1, tiled=True
        )
        mixed_two = mixed_one + flat_dot(context_time, t_out)
        normed_three = layer_norm(mixed_two, gain_rows[2]).astype(jnp.bfloat16)
        hidden = flat_dot(normed_three, h_in)
        activated = gelu(hidden).astype(jnp.bfloat16)
        results.append(mixed_two + flat_dot(activated, h_out))
        saved.append(
            dict(
                frames_in=frames_in,
                normed_one=normed_one,
                join_space=join_space,
                total_space=total_space,
                context_space=context_space,
                mixed_one=mixed_one,
                placed=placed,
                join_time=join_time,
                total_time=total_time,
                context_time=context_time,
                mixed_two=mixed_two,
                normed_three=normed_three,
                hidden=hidden,
                activated=activated,
            )
        )

    def summed(terms):
        total = terms[0]
        for term in terms[1:]:
            total = total + term
        return total

    upstreams = []
    back_threes = []
    gain_two_terms = []
    hidden_out_terms = []
    hidden_in_terms = []
    for index in range(micro):
        s = saved[index]
        upstream = cotangent[index, 0].astype(jnp.float32)
        rounded = upstream.astype(jnp.bfloat16)
        hidden_out_terms.append(token_sum(s["activated"], rounded))
        back_active = back_dot(rounded, h_out).astype(jnp.bfloat16)
        _, gelu_pull = jax.vjp(gelu, s["hidden"])
        back_hidden = gelu_pull(back_active.astype(jnp.float32))[0].astype(jnp.bfloat16)
        hidden_in_terms.append(token_sum(s["normed_three"], back_hidden))
        back_threes.append(back_dot(back_hidden, h_in).astype(jnp.bfloat16))
        upstreams.append(upstream)
    ffn_grads = (summed(hidden_in_terms), summed(hidden_out_terms))
    ffn_kinds = ("plain", "grouped")
    packed_ffn, back_threes[-1] = lax.optimization_barrier(
        (pack_group(ffn_grads, ffn_kinds, members, half), back_threes[-1])
    )
    grad_ffn = reduce_group(packed_ffn, ffn_grads, ffn_kinds, half)

    back_twos_placed = []
    time_out_terms = []
    time_in_terms = []
    for index in range(micro):
        s = saved[index]
        back_mixed, gain_grad = norm_back(
            s["mixed_two"], gain_rows[2], back_threes[index].astype(jnp.float32)
        )
        gain_two_terms.append(gain_grad)
        upstream = upstreams[index] + back_mixed
        upstreams[index] = upstream
        rounded = upstream.astype(jnp.bfloat16)
        time_out_terms.append(token_sum(s["context_time"], rounded))
        back_context = back_dot(rounded, t_out).astype(jnp.bfloat16)
        back_placed = lax.all_to_all(back_context, "fsdp", split_axis=1, concat_axis=0, tiled=True)
        back_join = attend_back(s["join_time"], s["total_time"], back_placed, *temporal)
        time_in_terms.append(token_sum(s["placed"], back_join))
        back_twos_placed.append(back_dot(back_join, t_in).astype(jnp.bfloat16))
    time_grads = (summed(time_in_terms), summed(time_out_terms))
    time_kinds = ("plain", "plain")
    packed_time, back_twos_placed[-1] = lax.optimization_barrier(
        (pack_group(time_grads, time_kinds, members, half), back_twos_placed[-1])
    )
    grad_time = reduce_group(packed_time, time_grads, time_kinds, half)

    input_grads = []
    gain_one_terms = []
    gain_zero_terms = []
    space_out_terms = []
    space_in_terms = []
    for index in range(micro):
        s = saved[index]
        back_two = lax.all_to_all(
            back_twos_placed[index], "fsdp", split_axis=0, concat_axis=1, tiled=True
        )
        back_mixed, gain_grad = norm_back(s["mixed_one"], gain_rows[1], back_two.astype(jnp.float32))
        gain_one_terms.append(gain_grad)
        upstream = upstreams[index] + back_mixed
        rounded = upstream.astype(jnp.bfloat16)
        space_out_terms.append(token_sum(s["context_space"], rounded))
        back_context = back_dot(rounded, s_out).astype(jnp.bfloat16)
        back_join = attend_back(s["join_space"], s["total_space"], back_context, *spatial)
        space_in_terms.append(token_sum(s["normed_one"], back_join))
        back_one = back_dot(back_join, s_in).astype(jnp.bfloat16)
        back_mixed, gain_grad = norm_back(
            s["frames_in"], gain_rows[0], back_one.astype(jnp.float32)
        )
        gain_zero_terms.append(gain_grad)
        input_grads.append(upstream + back_mixed)
    grad_space_in = summed(space_in_terms)
    grad_space_out = summed(space_out_terms)
    gain_grad_zero = summed(gain_zero_terms)
    gain_grad_one = summed(gain_one_terms)
    gain_grad_two = summed(gain_two_terms)
    result = jnp.stack(results)
    input_grad = jnp.stack(input_grads)

    gain_grads = jnp.stack((gain_grad_zero, gain_grad_one, gain_grad_two))
    space_grads = (grad_space_in, grad_space_out, gain_grads)
    space_kinds = ("plain", "plain", "gains")
    grad_space = reduce_group(
        pack_group(space_grads, space_kinds, members, half), space_grads, space_kinds, half
    )
    return (
        result[:, None],
        input_grad[:, None],
        grad_space[0],
        grad_space[1],
        grad_time[0],
        grad_time[1],
        grad_ffn[0],
        grad_ffn[1],
        grad_space[2],
    )


def solution(mesh):
    dp_size, fsdp_size = mesh.devices.shape
    split = Mesh(mesh.devices.reshape(dp_size // 2, 2, fsdp_size), ("dpo", "core", "fsdp"))
    tokens = P(None, ("dpo", "core"), "fsdp", None, None)
    rows = P("fsdp", None)
    return jax.shard_map(
        layer,
        mesh=split,
        in_specs=(tokens, rows, rows, rows, rows, rows, rows, P(None, "fsdp"), tokens),
        out_specs=(tokens, tokens, rows, rows, rows, rows, rows, rows, P(None, "fsdp")),
        check_vma=False,
    )
```

```python
import jax
import jax.numpy as jnp
from jax import lax
from jax.sharding import Mesh
from jax.sharding import PartitionSpec as P


D = 768
HEADS = 12
HEAD_DIM = 64
GAIN_COLS = 128

EPS = 1e-06

MEMBERS = ("fsdp", "core")


def layer_norm(values, scales):
    average = jnp.mean(values, axis=-1, keepdims=True)
    centred = values - average
    spread = jnp.mean(centred * centred, axis=-1, keepdims=True)
    return centred * lax.rsqrt(spread + EPS) * scales


def norm_back(values, scales, incoming):
    _, pullback = jax.vjp(layer_norm, values, scales)
    return pullback(incoming)


def flat_dot(left, right):
    flat = left.reshape(-1, left.shape[-1])
    product = jnp.dot(flat, right, preferred_element_type=jnp.float32)
    return product.reshape(left.shape[:-1] + (right.shape[1],))


def back_dot(left, right):
    flat = left.reshape(-1, left.shape[-1])
    product = lax.dot_general(
        flat, right, (((1,), (1,)), ((), ())), preferred_element_type=jnp.float32
    )
    return product.reshape(left.shape[:-1] + (right.shape[0],))


def token_sum(left, right):
    left_rows = left.reshape(-1, left.shape[-1])
    right_rows = right.reshape(-1, right.shape[-1])
    return lax.dot_general(
        left_rows, right_rows, (((0,), (0,)), ((), ())), preferred_element_type=jnp.float32
    )


def split_join(joined):
    split_heads = joined.reshape(joined.shape[:-1] + (3, HEADS, HEAD_DIM))
    return (split_heads[..., 0, :, :], split_heads[..., 1, :, :], split_heads[..., 2, :, :])


def attend_core(normed, weight_in, token_form, key_form, score_form):
    joined = flat_dot(normed, weight_in).astype(jnp.bfloat16)
    queries, keyset, valueset = split_join(joined)
    factor = HEAD_DIM ** (-0.5)
    scores = (
        jnp.einsum(
            token_form + "hd," + key_form + "hd->" + score_form,
            queries,
            keyset,
            preferred_element_type=jnp.float32,
        )
        * factor
    )
    totals = jax.nn.logsumexp(scores, axis=-1, keepdims=True)
    weighting = jnp.exp(scores - totals).astype(jnp.bfloat16)
    context = jnp.einsum(
        score_form + "," + key_form + "hd->" + token_form + "hd",
        weighting,
        valueset,
        preferred_element_type=jnp.float32,
    )
    context = context.reshape(normed.shape[:-1] + (D,)).astype(jnp.bfloat16)
    return (joined, totals, context)


def attend_back(joined, totals, back_context, token_form, key_form, score_form):
    queries, keyset, valueset = split_join(joined)
    back_heads = back_context.reshape(back_context.shape[:-1] + (HEADS, HEAD_DIM))
    factor = HEAD_DIM ** (-0.5)
    scores = (
        jnp.einsum(
            token_form + "hd," + key_form + "hd->" + score_form,
            queries,
            keyset,
            preferred_element_type=jnp.float32,
        )
        * factor
    )
    weighting = jnp.exp(scores - totals)
    back_weight = jnp.einsum(
        token_form + "hd," + key_form + "hd->" + score_form,
        back_heads,
        valueset,
        preferred_element_type=jnp.float32,
    )
    back_weight = back_weight.astype(jnp.bfloat16).astype(jnp.float32)
    inner_sum = jnp.sum(weighting * back_weight, axis=-1, keepdims=True)
    back_scores = (weighting * (back_weight - inner_sum)).astype(jnp.bfloat16)
    back_query = (
        jnp.einsum(
            score_form + "," + key_form + "hd->" + token_form + "hd",
            back_scores,
            keyset,
            preferred_element_type=jnp.float32,
        )
        * factor
    )
    back_keys = (
        jnp.einsum(
            score_form + "," + token_form + "hd->" + key_form + "hd",
            back_scores,
            queries,
            preferred_element_type=jnp.float32,
        )
        * factor
    )
    back_values = jnp.einsum(
        score_form + "," + token_form + "hd->" + key_form + "hd",
        weighting.astype(jnp.bfloat16),
        back_heads,
        preferred_element_type=jnp.float32,
    )
    stacked = jnp.stack((back_query, back_keys, back_values), axis=-3)
    return stacked.reshape(back_context.shape[:-1] + (3 * D,)).astype(jnp.bfloat16)


def gelu(values):
    return 0.5 * values * (1.0 + lax.erf(values * (0.5 ** 0.5)))


def to_places(frames_major):
    peers = lax.axis_size("fsdp")
    frames, places, width = frames_major.shape
    blocks = frames_major.reshape(frames, peers, places // peers, width).transpose(1, 0, 2, 3)
    blocks = lax.all_to_all(blocks, "fsdp", split_axis=0, concat_axis=0, tiled=True)
    return blocks.reshape(peers * frames, places // peers, width)


def to_frames(places_major):
    peers = lax.axis_size("fsdp")
    all_frames, places, width = places_major.shape
    blocks = places_major.reshape(peers, all_frames // peers, places, width)
    blocks = lax.all_to_all(blocks, "fsdp", split_axis=0, concat_axis=0, tiled=True)
    return blocks.transpose(1, 0, 2, 3).reshape(all_frames // peers, peers * places, width)


def to_member(array, kind, part, half):
    if kind == "gains":
        gain_part = lax.dynamic_slice_in_dim(array, part * half, half, axis=1).T
        return jnp.pad(gain_part, ((0, 0), (0, GAIN_COLS - gain_part.shape[1])))
    if kind == "grouped":
        rows = lax.dynamic_slice_in_dim(array, part * 4 * half, 4 * half, axis=0)
        return jnp.concatenate([rows[q * half:(q + 1) * half] for q in range(4)], axis=1)
    return lax.dynamic_slice_in_dim(array, part * half, half, axis=0)


def width_of(array, kind):
    return {"gains": GAIN_COLS, "grouped": 4 * D}.get(kind, array.shape[-1])


def from_members(block, kinds, widths, half):
    members = block.shape[0] // half
    outs = []
    offset = 0
    for kind, width in zip(kinds, widths):
        part = block[:, offset:offset + width]
        offset += width
        if kind == "gains":
            outs.append(part[:, :3].T)
        elif kind == "grouped":
            grouped = part.reshape(members, half, 4 * D)
            outs.append(
                jnp.concatenate([grouped[:, :, q * D:(q + 1) * D] for q in range(4)], axis=1).reshape(
                    members * 4 * half, D
                )
            )
        else:
            outs.append(part)
    return outs


def to_members_full(array, kind, members, half):
    array = array.astype(jnp.bfloat16)
    if kind == "gains":
        cols = array.T
        return jnp.pad(cols, ((0, 0), (0, GAIN_COLS - cols.shape[1])))
    if kind == "grouped":
        grouped = array.reshape(members, 4 * half, D)
        return jnp.concatenate(
            [grouped[:, q * half:(q + 1) * half, :] for q in range(4)], axis=2
        ).reshape(members * half, 4 * D)
    return array


def gather_group(arrays, kinds, part, half):
    block = jnp.concatenate([to_member(a, k, part, half) for a, k in zip(arrays, kinds)], axis=1)
    widths = [width_of(a, k) for a, k in zip(arrays, kinds)]
    gathered = lax.all_gather(block, MEMBERS, axis=0, tiled=True)
    return from_members(gathered, kinds, widths, half)


def pair_sum(values, axis):
    if lax.axis_size(axis) == 2:
        return values + lax.ppermute(values, axis, [(0, 1), (1, 0)])
    return lax.psum(values, axis)


def core_gather(values):
    if lax.axis_size("core") == 2:
        other = lax.ppermute(values, "core", [(0, 1), (1, 0)])
        first = lax.axis_index("core") == 0
        return jnp.concatenate(
            [jnp.where(first, values, other), jnp.where(first, other, values)], axis=0
        )
    return lax.all_gather(values, "core", axis=0, tiled=True)


def pack_group(grads, kinds, members, half):
    return jnp.concatenate(
        [to_members_full(g, k, members, half) for g, k in zip(grads, kinds)], axis=1
    )


def reduce_group(packed, grads, kinds, half):
    widths = [width_of(g, k) for g, k in zip(grads, kinds)]
    owned = lax.psum_scatter(packed, MEMBERS, scatter_dimension=0, tiled=True)
    owned = core_gather(pair_sum(owned, "dpo"))
    return [part.astype(jnp.float32) for part in from_members(owned, kinds, widths, half)]


def layer(
    inputs, space_in, space_out, time_in, time_out, hidden_in, hidden_out, norm_gains, cotangent
):
    fsdp_size = lax.axis_size("fsdp")
    core_size = lax.axis_size("core")
    members = fsdp_size * core_size
    half = space_in.shape[0] // core_size
    core = lax.axis_index("core")

    s_in, s_out, gains = gather_group(
        (space_in, space_out, norm_gains), ("plain", "plain", "gains"), core, half
    )
    t_in, t_out = gather_group((time_in, time_out), ("plain", "plain"), core, half)
    h_in, h_out = gather_group((hidden_in, hidden_out), ("plain", "grouped"), core, half)
    gain_rows = gains.astype(jnp.float32)

    micro = inputs.shape[0]
    spatial = ("gl", "gm", "ghlm")
    temporal = ("lg", "mg", "ghlm")

    saved = []
    results = []
    for index in range(micro):
        frames_in = inputs[index, 0].astype(jnp.float32)
        normed_one = layer_norm(frames_in, gain_rows[0]).astype(jnp.bfloat16)
        join_space, total_space, context_space = attend_core(normed_one, s_in, *spatial)
        mixed_one = frames_in + flat_dot(context_space, s_out)
        normed_two = layer_norm(mixed_one, gain_rows[1]).astype(jnp.bfloat16)
        placed = to_places(normed_two)
        join_time, total_time, context_placed = attend_core(placed, t_in, *temporal)
        context_time = to_frames(context_placed)
        mixed_two = mixed_one + flat_dot(context_time, t_out)
        normed_three = layer_norm(mixed_two, gain_rows[2]).astype(jnp.bfloat16)
        hidden = flat_dot(normed_three, h_in)
        activated = gelu(hidden).astype(jnp.bfloat16)
        results.append(mixed_two + flat_dot(activated, h_out))
        saved.append(
            dict(
                frames_in=frames_in,
                normed_one=normed_one,
                join_space=join_space,
                total_space=total_space,
                context_space=context_space,
                mixed_one=mixed_one,
                placed=placed,
                join_time=join_time,
                total_time=total_time,
                context_time=context_time,
                mixed_two=mixed_two,
                normed_three=normed_three,
                hidden=hidden,
                activated=activated,
            )
        )

    def pooled(pairs):
        lefts = [left.reshape(-1, left.shape[-1]) for left, _ in pairs]
        rights = [right.reshape(-1, right.shape[-1]) for _, right in pairs]
        return token_sum(jnp.concatenate(lefts, axis=0), jnp.concatenate(rights, axis=0))

    def summed(terms):
        total = terms[0]
        for term in terms[1:]:
            total = total + term
        return total

    upstreams = []
    back_threes = []
    gain_two_terms = []
    hidden_out_terms = []
    hidden_in_terms = []
    for index in range(micro):
        s = saved[index]
        upstream = cotangent[index, 0].astype(jnp.float32)
        rounded = upstream.astype(jnp.bfloat16)
        hidden_out_terms.append((s["activated"], rounded))
        back_active = back_dot(rounded, h_out).astype(jnp.bfloat16)
        _, gelu_pull = jax.vjp(gelu, s["hidden"])
        back_hidden = gelu_pull(back_active.astype(jnp.float32))[0].astype(jnp.bfloat16)
        hidden_in_terms.append((s["normed_three"], back_hidden))
        back_threes.append(back_dot(back_hidden, h_in).astype(jnp.bfloat16))
        upstreams.append(upstream)
    ffn_grads = (pooled(hidden_in_terms), pooled(hidden_out_terms))
    ffn_kinds = ("plain", "grouped")
    packed_ffn, back_threes[-1] = lax.optimization_barrier(
        (pack_group(ffn_grads, ffn_kinds, members, half), back_threes[-1])
    )
    grad_ffn = reduce_group(packed_ffn, ffn_grads, ffn_kinds, half)

    back_twos_placed = []
    time_out_terms = []
    time_in_terms = []
    for index in range(micro):
        s = saved[index]
        back_mixed, gain_grad = norm_back(
            s["mixed_two"], gain_rows[2], back_threes[index].astype(jnp.float32)
        )
        gain_two_terms.append(gain_grad)
        upstream = upstreams[index] + back_mixed
        upstreams[index] = upstream
        rounded = upstream.astype(jnp.bfloat16)
        time_out_terms.append((s["context_time"], rounded))
        back_context = back_dot(rounded, t_out).astype(jnp.bfloat16)
        back_placed = to_places(back_context)
        back_join = attend_back(s["join_time"], s["total_time"], back_placed, *temporal)
        time_in_terms.append((s["placed"], back_join))
        back_twos_placed.append(back_dot(back_join, t_in).astype(jnp.bfloat16))
    time_grads = (pooled(time_in_terms), pooled(time_out_terms))
    time_kinds = ("plain", "plain")
    packed_time, back_twos_placed[-1] = lax.optimization_barrier(
        (pack_group(time_grads, time_kinds, members, half), back_twos_placed[-1])
    )
    grad_time = reduce_group(packed_time, time_grads, time_kinds, half)

    input_grads = []
    gain_one_terms = []
    gain_zero_terms = []
    space_out_terms = []
    space_in_terms = []
    for index in range(micro):
        s = saved[index]
        back_two = to_frames(back_twos_placed[index])
        back_mixed, gain_grad = norm_back(s["mixed_one"], gain_rows[1], back_two.astype(jnp.float32))
        gain_one_terms.append(gain_grad)
        upstream = upstreams[index] + back_mixed
        rounded = upstream.astype(jnp.bfloat16)
        space_out_terms.append((s["context_space"], rounded))
        back_context = back_dot(rounded, s_out).astype(jnp.bfloat16)
        back_join = attend_back(s["join_space"], s["total_space"], back_context, *spatial)
        space_in_terms.append((s["normed_one"], back_join))
        back_one = back_dot(back_join, s_in).astype(jnp.bfloat16)
        back_mixed, gain_grad = norm_back(
            s["frames_in"], gain_rows[0], back_one.astype(jnp.float32)
        )
        gain_zero_terms.append(gain_grad)
        input_grads.append(upstream + back_mixed)
    grad_space_in = pooled(space_in_terms)
    grad_space_out = pooled(space_out_terms)
    gain_grad_zero = summed(gain_zero_terms)
    gain_grad_one = summed(gain_one_terms)
    gain_grad_two = summed(gain_two_terms)
    result = jnp.stack(results)
    input_grad = jnp.stack(input_grads)

    gain_grads = jnp.stack((gain_grad_zero, gain_grad_one, gain_grad_two))
    space_grads = (grad_space_in, grad_space_out, gain_grads)
    space_kinds = ("plain", "plain", "gains")
    grad_space = reduce_group(
        pack_group(space_grads, space_kinds, members, half), space_grads, space_kinds, half
    )
    return (
        result[:, None],
        input_grad[:, None],
        grad_space[0],
        grad_space[1],
        grad_time[0],
        grad_time[1],
        grad_ffn[0],
        grad_ffn[1],
        grad_space[2],
    )


def solution(mesh):
    dp_size, fsdp_size = mesh.devices.shape
    split = Mesh(mesh.devices.reshape(dp_size // 2, 2, fsdp_size), ("dpo", "core", "fsdp"))
    tokens = P(None, ("dpo", "core"), "fsdp", None, None)
    rows = P("fsdp", None)
    return jax.shard_map(
        layer,
        mesh=split,
        in_specs=(tokens, rows, rows, rows, rows, rows, rows, P(None, "fsdp"), tokens),
        out_specs=(tokens, tokens, rows, rows, rows, rows, rows, rows, P(None, "fsdp")),
        check_vma=False,
    )
```

```python
import jax
import jax.numpy as jnp
from jax import lax
from jax.sharding import Mesh
from jax.sharding import PartitionSpec as P


D = 768
HEADS = 12
HEAD_DIM = 64
GAIN_COLS = 128

EPS = 1e-06

MEMBERS = ("fsdp", "core")


def layer_norm(values, scales):
    average = jnp.mean(values, axis=-1, keepdims=True)
    centred = values - average
    spread = jnp.mean(centred * centred, axis=-1, keepdims=True)
    return centred * lax.rsqrt(spread + EPS) * scales


def norm_back(values, scales, incoming):
    _, pullback = jax.vjp(layer_norm, values, scales)
    return pullback(incoming)


def flat_dot(left, right):
    flat = left.reshape(-1, left.shape[-1])
    product = jnp.dot(flat, right, preferred_element_type=jnp.float32)
    return product.reshape(left.shape[:-1] + (right.shape[1],))


def back_dot(left, right):
    flat = left.reshape(-1, left.shape[-1])
    product = lax.dot_general(
        flat, right, (((1,), (1,)), ((), ())), preferred_element_type=jnp.float32
    )
    return product.reshape(left.shape[:-1] + (right.shape[0],))


def token_sum(left, right):
    left_rows = left.reshape(-1, left.shape[-1])
    right_rows = right.reshape(-1, right.shape[-1])
    return lax.dot_general(
        left_rows, right_rows, (((0,), (0,)), ((), ())), preferred_element_type=jnp.float32
    )


def split_join(joined):
    split_heads = joined.reshape(joined.shape[:-1] + (3, HEADS, HEAD_DIM))
    return (split_heads[..., 0, :, :], split_heads[..., 1, :, :], split_heads[..., 2, :, :])


def attend_core(normed, weight_in, token_form, key_form, score_form):
    joined = flat_dot(normed, weight_in).astype(jnp.bfloat16)
    queries, keyset, valueset = split_join(joined)
    factor = HEAD_DIM ** (-0.5)
    scores = (
        jnp.einsum(
            token_form + "hd," + key_form + "hd->" + score_form,
            queries,
            keyset,
            preferred_element_type=jnp.float32,
        )
        * factor
    )
    totals = jax.nn.logsumexp(scores, axis=-1, keepdims=True)
    weighting = jnp.exp(scores - totals).astype(jnp.bfloat16)
    context = jnp.einsum(
        score_form + "," + key_form + "hd->" + token_form + "hd",
        weighting,
        valueset,
        preferred_element_type=jnp.float32,
    )
    context = context.reshape(normed.shape[:-1] + (D,)).astype(jnp.bfloat16)
    return (joined, totals, context)


def attend_back(joined, totals, back_context, token_form, key_form, score_form):
    queries, keyset, valueset = split_join(joined)
    back_heads = back_context.reshape(back_context.shape[:-1] + (HEADS, HEAD_DIM))
    factor = HEAD_DIM ** (-0.5)
    scores = (
        jnp.einsum(
            token_form + "hd," + key_form + "hd->" + score_form,
            queries,
            keyset,
            preferred_element_type=jnp.float32,
        )
        * factor
    )
    weighting = jnp.exp(scores - totals)
    back_weight = jnp.einsum(
        token_form + "hd," + key_form + "hd->" + score_form,
        back_heads,
        valueset,
        preferred_element_type=jnp.float32,
    )
    back_weight = back_weight.astype(jnp.bfloat16).astype(jnp.float32)
    inner_sum = jnp.sum(weighting * back_weight, axis=-1, keepdims=True)
    back_scores = (weighting * (back_weight - inner_sum)).astype(jnp.bfloat16)
    back_query = (
        jnp.einsum(
            score_form + "," + key_form + "hd->" + token_form + "hd",
            back_scores,
            keyset,
            preferred_element_type=jnp.float32,
        )
        * factor
    )
    back_keys = (
        jnp.einsum(
            score_form + "," + token_form + "hd->" + key_form + "hd",
            back_scores,
            queries,
            preferred_element_type=jnp.float32,
        )
        * factor
    )
    back_values = jnp.einsum(
        score_form + "," + token_form + "hd->" + key_form + "hd",
        weighting.astype(jnp.bfloat16),
        back_heads,
        preferred_element_type=jnp.float32,
    )
    stacked = jnp.stack((back_query, back_keys, back_values), axis=-3)
    return stacked.reshape(back_context.shape[:-1] + (3 * D,)).astype(jnp.bfloat16)


def gelu(values):
    return 0.5 * values * (1.0 + lax.erf(values * (0.5 ** 0.5)))


def to_places(frames_major):
    peers = lax.axis_size("fsdp")
    frames, places, width = frames_major.shape
    blocks = frames_major.reshape(frames, peers, places // peers, width).transpose(1, 0, 2, 3)
    blocks = lax.all_to_all(blocks, "fsdp", split_axis=0, concat_axis=0, tiled=True)
    return blocks.reshape(peers * frames, places // peers, width)


def to_frames(places_major):
    peers = lax.axis_size("fsdp")
    all_frames, places, width = places_major.shape
    blocks = places_major.reshape(peers, all_frames // peers, places, width)
    blocks = lax.all_to_all(blocks, "fsdp", split_axis=0, concat_axis=0, tiled=True)
    return blocks.transpose(1, 0, 2, 3).reshape(all_frames // peers, peers * places, width)


def to_member(array, kind, part, half):
    if kind == "gains":
        gain_part = lax.dynamic_slice_in_dim(array, part * half, half, axis=1).T
        return jnp.pad(gain_part, ((0, 0), (0, GAIN_COLS - gain_part.shape[1])))
    if kind == "grouped":
        rows = lax.dynamic_slice_in_dim(array, part * 4 * half, 4 * half, axis=0)
        return jnp.concatenate([rows[q * half:(q + 1) * half] for q in range(4)], axis=1)
    return lax.dynamic_slice_in_dim(array, part * half, half, axis=0)


def width_of(array, kind):
    return {"gains": GAIN_COLS, "grouped": 4 * D}.get(kind, array.shape[-1])


def from_members(block, kinds, widths, half):
    members = block.shape[0] // half
    outs = []
    offset = 0
    for kind, width in zip(kinds, widths):
        part = block[:, offset:offset + width]
        offset += width
        if kind == "gains":
            outs.append(part[:, :3].T)
        elif kind == "grouped":
            grouped = part.reshape(members, half, 4 * D)
            outs.append(
                jnp.concatenate([grouped[:, :, q * D:(q + 1) * D] for q in range(4)], axis=1).reshape(
                    members * 4 * half, D
                )
            )
        else:
            outs.append(part)
    return outs


def to_members_full(array, kind, members, half):
    array = array.astype(jnp.bfloat16)
    if kind == "gains":
        cols = array.T
        return jnp.pad(cols, ((0, 0), (0, GAIN_COLS - cols.shape[1])))
    if kind == "grouped":
        grouped = array.reshape(members, 4 * half, D)
        return jnp.concatenate(
            [grouped[:, q * half:(q + 1) * half, :] for q in range(4)], axis=2
        ).reshape(members * half, 4 * D)
    return array


def gather_group(arrays, kinds, part, half):
    block = jnp.concatenate([to_member(a, k, part, half) for a, k in zip(arrays, kinds)], axis=1)
    widths = [width_of(a, k) for a, k in zip(arrays, kinds)]
    gathered = lax.all_gather(block, MEMBERS, axis=0, tiled=True)
    return from_members(gathered, kinds, widths, half)


def pair_sum(values, axis):
    if lax.axis_size(axis) == 2:
        return values + lax.ppermute(values, axis, [(0, 1), (1, 0)])
    return lax.psum(values, axis)


def core_gather(values):
    if lax.axis_size("core") == 2:
        other = lax.ppermute(values, "core", [(0, 1), (1, 0)])
        first = lax.axis_index("core") == 0
        return jnp.concatenate(
            [jnp.where(first, values, other), jnp.where(first, other, values)], axis=0
        )
    return lax.all_gather(values, "core", axis=0, tiled=True)


def pack_group(grads, kinds, members, half):
    return jnp.concatenate(
        [to_members_full(g, k, members, half) for g, k in zip(grads, kinds)], axis=1
    )


def reduce_group(packed, grads, kinds, half):
    widths = [width_of(g, k) for g, k in zip(grads, kinds)]
    owned = lax.psum_scatter(packed, MEMBERS, scatter_dimension=0, tiled=True)
    owned = core_gather(pair_sum(owned, "dpo"))
    return [part.astype(jnp.float32) for part in from_members(owned, kinds, widths, half)]


def layer(
    inputs, space_in, space_out, time_in, time_out, hidden_in, hidden_out, norm_gains, cotangent
):
    fsdp_size = lax.axis_size("fsdp")
    core_size = lax.axis_size("core")
    members = fsdp_size * core_size
    half = space_in.shape[0] // core_size
    core = lax.axis_index("core")

    s_in, s_out, gains = gather_group(
        (space_in, space_out, norm_gains), ("plain", "plain", "gains"), core, half
    )
    t_in, t_out = gather_group((time_in, time_out), ("plain", "plain"), core, half)
    h_in, h_out = gather_group((hidden_in, hidden_out), ("plain", "grouped"), core, half)
    gain_rows = gains.astype(jnp.float32)

    micro = inputs.shape[0]
    spatial = ("gl", "gm", "ghlm")
    temporal = ("lg", "mg", "ghlm")

    saved = []
    results = []
    for index in range(micro):
        frames_in = inputs[index, 0].astype(jnp.float32)
        normed_one = layer_norm(frames_in, gain_rows[0]).astype(jnp.bfloat16)
        join_space, total_space, context_space = attend_core(normed_one, s_in, *spatial)
        mixed_one = frames_in + flat_dot(context_space, s_out)
        normed_two = layer_norm(mixed_one, gain_rows[1]).astype(jnp.bfloat16)
        placed = to_places(normed_two)
        join_time, total_time, context_placed = attend_core(placed, t_in, *temporal)
        context_time = to_frames(context_placed)
        mixed_two = mixed_one + flat_dot(context_time, t_out)
        normed_three = layer_norm(mixed_two, gain_rows[2]).astype(jnp.bfloat16)
        hidden = flat_dot(normed_three, h_in)
        activated = gelu(hidden).astype(jnp.bfloat16)
        results.append(mixed_two + flat_dot(activated, h_out))
        saved.append(
            dict(
                frames_in=frames_in,
                normed_one=normed_one,
                join_space=join_space,
                total_space=total_space,
                context_space=context_space,
                mixed_one=mixed_one,
                placed=placed,
                join_time=join_time,
                total_time=total_time,
                context_time=context_time,
                mixed_two=mixed_two,
                normed_three=normed_three,
                hidden=hidden,
                activated=activated,
            )
        )

    def summed(terms):
        total = terms[0]
        for term in terms[1:]:
            total = total + term
        return total

    upstreams = []
    back_threes = []
    gain_two_terms = []
    hidden_out_terms = []
    hidden_in_terms = []
    for index in range(micro):
        s = saved[index]
        upstream = cotangent[index, 0].astype(jnp.float32)
        rounded = upstream.astype(jnp.bfloat16)
        hidden_out_terms.append(token_sum(s["activated"], rounded))
        back_active = back_dot(rounded, h_out).astype(jnp.bfloat16)
        _, gelu_pull = jax.vjp(gelu, s["hidden"])
        back_hidden = gelu_pull(back_active.astype(jnp.float32))[0].astype(jnp.bfloat16)
        hidden_in_terms.append(token_sum(s["normed_three"], back_hidden))
        back_threes.append(back_dot(back_hidden, h_in).astype(jnp.bfloat16))
        upstreams.append(upstream)
    ffn_grads = (summed(hidden_in_terms), summed(hidden_out_terms))
    ffn_kinds = ("plain", "grouped")
    packed_ffn, back_threes[0] = lax.optimization_barrier(
        (pack_group(ffn_grads, ffn_kinds, members, half), back_threes[0])
    )
    grad_ffn = reduce_group(packed_ffn, ffn_grads, ffn_kinds, half)

    back_twos_placed = []
    time_out_terms = []
    time_in_terms = []
    for index in range(micro):
        s = saved[index]
        back_mixed, gain_grad = norm_back(
            s["mixed_two"], gain_rows[2], back_threes[index].astype(jnp.float32)
        )
        gain_two_terms.append(gain_grad)
        upstream = upstreams[index] + back_mixed
        upstreams[index] = upstream
        rounded = upstream.astype(jnp.bfloat16)
        time_out_terms.append(token_sum(s["context_time"], rounded))
        back_context = back_dot(rounded, t_out).astype(jnp.bfloat16)
        back_placed = to_places(back_context)
        back_join = attend_back(s["join_time"], s["total_time"], back_placed, *temporal)
        time_in_terms.append(token_sum(s["placed"], back_join))
        back_twos_placed.append(back_dot(back_join, t_in).astype(jnp.bfloat16))
    time_grads = (summed(time_in_terms), summed(time_out_terms))
    time_kinds = ("plain", "plain")
    packed_time, back_twos_placed[-1] = lax.optimization_barrier(
        (pack_group(time_grads, time_kinds, members, half), back_twos_placed[-1])
    )
    grad_time = reduce_group(packed_time, time_grads, time_kinds, half)

    input_grads = []
    gain_one_terms = []
    gain_zero_terms = []
    space_out_terms = []
    space_in_terms = []
    for index in range(micro):
        s = saved[index]
        back_two = to_frames(back_twos_placed[index])
        back_mixed, gain_grad = norm_back(s["mixed_one"], gain_rows[1], back_two.astype(jnp.float32))
        gain_one_terms.append(gain_grad)
        upstream = upstreams[index] + back_mixed
        rounded = upstream.astype(jnp.bfloat16)
        space_out_terms.append(token_sum(s["context_space"], rounded))
        back_context = back_dot(rounded, s_out).astype(jnp.bfloat16)
        back_join = attend_back(s["join_space"], s["total_space"], back_context, *spatial)
        space_in_terms.append(token_sum(s["normed_one"], back_join))
        back_one = back_dot(back_join, s_in).astype(jnp.bfloat16)
        back_mixed, gain_grad = norm_back(
            s["frames_in"], gain_rows[0], back_one.astype(jnp.float32)
        )
        gain_zero_terms.append(gain_grad)
        input_grads.append(upstream + back_mixed)
    grad_space_in = summed(space_in_terms)
    grad_space_out = summed(space_out_terms)
    gain_grad_zero = summed(gain_zero_terms)
    gain_grad_one = summed(gain_one_terms)
    gain_grad_two = summed(gain_two_terms)
    result = jnp.stack(results)
    input_grad = jnp.stack(input_grads)

    gain_grads = jnp.stack((gain_grad_zero, gain_grad_one, gain_grad_two))
    space_grads = (grad_space_in, grad_space_out, gain_grads)
    space_kinds = ("plain", "plain", "gains")
    grad_space = reduce_group(
        pack_group(space_grads, space_kinds, members, half), space_grads, space_kinds, half
    )
    return (
        result[:, None],
        input_grad[:, None],
        grad_space[0],
        grad_space[1],
        grad_time[0],
        grad_time[1],
        grad_ffn[0],
        grad_ffn[1],
        grad_space[2],
    )


def solution(mesh):
    dp_size, fsdp_size = mesh.devices.shape
    split = Mesh(mesh.devices.reshape(dp_size // 2, 2, fsdp_size), ("dpo", "core", "fsdp"))
    tokens = P(None, ("dpo", "core"), "fsdp", None, None)
    rows = P("fsdp", None)
    return jax.shard_map(
        layer,
        mesh=split,
        in_specs=(tokens, rows, rows, rows, rows, rows, rows, P(None, "fsdp"), tokens),
        out_specs=(tokens, tokens, rows, rows, rows, rows, rows, rows, P(None, "fsdp")),
        check_vma=False,
    )
```

```python
import jax
import jax.numpy as jnp
from jax import lax
from jax.sharding import Mesh
from jax.sharding import PartitionSpec as P


D = 768
HEADS = 12
HEAD_DIM = 64
GAIN_COLS = 128

EPS = 1e-06

MEMBERS = ("fsdp", "core")


def layer_norm(values, scales):
    average = jnp.mean(values, axis=-1, keepdims=True)
    centred = values - average
    spread = jnp.mean(centred * centred, axis=-1, keepdims=True)
    return centred * lax.rsqrt(spread + EPS) * scales


def norm_back(values, scales, incoming):
    _, pullback = jax.vjp(layer_norm, values, scales)
    return pullback(incoming)


def flat_dot(left, right):
    flat = left.reshape(-1, left.shape[-1])
    product = jnp.dot(flat, right, preferred_element_type=jnp.float32)
    return product.reshape(left.shape[:-1] + (right.shape[1],))


def back_dot(left, right):
    flat = left.reshape(-1, left.shape[-1])
    product = lax.dot_general(
        flat, right, (((1,), (1,)), ((), ())), preferred_element_type=jnp.float32
    )
    return product.reshape(left.shape[:-1] + (right.shape[0],))


def token_sum(left, right):
    left_rows = left.reshape(-1, left.shape[-1])
    right_rows = right.reshape(-1, right.shape[-1])
    return lax.dot_general(
        left_rows, right_rows, (((0,), (0,)), ((), ())), preferred_element_type=jnp.float32
    )


def split_join(joined):
    split_heads = joined.reshape(joined.shape[:-1] + (3, HEADS, HEAD_DIM))
    return (split_heads[..., 0, :, :], split_heads[..., 1, :, :], split_heads[..., 2, :, :])


def attend_core(normed, weight_in, token_form, key_form, score_form):
    joined = flat_dot(normed, weight_in).astype(jnp.bfloat16)
    queries, keyset, valueset = split_join(joined)
    factor = HEAD_DIM ** (-0.5)
    scores = (
        jnp.einsum(
            token_form + "hd," + key_form + "hd->" + score_form,
            queries,
            keyset,
            preferred_element_type=jnp.float32,
        )
        * factor
    )
    totals = jax.nn.logsumexp(scores, axis=-1, keepdims=True)
    weighting = jnp.exp(scores - totals).astype(jnp.bfloat16)
    context = jnp.einsum(
        score_form + "," + key_form + "hd->" + token_form + "hd",
        weighting,
        valueset,
        preferred_element_type=jnp.float32,
    )
    context = context.reshape(normed.shape[:-1] + (D,)).astype(jnp.bfloat16)
    return (joined, totals, context)


def attend_back(joined, totals, back_context, token_form, key_form, score_form):
    queries, keyset, valueset = split_join(joined)
    back_heads = back_context.reshape(back_context.shape[:-1] + (HEADS, HEAD_DIM))
    factor = HEAD_DIM ** (-0.5)
    scores = (
        jnp.einsum(
            token_form + "hd," + key_form + "hd->" + score_form,
            queries,
            keyset,
            preferred_element_type=jnp.float32,
        )
        * factor
    )
    weighting = jnp.exp(scores - totals)
    back_weight = jnp.einsum(
        token_form + "hd," + key_form + "hd->" + score_form,
        back_heads,
        valueset,
        preferred_element_type=jnp.float32,
    )
    back_weight = back_weight.astype(jnp.bfloat16).astype(jnp.float32)
    inner_sum = jnp.sum(weighting * back_weight, axis=-1, keepdims=True)
    back_scores = (weighting * (back_weight - inner_sum)).astype(jnp.bfloat16)
    back_query = (
        jnp.einsum(
            score_form + "," + key_form + "hd->" + token_form + "hd",
            back_scores,
            keyset,
            preferred_element_type=jnp.float32,
        )
        * factor
    )
    back_keys = (
        jnp.einsum(
            score_form + "," + token_form + "hd->" + key_form + "hd",
            back_scores,
            queries,
            preferred_element_type=jnp.float32,
        )
        * factor
    )
    back_values = jnp.einsum(
        score_form + "," + token_form + "hd->" + key_form + "hd",
        weighting.astype(jnp.bfloat16),
        back_heads,
        preferred_element_type=jnp.float32,
    )
    stacked = jnp.stack((back_query, back_keys, back_values), axis=-3)
    return stacked.reshape(back_context.shape[:-1] + (3 * D,)).astype(jnp.bfloat16)


def gelu(values):
    return 0.5 * values * (1.0 + lax.erf(values * (0.5 ** 0.5)))


def to_places(frames_major):
    peers = lax.axis_size("fsdp")
    frames, places, width = frames_major.shape
    blocks = frames_major.reshape(frames, peers, places // peers, width).transpose(1, 0, 2, 3)
    blocks = lax.all_to_all(blocks, "fsdp", split_axis=0, concat_axis=0, tiled=True)
    return blocks.reshape(peers * frames, places // peers, width)


def to_frames(places_major):
    peers = lax.axis_size("fsdp")
    all_frames, places, width = places_major.shape
    blocks = places_major.reshape(peers, all_frames // peers, places, width)
    blocks = lax.all_to_all(blocks, "fsdp", split_axis=0, concat_axis=0, tiled=True)
    return blocks.transpose(1, 0, 2, 3).reshape(all_frames // peers, peers * places, width)


def to_member(array, kind, part, half):
    if kind == "gains":
        gain_part = lax.dynamic_slice_in_dim(array, part * half, half, axis=1).T
        return jnp.pad(gain_part, ((0, 0), (0, GAIN_COLS - gain_part.shape[1])))
    if kind == "grouped":
        rows = lax.dynamic_slice_in_dim(array, part * 4 * half, 4 * half, axis=0)
        return jnp.concatenate([rows[q * half:(q + 1) * half] for q in range(4)], axis=1)
    return lax.dynamic_slice_in_dim(array, part * half, half, axis=0)


def width_of(array, kind):
    return {"gains": GAIN_COLS, "grouped": 4 * D}.get(kind, array.shape[-1])


def from_members(block, kinds, widths, half):
    members = block.shape[0] // half
    outs = []
    offset = 0
    for kind, width in zip(kinds, widths):
        part = block[:, offset:offset + width]
        offset += width
        if kind == "gains":
            outs.append(part[:, :3].T)
        elif kind == "grouped":
            grouped = part.reshape(members, half, 4 * D)
            outs.append(
                jnp.concatenate([grouped[:, :, q * D:(q + 1) * D] for q in range(4)], axis=1).reshape(
                    members * 4 * half, D
                )
            )
        else:
            outs.append(part)
    return outs


def to_members_full(array, kind, members, half):
    array = array.astype(jnp.bfloat16)
    if kind == "gains":
        cols = array.T
        return jnp.pad(cols, ((0, 0), (0, GAIN_COLS - cols.shape[1])))
    if kind == "grouped":
        grouped = array.reshape(members, 4 * half, D)
        return jnp.concatenate(
            [grouped[:, q * half:(q + 1) * half, :] for q in range(4)], axis=2
        ).reshape(members * half, 4 * D)
    return array


def gather_group(arrays, kinds, part, half):
    block = jnp.concatenate([to_member(a, k, part, half) for a, k in zip(arrays, kinds)], axis=1)
    widths = [width_of(a, k) for a, k in zip(arrays, kinds)]
    gathered = lax.all_gather(block, MEMBERS, axis=0, tiled=True)
    return from_members(gathered, kinds, widths, half)


def pair_sum(values, axis):
    if lax.axis_size(axis) == 2:
        return values + lax.ppermute(values, axis, [(0, 1), (1, 0)])
    return lax.psum(values, axis)


def core_gather(values):
    if lax.axis_size("core") == 2:
        other = lax.ppermute(values, "core", [(0, 1), (1, 0)])
        first = lax.axis_index("core") == 0
        return jnp.concatenate(
            [jnp.where(first, values, other), jnp.where(first, other, values)], axis=0
        )
    return lax.all_gather(values, "core", axis=0, tiled=True)


def pack_group(grads, kinds, members, half):
    return jnp.concatenate(
        [to_members_full(g, k, members, half) for g, k in zip(grads, kinds)], axis=1
    )


def reduce_group(packed, grads, kinds, half):
    widths = [width_of(g, k) for g, k in zip(grads, kinds)]
    owned = lax.psum_scatter(packed, MEMBERS, scatter_dimension=0, tiled=True)
    owned = core_gather(pair_sum(owned, "dpo"))
    return [part.astype(jnp.float32) for part in from_members(owned, kinds, widths, half)]


def layer(
    inputs, space_in, space_out, time_in, time_out, hidden_in, hidden_out, norm_gains, cotangent
):
    fsdp_size = lax.axis_size("fsdp")
    core_size = lax.axis_size("core")
    members = fsdp_size * core_size
    half = space_in.shape[0] // core_size
    core = lax.axis_index("core")

    s_in, s_out, gains = gather_group(
        (space_in, space_out, norm_gains), ("plain", "plain", "gains"), core, half
    )
    t_in, t_out, h_in, h_out = gather_group(
        (time_in, time_out, hidden_in, hidden_out),
        ("plain", "plain", "plain", "grouped"),
        core,
        half,
    )
    gain_rows = gains.astype(jnp.float32)

    micro = inputs.shape[0]
    spatial = ("gl", "gm", "ghlm")
    temporal = ("lg", "mg", "ghlm")

    saved = []
    results = []
    for index in range(micro):
        frames_in = inputs[index, 0].astype(jnp.float32)
        normed_one = layer_norm(frames_in, gain_rows[0]).astype(jnp.bfloat16)
        join_space, total_space, context_space = attend_core(normed_one, s_in, *spatial)
        mixed_one = frames_in + flat_dot(context_space, s_out)
        normed_two = layer_norm(mixed_one, gain_rows[1]).astype(jnp.bfloat16)
        placed = to_places(normed_two)
        join_time, total_time, context_placed = attend_core(placed, t_in, *temporal)
        context_time = to_frames(context_placed)
        mixed_two = mixed_one + flat_dot(context_time, t_out)
        normed_three = layer_norm(mixed_two, gain_rows[2]).astype(jnp.bfloat16)
        hidden = flat_dot(normed_three, h_in)
        activated = gelu(hidden).astype(jnp.bfloat16)
        results.append(mixed_two + flat_dot(activated, h_out))
        saved.append(
            dict(
                frames_in=frames_in,
                normed_one=normed_one,
                join_space=join_space,
                total_space=total_space,
                context_space=context_space,
                mixed_one=mixed_one,
                placed=placed,
                join_time=join_time,
                total_time=total_time,
                context_time=context_time,
                mixed_two=mixed_two,
                normed_three=normed_three,
                hidden=hidden,
                activated=activated,
            )
        )

    def summed(terms):
        total = terms[0]
        for term in terms[1:]:
            total = total + term
        return total

    upstreams = []
    back_threes = []
    gain_two_terms = []
    hidden_out_terms = []
    hidden_in_terms = []
    for index in range(micro):
        s = saved[index]
        upstream = cotangent[index, 0].astype(jnp.float32)
        rounded = upstream.astype(jnp.bfloat16)
        hidden_out_terms.append(token_sum(s["activated"], rounded))
        back_active = back_dot(rounded, h_out).astype(jnp.bfloat16)
        _, gelu_pull = jax.vjp(gelu, s["hidden"])
        back_hidden = gelu_pull(back_active.astype(jnp.float32))[0].astype(jnp.bfloat16)
        hidden_in_terms.append(token_sum(s["normed_three"], back_hidden))
        back_threes.append(back_dot(back_hidden, h_in).astype(jnp.bfloat16))
        upstreams.append(upstream)
    ffn_grads = (summed(hidden_in_terms), summed(hidden_out_terms))
    ffn_kinds = ("plain", "grouped")
    packed_ffn, back_threes[-1] = lax.optimization_barrier(
        (pack_group(ffn_grads, ffn_kinds, members, half), back_threes[-1])
    )
    grad_ffn = reduce_group(packed_ffn, ffn_grads, ffn_kinds, half)

    back_twos_placed = []
    time_out_terms = []
    time_in_terms = []
    for index in range(micro):
        s = saved[index]
        back_mixed, gain_grad = norm_back(
            s["mixed_two"], gain_rows[2], back_threes[index].astype(jnp.float32)
        )
        gain_two_terms.append(gain_grad)
        upstream = upstreams[index] + back_mixed
        upstreams[index] = upstream
        rounded = upstream.astype(jnp.bfloat16)
        time_out_terms.append(token_sum(s["context_time"], rounded))
        back_context = back_dot(rounded, t_out).astype(jnp.bfloat16)
        back_placed = to_places(back_context)
        back_join = attend_back(s["join_time"], s["total_time"], back_placed, *temporal)
        time_in_terms.append(token_sum(s["placed"], back_join))
        back_twos_placed.append(back_dot(back_join, t_in).astype(jnp.bfloat16))
    time_grads = (summed(time_in_terms), summed(time_out_terms))
    time_kinds = ("plain", "plain")
    packed_time, back_twos_placed[-1] = lax.optimization_barrier(
        (pack_group(time_grads, time_kinds, members, half), back_twos_placed[-1])
    )
    grad_time = reduce_group(packed_time, time_grads, time_kinds, half)

    input_grads = []
    gain_one_terms = []
    gain_zero_terms = []
    space_out_terms = []
    space_in_terms = []
    for index in range(micro):
        s = saved[index]
        back_two = to_frames(back_twos_placed[index])
        back_mixed, gain_grad = norm_back(s["mixed_one"], gain_rows[1], back_two.astype(jnp.float32))
        gain_one_terms.append(gain_grad)
        upstream = upstreams[index] + back_mixed
        rounded = upstream.astype(jnp.bfloat16)
        space_out_terms.append(token_sum(s["context_space"], rounded))
        back_context = back_dot(rounded, s_out).astype(jnp.bfloat16)
        back_join = attend_back(s["join_space"], s["total_space"], back_context, *spatial)
        space_in_terms.append(token_sum(s["normed_one"], back_join))
        back_one = back_dot(back_join, s_in).astype(jnp.bfloat16)
        back_mixed, gain_grad = norm_back(
            s["frames_in"], gain_rows[0], back_one.astype(jnp.float32)
        )
        gain_zero_terms.append(gain_grad)
        input_grads.append(upstream + back_mixed)
    grad_space_in = summed(space_in_terms)
    grad_space_out = summed(space_out_terms)
    gain_grad_zero = summed(gain_zero_terms)
    gain_grad_one = summed(gain_one_terms)
    gain_grad_two = summed(gain_two_terms)
    result = jnp.stack(results)
    input_grad = jnp.stack(input_grads)

    gain_grads = jnp.stack((gain_grad_zero, gain_grad_one, gain_grad_two))
    space_grads = (grad_space_in, grad_space_out, gain_grads)
    space_kinds = ("plain", "plain", "gains")
    grad_space = reduce_group(
        pack_group(space_grads, space_kinds, members, half), space_grads, space_kinds, half
    )
    return (
        result[:, None],
        input_grad[:, None],
        grad_space[0],
        grad_space[1],
        grad_time[0],
        grad_time[1],
        grad_ffn[0],
        grad_ffn[1],
        grad_space[2],
    )


def solution(mesh):
    dp_size, fsdp_size = mesh.devices.shape
    split = Mesh(mesh.devices.reshape(dp_size // 2, 2, fsdp_size), ("dpo", "core", "fsdp"))
    tokens = P(None, ("dpo", "core"), "fsdp", None, None)
    rows = P("fsdp", None)
    return jax.shard_map(
        layer,
        mesh=split,
        in_specs=(tokens, rows, rows, rows, rows, rows, rows, P(None, "fsdp"), tokens),
        out_specs=(tokens, tokens, rows, rows, rows, rows, rows, rows, P(None, "fsdp")),
        check_vma=False,
    )
```

```python
import jax
import jax.numpy as jnp
from jax import lax
from jax.sharding import Mesh
from jax.sharding import PartitionSpec as P


D = 768
HEADS = 12
HEAD_DIM = 64
GAIN_COLS = 128

EPS = 1e-06

MEMBERS = ("fsdp", "core")


def layer_norm(values, scales):
    average = jnp.mean(values, axis=-1, keepdims=True)
    centred = values - average
    spread = jnp.mean(centred * centred, axis=-1, keepdims=True)
    return centred * lax.rsqrt(spread + EPS) * scales


def norm_back(values, scales, incoming):
    _, pullback = jax.vjp(layer_norm, values, scales)
    return pullback(incoming)


def flat_dot(left, right):
    flat = left.reshape(-1, left.shape[-1])
    product = jnp.dot(flat, right, preferred_element_type=jnp.float32)
    return product.reshape(left.shape[:-1] + (right.shape[1],))


def back_dot(left, right):
    flat = left.reshape(-1, left.shape[-1])
    product = lax.dot_general(
        flat, right, (((1,), (1,)), ((), ())), preferred_element_type=jnp.float32
    )
    return product.reshape(left.shape[:-1] + (right.shape[0],))


def token_sum(left, right):
    left_rows = left.reshape(-1, left.shape[-1])
    right_rows = right.reshape(-1, right.shape[-1])
    return lax.dot_general(
        left_rows, right_rows, (((0,), (0,)), ((), ())), preferred_element_type=jnp.float32
    )


def split_join(joined):
    split_heads = joined.reshape(joined.shape[:-1] + (3, HEADS, HEAD_DIM))
    return (split_heads[..., 0, :, :], split_heads[..., 1, :, :], split_heads[..., 2, :, :])


def attend_core(normed, weight_in, token_form, key_form, score_form):
    joined = flat_dot(normed, weight_in).astype(jnp.bfloat16)
    queries, keyset, valueset = split_join(joined)
    factor = HEAD_DIM ** (-0.5)
    scores = (
        jnp.einsum(
            token_form + "hd," + key_form + "hd->" + score_form,
            queries,
            keyset,
            preferred_element_type=jnp.float32,
        )
        * factor
    )
    totals = jax.nn.logsumexp(scores, axis=-1, keepdims=True)
    weighting = jnp.exp(scores - totals).astype(jnp.bfloat16)
    context = jnp.einsum(
        score_form + "," + key_form + "hd->" + token_form + "hd",
        weighting,
        valueset,
        preferred_element_type=jnp.float32,
    )
    context = context.reshape(normed.shape[:-1] + (D,)).astype(jnp.bfloat16)
    return (joined, totals, context)


def attend_back(joined, totals, back_context, token_form, key_form, score_form):
    queries, keyset, valueset = split_join(joined)
    back_heads = back_context.reshape(back_context.shape[:-1] + (HEADS, HEAD_DIM))
    factor = HEAD_DIM ** (-0.5)
    scores = (
        jnp.einsum(
            token_form + "hd," + key_form + "hd->" + score_form,
            queries,
            keyset,
            preferred_element_type=jnp.float32,
        )
        * factor
    )
    weighting = jnp.exp(scores - totals)
    back_weight = jnp.einsum(
        token_form + "hd," + key_form + "hd->" + score_form,
        back_heads,
        valueset,
        preferred_element_type=jnp.float32,
    )
    back_weight = back_weight.astype(jnp.bfloat16).astype(jnp.float32)
    inner_sum = jnp.sum(weighting * back_weight, axis=-1, keepdims=True)
    back_scores = (weighting * (back_weight - inner_sum)).astype(jnp.bfloat16)
    back_query = (
        jnp.einsum(
            score_form + "," + key_form + "hd->" + token_form + "hd",
            back_scores,
            keyset,
            preferred_element_type=jnp.float32,
        )
        * factor
    )
    back_keys = (
        jnp.einsum(
            score_form + "," + token_form + "hd->" + key_form + "hd",
            back_scores,
            queries,
            preferred_element_type=jnp.float32,
        )
        * factor
    )
    back_values = jnp.einsum(
        score_form + "," + token_form + "hd->" + key_form + "hd",
        weighting.astype(jnp.bfloat16),
        back_heads,
        preferred_element_type=jnp.float32,
    )
    stacked = jnp.stack((back_query, back_keys, back_values), axis=-3)
    return stacked.reshape(back_context.shape[:-1] + (3 * D,)).astype(jnp.bfloat16)


def gelu(values):
    return 0.5 * values * (1.0 + lax.erf(values * (0.5 ** 0.5)))


def to_places(frames_major):
    peers = lax.axis_size("fsdp")
    frames, places, width = frames_major.shape
    blocks = frames_major.reshape(frames, peers, places // peers, width).transpose(1, 0, 2, 3)
    blocks = lax.all_to_all(blocks, "fsdp", split_axis=0, concat_axis=0, tiled=True)
    return blocks.reshape(peers * frames, places // peers, width)


def to_frames(places_major):
    peers = lax.axis_size("fsdp")
    all_frames, places, width = places_major.shape
    blocks = places_major.reshape(peers, all_frames // peers, places, width)
    blocks = lax.all_to_all(blocks, "fsdp", split_axis=0, concat_axis=0, tiled=True)
    return blocks.transpose(1, 0, 2, 3).reshape(all_frames // peers, peers * places, width)


def to_member(array, kind, part, half):
    if kind == "gains":
        gain_part = lax.dynamic_slice_in_dim(array, part * half, half, axis=1).T
        return jnp.pad(gain_part, ((0, 0), (0, GAIN_COLS - gain_part.shape[1])))
    if kind == "grouped":
        rows = lax.dynamic_slice_in_dim(array, part * 4 * half, 4 * half, axis=0)
        return jnp.concatenate([rows[q * half:(q + 1) * half] for q in range(4)], axis=1)
    return lax.dynamic_slice_in_dim(array, part * half, half, axis=0)


def width_of(array, kind):
    return {"gains": GAIN_COLS, "grouped": 4 * D}.get(kind, array.shape[-1])


def from_members(block, kinds, widths, half):
    members = block.shape[0] // half
    outs = []
    offset = 0
    for kind, width in zip(kinds, widths):
        part = block[:, offset:offset + width]
        offset += width
        if kind == "gains":
            outs.append(part[:, :3].T)
        elif kind == "grouped":
            grouped = part.reshape(members, half, 4 * D)
            outs.append(
                jnp.concatenate([grouped[:, :, q * D:(q + 1) * D] for q in range(4)], axis=1).reshape(
                    members * 4 * half, D
                )
            )
        else:
            outs.append(part)
    return outs


def to_members_full(array, kind, members, half):
    array = array.astype(jnp.bfloat16)
    if kind == "gains":
        cols = array.T
        return jnp.pad(cols, ((0, 0), (0, GAIN_COLS - cols.shape[1])))
    if kind == "grouped":
        grouped = array.reshape(members, 4 * half, D)
        return jnp.concatenate(
            [grouped[:, q * half:(q + 1) * half, :] for q in range(4)], axis=2
        ).reshape(members * half, 4 * D)
    return array


def gather_group(arrays, kinds, part, half):
    block = jnp.concatenate([to_member(a, k, part, half) for a, k in zip(arrays, kinds)], axis=1)
    widths = [width_of(a, k) for a, k in zip(arrays, kinds)]
    gathered = lax.all_gather(block, MEMBERS, axis=0, tiled=True)
    return from_members(gathered, kinds, widths, half)


def pair_sum(values, axis):
    if lax.axis_size(axis) == 2:
        return values + lax.ppermute(values, axis, [(0, 1), (1, 0)])
    return lax.psum(values, axis)


def core_gather(values):
    if lax.axis_size("core") == 2:
        other = lax.ppermute(values, "core", [(0, 1), (1, 0)])
        first = lax.axis_index("core") == 0
        return jnp.concatenate(
            [jnp.where(first, values, other), jnp.where(first, other, values)], axis=0
        )
    return lax.all_gather(values, "core", axis=0, tiled=True)


def pack_group(grads, kinds, members, half):
    return jnp.concatenate(
        [to_members_full(g, k, members, half) for g, k in zip(grads, kinds)], axis=1
    )


def reduce_group(packed, grads, kinds, half):
    widths = [width_of(g, k) for g, k in zip(grads, kinds)]
    owned = lax.psum_scatter(packed, MEMBERS, scatter_dimension=0, tiled=True)
    owned = core_gather(pair_sum(owned, "dpo"))
    return [part.astype(jnp.float32) for part in from_members(owned, kinds, widths, half)]


def layer(
    inputs, space_in, space_out, time_in, time_out, hidden_in, hidden_out, norm_gains, cotangent
):
    fsdp_size = lax.axis_size("fsdp")
    core_size = lax.axis_size("core")
    members = fsdp_size * core_size
    half = space_in.shape[0] // core_size
    core = lax.axis_index("core")

    s_in, s_out, gains = gather_group(
        (space_in, space_out, norm_gains), ("plain", "plain", "gains"), core, half
    )
    t_in, t_out = gather_group((time_in, time_out), ("plain", "plain"), core, half)
    h_in, h_out = gather_group((hidden_in, hidden_out), ("plain", "grouped"), core, half)
    gain_rows = gains.astype(jnp.float32)

    micro = inputs.shape[0]
    spatial = ("gl", "gm", "ghlm")
    temporal = ("lg", "mg", "ghlm")

    saved = []
    mixed_twos = []
    for index in range(micro):
        frames_in = inputs[index, 0].astype(jnp.float32)
        normed_one = layer_norm(frames_in, gain_rows[0]).astype(jnp.bfloat16)
        join_space, total_space, context_space = attend_core(normed_one, s_in, *spatial)
        mixed_one = frames_in + flat_dot(context_space, s_out)
        normed_two = layer_norm(mixed_one, gain_rows[1]).astype(jnp.bfloat16)
        placed = to_places(normed_two)
        join_time, total_time, context_placed = attend_core(placed, t_in, *temporal)
        context_time = to_frames(context_placed)
        mixed_two = mixed_one + flat_dot(context_time, t_out)
        saved.append(
            dict(
                frames_in=frames_in,
                normed_one=normed_one,
                join_space=join_space,
                total_space=total_space,
                context_space=context_space,
                mixed_one=mixed_one,
                placed=placed,
                join_time=join_time,
                total_time=total_time,
                context_time=context_time,
            )
        )
        mixed_twos.append(mixed_two)

    mixed_two = jnp.stack(mixed_twos)
    normed_three = layer_norm(mixed_two, gain_rows[2]).astype(jnp.bfloat16)
    hidden = flat_dot(normed_three, h_in)
    activated = gelu(hidden).astype(jnp.bfloat16)
    result = mixed_two + flat_dot(activated, h_out)

    def summed(terms):
        total = terms[0]
        for term in terms[1:]:
            total = total + term
        return total

    gain_two_terms = []
    upstream_all = cotangent[:, 0].astype(jnp.float32)
    rounded = upstream_all.astype(jnp.bfloat16)
    grad_hidden_out = token_sum(activated, rounded)
    back_active = back_dot(rounded, h_out).astype(jnp.bfloat16)
    _, gelu_pull = jax.vjp(gelu, hidden)
    back_hidden = gelu_pull(back_active.astype(jnp.float32))[0].astype(jnp.bfloat16)
    grad_hidden_in = token_sum(normed_three, back_hidden)
    back_three_all = back_dot(back_hidden, h_in).astype(jnp.bfloat16)
    ffn_grads = (grad_hidden_in, grad_hidden_out)
    ffn_kinds = ("plain", "grouped")
    packed_ffn, back_three_all = lax.optimization_barrier(
        (pack_group(ffn_grads, ffn_kinds, members, half), back_three_all)
    )
    grad_ffn = reduce_group(packed_ffn, ffn_grads, ffn_kinds, half)
    back_threes = [back_three_all[index] for index in range(micro)]
    upstreams = [upstream_all[index] for index in range(micro)]

    back_twos_placed = []
    time_out_terms = []
    time_in_terms = []
    for index in range(micro):
        s = saved[index]
        back_mixed, gain_grad = norm_back(
            mixed_twos[index], gain_rows[2], back_threes[index].astype(jnp.float32)
        )
        gain_two_terms.append(gain_grad)
        upstream = upstreams[index] + back_mixed
        upstreams[index] = upstream
        rounded = upstream.astype(jnp.bfloat16)
        time_out_terms.append(token_sum(s["context_time"], rounded))
        back_context = back_dot(rounded, t_out).astype(jnp.bfloat16)
        back_placed = to_places(back_context)
        back_join = attend_back(s["join_time"], s["total_time"], back_placed, *temporal)
        time_in_terms.append(token_sum(s["placed"], back_join))
        back_twos_placed.append(back_dot(back_join, t_in).astype(jnp.bfloat16))
    time_grads = (summed(time_in_terms), summed(time_out_terms))
    time_kinds = ("plain", "plain")
    packed_time, back_twos_placed[-1] = lax.optimization_barrier(
        (pack_group(time_grads, time_kinds, members, half), back_twos_placed[-1])
    )
    grad_time = reduce_group(packed_time, time_grads, time_kinds, half)

    input_grads = []
    gain_one_terms = []
    gain_zero_terms = []
    space_out_terms = []
    space_in_terms = []
    for index in range(micro):
        s = saved[index]
        back_two = to_frames(back_twos_placed[index])
        back_mixed, gain_grad = norm_back(s["mixed_one"], gain_rows[1], back_two.astype(jnp.float32))
        gain_one_terms.append(gain_grad)
        upstream = upstreams[index] + back_mixed
        rounded = upstream.astype(jnp.bfloat16)
        space_out_terms.append(token_sum(s["context_space"], rounded))
        back_context = back_dot(rounded, s_out).astype(jnp.bfloat16)
        back_join = attend_back(s["join_space"], s["total_space"], back_context, *spatial)
        space_in_terms.append(token_sum(s["normed_one"], back_join))
        back_one = back_dot(back_join, s_in).astype(jnp.bfloat16)
        back_mixed, gain_grad = norm_back(
            s["frames_in"], gain_rows[0], back_one.astype(jnp.float32)
        )
        gain_zero_terms.append(gain_grad)
        input_grads.append(upstream + back_mixed)
    grad_space_in = summed(space_in_terms)
    grad_space_out = summed(space_out_terms)
    gain_grad_zero = summed(gain_zero_terms)
    gain_grad_one = summed(gain_one_terms)
    gain_grad_two = summed(gain_two_terms)
    input_grad = jnp.stack(input_grads)

    gain_grads = jnp.stack((gain_grad_zero, gain_grad_one, gain_grad_two))
    space_grads = (grad_space_in, grad_space_out, gain_grads)
    space_kinds = ("plain", "plain", "gains")
    grad_space = reduce_group(
        pack_group(space_grads, space_kinds, members, half), space_grads, space_kinds, half
    )
    return (
        result[:, None],
        input_grad[:, None],
        grad_space[0],
        grad_space[1],
        grad_time[0],
        grad_time[1],
        grad_ffn[0],
        grad_ffn[1],
        grad_space[2],
    )


def solution(mesh):
    dp_size, fsdp_size = mesh.devices.shape
    split = Mesh(mesh.devices.reshape(dp_size // 2, 2, fsdp_size), ("dpo", "core", "fsdp"))
    tokens = P(None, ("dpo", "core"), "fsdp", None, None)
    rows = P("fsdp", None)
    return jax.shard_map(
        layer,
        mesh=split,
        in_specs=(tokens, rows, rows, rows, rows, rows, rows, P(None, "fsdp"), tokens),
        out_specs=(tokens, tokens, rows, rows, rows, rows, rows, rows, P(None, "fsdp")),
        check_vma=False,
    )
```

```python
import jax
import jax.numpy as jnp
from jax import lax
from jax.sharding import Mesh
from jax.sharding import PartitionSpec as P


D = 768
HEADS = 12
HEAD_DIM = 64
GAIN_COLS = 128

EPS = 1e-06

MEMBERS = ("fsdp", "core")


def layer_norm(values, scales):
    average = jnp.mean(values, axis=-1, keepdims=True)
    centred = values - average
    spread = jnp.mean(centred * centred, axis=-1, keepdims=True)
    return centred * lax.rsqrt(spread + EPS) * scales


def norm_back(values, scales, incoming):
    _, pullback = jax.vjp(layer_norm, values, scales)
    return pullback(incoming)


def flat_dot(left, right):
    flat = left.reshape(-1, left.shape[-1])
    product = jnp.dot(flat, right, preferred_element_type=jnp.float32)
    return product.reshape(left.shape[:-1] + (right.shape[1],))


def back_dot(left, right):
    flat = left.reshape(-1, left.shape[-1])
    product = lax.dot_general(
        flat, right, (((1,), (1,)), ((), ())), preferred_element_type=jnp.float32
    )
    return product.reshape(left.shape[:-1] + (right.shape[0],))


def token_sum(left, right):
    left_rows = left.reshape(-1, left.shape[-1])
    right_rows = right.reshape(-1, right.shape[-1])
    return lax.dot_general(
        left_rows, right_rows, (((0,), (0,)), ((), ())), preferred_element_type=jnp.float32
    )


def split_join(joined):
    split_heads = joined.reshape(joined.shape[:-1] + (3, HEADS, HEAD_DIM))
    return (split_heads[..., 0, :, :], split_heads[..., 1, :, :], split_heads[..., 2, :, :])


def attend_core(normed, weight_in, token_form, key_form, score_form):
    joined = flat_dot(normed, weight_in).astype(jnp.bfloat16)
    queries, keyset, valueset = split_join(joined)
    factor = HEAD_DIM ** (-0.5)
    scores = (
        jnp.einsum(
            token_form + "hd," + key_form + "hd->" + score_form,
            queries,
            keyset,
            preferred_element_type=jnp.float32,
        )
        * factor
    )
    totals = jax.nn.logsumexp(scores, axis=-1, keepdims=True)
    weighting = jnp.exp(scores - totals).astype(jnp.bfloat16)
    context = jnp.einsum(
        score_form + "," + key_form + "hd->" + token_form + "hd",
        weighting,
        valueset,
        preferred_element_type=jnp.float32,
    )
    context = context.reshape(normed.shape[:-1] + (D,)).astype(jnp.bfloat16)
    return (joined, totals, context)


def attend_back(joined, totals, back_context, token_form, key_form, score_form):
    queries, keyset, valueset = split_join(joined)
    back_heads = back_context.reshape(back_context.shape[:-1] + (HEADS, HEAD_DIM))
    factor = HEAD_DIM ** (-0.5)
    scores = (
        jnp.einsum(
            token_form + "hd," + key_form + "hd->" + score_form,
            queries,
            keyset,
            preferred_element_type=jnp.float32,
        )
        * factor
    )
    weighting = jnp.exp(scores - totals)
    back_weight = jnp.einsum(
        token_form + "hd," + key_form + "hd->" + score_form,
        back_heads,
        valueset,
        preferred_element_type=jnp.float32,
    )
    back_weight = back_weight.astype(jnp.bfloat16).astype(jnp.float32)
    inner_sum = jnp.sum(weighting * back_weight, axis=-1, keepdims=True)
    back_scores = (weighting * (back_weight - inner_sum)).astype(jnp.bfloat16)
    back_query = (
        jnp.einsum(
            score_form + "," + key_form + "hd->" + token_form + "hd",
            back_scores,
            keyset,
            preferred_element_type=jnp.float32,
        )
        * factor
    )
    back_keys = (
        jnp.einsum(
            score_form + "," + token_form + "hd->" + key_form + "hd",
            back_scores,
            queries,
            preferred_element_type=jnp.float32,
        )
        * factor
    )
    back_values = jnp.einsum(
        score_form + "," + token_form + "hd->" + key_form + "hd",
        weighting.astype(jnp.bfloat16),
        back_heads,
        preferred_element_type=jnp.float32,
    )
    stacked = jnp.stack((back_query, back_keys, back_values), axis=-3)
    return stacked.reshape(back_context.shape[:-1] + (3 * D,)).astype(jnp.bfloat16)


def gelu(values):
    return 0.5 * values * (1.0 + lax.erf(values * (0.5 ** 0.5)))


def to_places(frames_major):
    peers = lax.axis_size("fsdp")
    frames, places, width = frames_major.shape
    blocks = frames_major.reshape(frames, peers, places // peers, width).transpose(1, 0, 2, 3)
    blocks = lax.all_to_all(blocks, "fsdp", split_axis=0, concat_axis=0, tiled=True)
    return blocks.reshape(peers * frames, places // peers, width)


def to_frames(places_major):
    peers = lax.axis_size("fsdp")
    all_frames, places, width = places_major.shape
    blocks = places_major.reshape(peers, all_frames // peers, places, width)
    blocks = lax.all_to_all(blocks, "fsdp", split_axis=0, concat_axis=0, tiled=True)
    return blocks.transpose(1, 0, 2, 3).reshape(all_frames // peers, peers * places, width)


def to_member(array, kind, part, half):
    if kind == "gains":
        gain_part = lax.dynamic_slice_in_dim(array, part * half, half, axis=1).T
        return jnp.pad(gain_part, ((0, 0), (0, GAIN_COLS - gain_part.shape[1])))
    if kind == "grouped":
        rows = lax.dynamic_slice_in_dim(array, part * 4 * half, 4 * half, axis=0)
        return jnp.concatenate([rows[q * half:(q + 1) * half] for q in range(4)], axis=1)
    return lax.dynamic_slice_in_dim(array, part * half, half, axis=0)


def width_of(array, kind):
    return {"gains": GAIN_COLS, "grouped": 4 * D}.get(kind, array.shape[-1])


def from_members(block, kinds, widths, half):
    members = block.shape[0] // half
    outs = []
    offset = 0
    for kind, width in zip(kinds, widths):
        part = block[:, offset:offset + width]
        offset += width
        if kind == "gains":
            outs.append(part[:, :3].T)
        elif kind == "grouped":
            grouped = part.reshape(members, half, 4 * D)
            outs.append(
                jnp.concatenate([grouped[:, :, q * D:(q + 1) * D] for q in range(4)], axis=1).reshape(
                    members * 4 * half, D
                )
            )
        else:
            outs.append(part)
    return outs


def to_members_full(array, kind, members, half):
    array = array.astype(jnp.bfloat16)
    if kind == "gains":
        cols = array.T
        return jnp.pad(cols, ((0, 0), (0, GAIN_COLS - cols.shape[1])))
    if kind == "grouped":
        grouped = array.reshape(members, 4 * half, D)
        return jnp.concatenate(
            [grouped[:, q * half:(q + 1) * half, :] for q in range(4)], axis=2
        ).reshape(members * half, 4 * D)
    return array


def gather_group(arrays, kinds, part, half):
    block = jnp.concatenate([to_member(a, k, part, half) for a, k in zip(arrays, kinds)], axis=1)
    widths = [width_of(a, k) for a, k in zip(arrays, kinds)]
    gathered = lax.all_gather(block, MEMBERS, axis=0, tiled=True)
    return from_members(gathered, kinds, widths, half)


def pair_sum(values, axis):
    if lax.axis_size(axis) == 2:
        return values + lax.ppermute(values, axis, [(0, 1), (1, 0)])
    return lax.psum(values, axis)


def core_gather(values):
    if lax.axis_size("core") == 2:
        other = lax.ppermute(values, "core", [(0, 1), (1, 0)])
        first = lax.axis_index("core") == 0
        return jnp.concatenate(
            [jnp.where(first, values, other), jnp.where(first, other, values)], axis=0
        )
    return lax.all_gather(values, "core", axis=0, tiled=True)


def pack_group(grads, kinds, members, half):
    return jnp.concatenate(
        [to_members_full(g, k, members, half) for g, k in zip(grads, kinds)], axis=1
    )


def reduce_group(packed, grads, kinds, half):
    widths = [width_of(g, k) for g, k in zip(grads, kinds)]
    owned = lax.psum_scatter(packed, MEMBERS, scatter_dimension=0, tiled=True)
    owned = core_gather(pair_sum(owned, "dpo"))
    return [part.astype(jnp.float32) for part in from_members(owned, kinds, widths, half)]


def layer(
    inputs, space_in, space_out, time_in, time_out, hidden_in, hidden_out, norm_gains, cotangent
):
    fsdp_size = lax.axis_size("fsdp")
    core_size = lax.axis_size("core")
    members = fsdp_size * core_size
    half = space_in.shape[0] // core_size
    core = lax.axis_index("core")

    s_in, s_out, gains = gather_group(
        (space_in, space_out, norm_gains), ("plain", "plain", "gains"), core, half
    )
    t_in, t_out = gather_group((time_in, time_out), ("plain", "plain"), core, half)
    h_in, h_out = gather_group((hidden_in, hidden_out), ("plain", "grouped"), core, half)
    gain_rows = gains.astype(jnp.float32)

    micro = inputs.shape[0]
    spatial = ("gl", "gm", "ghlm")
    temporal = ("lg", "mg", "ghlm")

    saved = []
    mixed_twos = []
    for index in range(micro):
        frames_in = inputs[index, 0].astype(jnp.float32)
        normed_one = layer_norm(frames_in, gain_rows[0]).astype(jnp.bfloat16)
        join_space, total_space, context_space = attend_core(normed_one, s_in, *spatial)
        mixed_one = frames_in + flat_dot(context_space, s_out)
        normed_two = layer_norm(mixed_one, gain_rows[1]).astype(jnp.bfloat16)
        placed = to_places(normed_two)
        join_time, total_time, context_placed = attend_core(placed, t_in, *temporal)
        context_time = to_frames(context_placed)
        mixed_two = mixed_one + flat_dot(context_time, t_out)
        saved.append(
            dict(
                frames_in=frames_in,
                normed_one=normed_one,
                join_space=join_space,
                total_space=total_space,
                context_space=context_space,
                mixed_one=mixed_one,
                placed=placed,
                join_time=join_time,
                total_time=total_time,
                context_time=context_time,
            )
        )
        mixed_twos.append(mixed_two)

    mixed_two = jnp.stack(mixed_twos)
    normed_three = layer_norm(mixed_two, gain_rows[2]).astype(jnp.bfloat16)
    hidden = flat_dot(normed_three, h_in)
    activated = gelu(hidden).astype(jnp.bfloat16)
    result = mixed_two + flat_dot(activated, h_out)

    def summed(terms):
        total = terms[0]
        for term in terms[1:]:
            total = total + term
        return total

    gain_two_terms = []
    upstream_all = cotangent[:, 0].astype(jnp.float32)
    rounded = upstream_all.astype(jnp.bfloat16)
    grad_hidden_out = token_sum(activated, rounded)
    back_active = back_dot(rounded, h_out).astype(jnp.bfloat16)
    _, gelu_pull = jax.vjp(gelu, hidden)
    back_hidden = gelu_pull(back_active.astype(jnp.float32))[0].astype(jnp.bfloat16)
    grad_hidden_in = token_sum(normed_three, back_hidden)
    back_three_all = back_dot(back_hidden, h_in).astype(jnp.bfloat16)
    ffn_grads = (grad_hidden_in, grad_hidden_out)
    ffn_kinds = ("plain", "grouped")
    packed_ffn, t_in, t_out = lax.optimization_barrier(
        (pack_group(ffn_grads, ffn_kinds, members, half), t_in, t_out)
    )
    grad_ffn = reduce_group(packed_ffn, ffn_grads, ffn_kinds, half)
    back_threes = [back_three_all[index] for index in range(micro)]
    upstreams = [upstream_all[index] for index in range(micro)]

    back_twos_placed = []
    time_out_terms = []
    time_in_terms = []
    for index in range(micro):
        s = saved[index]
        back_mixed, gain_grad = norm_back(
            mixed_twos[index], gain_rows[2], back_threes[index].astype(jnp.float32)
        )
        gain_two_terms.append(gain_grad)
        upstream = upstreams[index] + back_mixed
        upstreams[index] = upstream
        rounded = upstream.astype(jnp.bfloat16)
        time_out_terms.append(token_sum(s["context_time"], rounded))
        back_context = back_dot(rounded, t_out).astype(jnp.bfloat16)
        back_placed = to_places(back_context)
        back_join = attend_back(s["join_time"], s["total_time"], back_placed, *temporal)
        time_in_terms.append(token_sum(s["placed"], back_join))
        back_twos_placed.append(back_dot(back_join, t_in).astype(jnp.bfloat16))
    time_grads = (summed(time_in_terms), summed(time_out_terms))
    time_kinds = ("plain", "plain")
    packed_time, s_in, s_out = lax.optimization_barrier(
        (pack_group(time_grads, time_kinds, members, half), s_in, s_out)
    )
    grad_time = reduce_group(packed_time, time_grads, time_kinds, half)

    input_grads = []
    gain_one_terms = []
    gain_zero_terms = []
    space_out_terms = []
    space_in_terms = []
    for index in range(micro):
        s = saved[index]
        back_two = to_frames(back_twos_placed[index])
        back_mixed, gain_grad = norm_back(s["mixed_one"], gain_rows[1], back_two.astype(jnp.float32))
        gain_one_terms.append(gain_grad)
        upstream = upstreams[index] + back_mixed
        rounded = upstream.astype(jnp.bfloat16)
        space_out_terms.append(token_sum(s["context_space"], rounded))
        back_context = back_dot(rounded, s_out).astype(jnp.bfloat16)
        back_join = attend_back(s["join_space"], s["total_space"], back_context, *spatial)
        space_in_terms.append(token_sum(s["normed_one"], back_join))
        back_one = back_dot(back_join, s_in).astype(jnp.bfloat16)
        back_mixed, gain_grad = norm_back(
            s["frames_in"], gain_rows[0], back_one.astype(jnp.float32)
        )
        gain_zero_terms.append(gain_grad)
        input_grads.append(upstream + back_mixed)
    grad_space_in = summed(space_in_terms)
    grad_space_out = summed(space_out_terms)
    gain_grad_zero = summed(gain_zero_terms)
    gain_grad_one = summed(gain_one_terms)
    gain_grad_two = summed(gain_two_terms)
    input_grad = jnp.stack(input_grads)

    gain_grads = jnp.stack((gain_grad_zero, gain_grad_one, gain_grad_two))
    space_grads = (grad_space_in, grad_space_out, gain_grads)
    space_kinds = ("plain", "plain", "gains")
    grad_space = reduce_group(
        pack_group(space_grads, space_kinds, members, half), space_grads, space_kinds, half
    )
    return (
        result[:, None],
        input_grad[:, None],
        grad_space[0],
        grad_space[1],
        grad_time[0],
        grad_time[1],
        grad_ffn[0],
        grad_ffn[1],
        grad_space[2],
    )


def solution(mesh):
    dp_size, fsdp_size = mesh.devices.shape
    split = Mesh(mesh.devices.reshape(dp_size // 2, 2, fsdp_size), ("dpo", "core", "fsdp"))
    tokens = P(None, ("dpo", "core"), "fsdp", None, None)
    rows = P("fsdp", None)
    return jax.shard_map(
        layer,
        mesh=split,
        in_specs=(tokens, rows, rows, rows, rows, rows, rows, P(None, "fsdp"), tokens),
        out_specs=(tokens, tokens, rows, rows, rows, rows, rows, rows, P(None, "fsdp")),
        check_vma=False,
    )
```

```python
import jax
import jax.numpy as jnp
from jax import lax
from jax.sharding import Mesh
from jax.sharding import PartitionSpec as P


D = 768
HEADS = 12
HEAD_DIM = 64
GAIN_COLS = 128

EPS = 1e-06

MEMBERS = ("fsdp", "core")


def layer_norm(values, scales):
    average = jnp.mean(values, axis=-1, keepdims=True)
    centred = values - average
    spread = jnp.mean(centred * centred, axis=-1, keepdims=True)
    return centred * lax.rsqrt(spread + EPS) * scales


def norm_back(values, scales, incoming):
    _, pullback = jax.vjp(layer_norm, values, scales)
    return pullback(incoming)


def flat_dot(left, right):
    flat = left.reshape(-1, left.shape[-1])
    product = jnp.dot(flat, right, preferred_element_type=jnp.float32)
    return product.reshape(left.shape[:-1] + (right.shape[1],))


def back_dot(left, right):
    flat = left.reshape(-1, left.shape[-1])
    product = lax.dot_general(
        flat, right, (((1,), (1,)), ((), ())), preferred_element_type=jnp.float32
    )
    return product.reshape(left.shape[:-1] + (right.shape[0],))


def token_sum(left, right):
    left_rows = left.reshape(-1, left.shape[-1])
    right_rows = right.reshape(-1, right.shape[-1])
    return lax.dot_general(
        left_rows, right_rows, (((0,), (0,)), ((), ())), preferred_element_type=jnp.float32
    )


def split_join(joined):
    split_heads = joined.reshape(joined.shape[:-1] + (3, HEADS, HEAD_DIM))
    return (split_heads[..., 0, :, :], split_heads[..., 1, :, :], split_heads[..., 2, :, :])


def attend_core(normed, weight_in, token_form, key_form, score_form):
    joined = flat_dot(normed, weight_in).astype(jnp.bfloat16)
    queries, keyset, valueset = split_join(joined)
    factor = HEAD_DIM ** (-0.5)
    scores = (
        jnp.einsum(
            token_form + "hd," + key_form + "hd->" + score_form,
            queries,
            keyset,
            preferred_element_type=jnp.float32,
        )
        * factor
    )
    totals = jax.nn.logsumexp(scores, axis=-1, keepdims=True)
    weighting = jnp.exp(scores - totals).astype(jnp.bfloat16)
    context = jnp.einsum(
        score_form + "," + key_form + "hd->" + token_form + "hd",
        weighting,
        valueset,
        preferred_element_type=jnp.float32,
    )
    context = context.reshape(normed.shape[:-1] + (D,)).astype(jnp.bfloat16)
    return (joined, totals, context)


def attend_back(joined, totals, back_context, token_form, key_form, score_form):
    queries, keyset, valueset = split_join(joined)
    back_heads = back_context.reshape(back_context.shape[:-1] + (HEADS, HEAD_DIM))
    factor = HEAD_DIM ** (-0.5)
    scores = (
        jnp.einsum(
            token_form + "hd," + key_form + "hd->" + score_form,
            queries,
            keyset,
            preferred_element_type=jnp.float32,
        )
        * factor
    )
    weighting = jnp.exp(scores - totals)
    back_weight = jnp.einsum(
        token_form + "hd," + key_form + "hd->" + score_form,
        back_heads,
        valueset,
        preferred_element_type=jnp.float32,
    )
    back_weight = back_weight.astype(jnp.bfloat16).astype(jnp.float32)
    inner_sum = jnp.sum(weighting * back_weight, axis=-1, keepdims=True)
    back_scores = (weighting * (back_weight - inner_sum)).astype(jnp.bfloat16)
    back_query = (
        jnp.einsum(
            score_form + "," + key_form + "hd->" + token_form + "hd",
            back_scores,
            keyset,
            preferred_element_type=jnp.float32,
        )
        * factor
    )
    back_keys = (
        jnp.einsum(
            score_form + "," + token_form + "hd->" + key_form + "hd",
            back_scores,
            queries,
            preferred_element_type=jnp.float32,
        )
        * factor
    )
    back_values = jnp.einsum(
        score_form + "," + token_form + "hd->" + key_form + "hd",
        weighting.astype(jnp.bfloat16),
        back_heads,
        preferred_element_type=jnp.float32,
    )
    stacked = jnp.stack((back_query, back_keys, back_values), axis=-3)
    return stacked.reshape(back_context.shape[:-1] + (3 * D,)).astype(jnp.bfloat16)


def gelu(values):
    return 0.5 * values * (1.0 + lax.erf(values * (0.5 ** 0.5)))


def to_places(frames_major):
    peers = lax.axis_size("fsdp")
    frames, places, width = frames_major.shape
    blocks = frames_major.reshape(frames, peers, places // peers, width).transpose(1, 0, 2, 3)
    blocks = lax.all_to_all(blocks, "fsdp", split_axis=0, concat_axis=0, tiled=True)
    return blocks.reshape(peers * frames, places // peers, width)


def to_frames(places_major):
    peers = lax.axis_size("fsdp")
    all_frames, places, width = places_major.shape
    blocks = places_major.reshape(peers, all_frames // peers, places, width)
    blocks = lax.all_to_all(blocks, "fsdp", split_axis=0, concat_axis=0, tiled=True)
    return blocks.transpose(1, 0, 2, 3).reshape(all_frames // peers, peers * places, width)


def to_member(array, kind, part, half):
    if kind == "gains":
        gain_part = lax.dynamic_slice_in_dim(array, part * half, half, axis=1).T
        return jnp.pad(gain_part, ((0, 0), (0, GAIN_COLS - gain_part.shape[1])))
    if kind == "grouped":
        rows = lax.dynamic_slice_in_dim(array, part * 4 * half, 4 * half, axis=0)
        return jnp.concatenate([rows[q * half:(q + 1) * half] for q in range(4)], axis=1)
    return lax.dynamic_slice_in_dim(array, part * half, half, axis=0)


def width_of(array, kind):
    return {"gains": GAIN_COLS, "grouped": 4 * D}.get(kind, array.shape[-1])


def from_members(block, kinds, widths, half):
    members = block.shape[0] // half
    outs = []
    offset = 0
    for kind, width in zip(kinds, widths):
        part = block[:, offset:offset + width]
        offset += width
        if kind == "gains":
            outs.append(part[:, :3].T)
        elif kind == "grouped":
            grouped = part.reshape(members, half, 4 * D)
            outs.append(
                jnp.concatenate([grouped[:, :, q * D:(q + 1) * D] for q in range(4)], axis=1).reshape(
                    members * 4 * half, D
                )
            )
        else:
            outs.append(part)
    return outs


def to_members_full(array, kind, members, half):
    array = array.astype(jnp.bfloat16)
    if kind == "gains":
        cols = array.T
        return jnp.pad(cols, ((0, 0), (0, GAIN_COLS - cols.shape[1])))
    if kind == "grouped":
        grouped = array.reshape(members, 4 * half, D)
        return jnp.concatenate(
            [grouped[:, q * half:(q + 1) * half, :] for q in range(4)], axis=2
        ).reshape(members * half, 4 * D)
    return array


def gather_group(arrays, kinds, part, half):
    block = jnp.concatenate([to_member(a, k, part, half) for a, k in zip(arrays, kinds)], axis=1)
    widths = [width_of(a, k) for a, k in zip(arrays, kinds)]
    gathered = lax.all_gather(block, MEMBERS, axis=0, tiled=True)
    return from_members(gathered, kinds, widths, half)


def pair_sum(values, axis):
    if lax.axis_size(axis) == 2:
        return values + lax.ppermute(values, axis, [(0, 1), (1, 0)])
    return lax.psum(values, axis)


def core_gather(values):
    if lax.axis_size("core") == 2:
        other = lax.ppermute(values, "core", [(0, 1), (1, 0)])
        first = lax.axis_index("core") == 0
        return jnp.concatenate(
            [jnp.where(first, values, other), jnp.where(first, other, values)], axis=0
        )
    return lax.all_gather(values, "core", axis=0, tiled=True)


def pack_group(grads, kinds, members, half):
    return jnp.concatenate(
        [to_members_full(g, k, members, half) for g, k in zip(grads, kinds)], axis=1
    )


def reduce_group(packed, grads, kinds, half):
    widths = [width_of(g, k) for g, k in zip(grads, kinds)]
    owned = lax.psum_scatter(packed, MEMBERS, scatter_dimension=0, tiled=True)
    owned = core_gather(pair_sum(owned, "dpo"))
    return [part.astype(jnp.float32) for part in from_members(owned, kinds, widths, half)]


def layer(
    inputs, space_in, space_out, time_in, time_out, hidden_in, hidden_out, norm_gains, cotangent
):
    fsdp_size = lax.axis_size("fsdp")
    core_size = lax.axis_size("core")
    members = fsdp_size * core_size
    half = space_in.shape[0] // core_size
    core = lax.axis_index("core")

    s_in, s_out, gains = gather_group(
        (space_in, space_out, norm_gains), ("plain", "plain", "gains"), core, half
    )
    t_in, t_out = gather_group((time_in, time_out), ("plain", "plain"), core, half)
    h_in, h_out = gather_group((hidden_in, hidden_out), ("plain", "grouped"), core, half)
    gain_rows = gains.astype(jnp.float32)

    micro = inputs.shape[0]
    spatial = ("gl", "gm", "ghlm")
    temporal = ("lg", "mg", "ghlm")

    saved = []
    mixed_twos = []
    for index in range(micro):
        frames_in = inputs[index, 0].astype(jnp.float32)
        normed_one = layer_norm(frames_in, gain_rows[0]).astype(jnp.bfloat16)
        join_space, total_space, context_space = attend_core(normed_one, s_in, *spatial)
        mixed_one = frames_in + flat_dot(context_space, s_out)
        normed_two = layer_norm(mixed_one, gain_rows[1]).astype(jnp.bfloat16)
        placed = to_places(normed_two)
        join_time, total_time, context_placed = attend_core(placed, t_in, *temporal)
        context_time = to_frames(context_placed)
        mixed_two = mixed_one + flat_dot(context_time, t_out)
        saved.append(
            dict(
                frames_in=frames_in,
                normed_one=normed_one,
                join_space=join_space,
                total_space=total_space,
                context_space=context_space,
                mixed_one=mixed_one,
                placed=placed,
                join_time=join_time,
                total_time=total_time,
                context_time=context_time,
            )
        )
        mixed_twos.append(mixed_two)

    mixed_two = jnp.stack(mixed_twos)
    normed_three = layer_norm(mixed_two, gain_rows[2]).astype(jnp.bfloat16)
    hidden = flat_dot(normed_three, h_in)
    activated = gelu(hidden).astype(jnp.bfloat16)
    result = mixed_two + flat_dot(activated, h_out)

    def summed(terms):
        total = terms[0]
        for term in terms[1:]:
            total = total + term
        return total

    gain_two_terms = []
    upstream_all = cotangent[:, 0].astype(jnp.float32)
    rounded = upstream_all.astype(jnp.bfloat16)
    grad_hidden_out = token_sum(activated, rounded)
    back_active = back_dot(rounded, h_out).astype(jnp.bfloat16)
    _, gelu_pull = jax.vjp(gelu, hidden)
    back_hidden = gelu_pull(back_active.astype(jnp.float32))[0].astype(jnp.bfloat16)
    grad_hidden_in = token_sum(normed_three, back_hidden)
    back_three_all = back_dot(back_hidden, h_in).astype(jnp.bfloat16)
    ffn_grads = (grad_hidden_in, grad_hidden_out)
    ffn_kinds = ("plain", "grouped")
    packed_ffn, t_in, t_out = lax.optimization_barrier(
        (pack_group(ffn_grads, ffn_kinds, members, half), t_in, t_out)
    )
    grad_ffn = reduce_group(packed_ffn, ffn_grads, ffn_kinds, half)
    back_mixed, gain_grad = norm_back(mixed_two, gain_rows[2], back_three_all.astype(jnp.float32))
    gain_two_terms.append(gain_grad)
    upstream_all = upstream_all + back_mixed
    rounded_all = upstream_all.astype(jnp.bfloat16)
    back_context_all = back_dot(rounded_all, t_out).astype(jnp.bfloat16)
    upstreams = [upstream_all[index] for index in range(micro)]

    back_twos_placed = []
    time_out_terms = []
    time_in_terms = []
    for index in range(micro):
        s = saved[index]
        time_out_terms.append(token_sum(s["context_time"], rounded_all[index]))
        back_placed = to_places(back_context_all[index])
        back_join = attend_back(s["join_time"], s["total_time"], back_placed, *temporal)
        time_in_terms.append(token_sum(s["placed"], back_join))
        back_twos_placed.append(back_dot(back_join, t_in).astype(jnp.bfloat16))
    time_grads = (summed(time_in_terms), summed(time_out_terms))
    time_kinds = ("plain", "plain")
    packed_time, back_twos_placed[-1] = lax.optimization_barrier(
        (pack_group(time_grads, time_kinds, members, half), back_twos_placed[-1])
    )
    grad_time = reduce_group(packed_time, time_grads, time_kinds, half)

    input_grads = []
    gain_one_terms = []
    gain_zero_terms = []
    space_out_terms = []
    space_in_terms = []
    for index in range(micro):
        s = saved[index]
        back_two = to_frames(back_twos_placed[index])
        back_mixed, gain_grad = norm_back(s["mixed_one"], gain_rows[1], back_two.astype(jnp.float32))
        gain_one_terms.append(gain_grad)
        upstream = upstreams[index] + back_mixed
        rounded = upstream.astype(jnp.bfloat16)
        space_out_terms.append(token_sum(s["context_space"], rounded))
        back_context = back_dot(rounded, s_out).astype(jnp.bfloat16)
        back_join = attend_back(s["join_space"], s["total_space"], back_context, *spatial)
        space_in_terms.append(token_sum(s["normed_one"], back_join))
        back_one = back_dot(back_join, s_in).astype(jnp.bfloat16)
        back_mixed, gain_grad = norm_back(
            s["frames_in"], gain_rows[0], back_one.astype(jnp.float32)
        )
        gain_zero_terms.append(gain_grad)
        input_grads.append(upstream + back_mixed)
    grad_space_in = summed(space_in_terms)
    grad_space_out = summed(space_out_terms)
    gain_grad_zero = summed(gain_zero_terms)
    gain_grad_one = summed(gain_one_terms)
    gain_grad_two = summed(gain_two_terms)
    input_grad = jnp.stack(input_grads)

    gain_grads = jnp.stack((gain_grad_zero, gain_grad_one, gain_grad_two))
    space_grads = (grad_space_in, grad_space_out, gain_grads)
    space_kinds = ("plain", "plain", "gains")
    grad_space = reduce_group(
        pack_group(space_grads, space_kinds, members, half), space_grads, space_kinds, half
    )
    return (
        result[:, None],
        input_grad[:, None],
        grad_space[0],
        grad_space[1],
        grad_time[0],
        grad_time[1],
        grad_ffn[0],
        grad_ffn[1],
        grad_space[2],
    )


def solution(mesh):
    dp_size, fsdp_size = mesh.devices.shape
    split = Mesh(mesh.devices.reshape(dp_size // 2, 2, fsdp_size), ("dpo", "core", "fsdp"))
    tokens = P(None, ("dpo", "core"), "fsdp", None, None)
    rows = P("fsdp", None)
    return jax.shard_map(
        layer,
        mesh=split,
        in_specs=(tokens, rows, rows, rows, rows, rows, rows, P(None, "fsdp"), tokens),
        out_specs=(tokens, tokens, rows, rows, rows, rows, rows, rows, P(None, "fsdp")),
        check_vma=False,
    )
```

```python
import jax
import jax.numpy as jnp
from jax import lax
from jax.sharding import Mesh
from jax.sharding import PartitionSpec as P


D = 768
HEADS = 12
HEAD_DIM = 64
GAIN_COLS = 128

EPS = 1e-06

MEMBERS = ("fsdp", "core")


def layer_norm(values, scales):
    average = jnp.mean(values, axis=-1, keepdims=True)
    centred = values - average
    spread = jnp.mean(centred * centred, axis=-1, keepdims=True)
    return centred * lax.rsqrt(spread + EPS) * scales


def norm_back(values, scales, incoming):
    _, pullback = jax.vjp(layer_norm, values, scales)
    return pullback(incoming)


def flat_dot(left, right):
    flat = left.reshape(-1, left.shape[-1])
    product = jnp.dot(flat, right, preferred_element_type=jnp.float32)
    return product.reshape(left.shape[:-1] + (right.shape[1],))


def back_dot(left, right):
    flat = left.reshape(-1, left.shape[-1])
    product = lax.dot_general(
        flat, right, (((1,), (1,)), ((), ())), preferred_element_type=jnp.float32
    )
    return product.reshape(left.shape[:-1] + (right.shape[0],))


def token_sum(left, right):
    left_rows = left.reshape(-1, left.shape[-1])
    right_rows = right.reshape(-1, right.shape[-1])
    return lax.dot_general(
        left_rows, right_rows, (((0,), (0,)), ((), ())), preferred_element_type=jnp.float32
    )


def split_join(joined):
    split_heads = joined.reshape(joined.shape[:-1] + (3, HEADS, HEAD_DIM))
    return (split_heads[..., 0, :, :], split_heads[..., 1, :, :], split_heads[..., 2, :, :])


def attend_core(normed, weight_in, token_form, key_form, score_form):
    joined = flat_dot(normed, weight_in).astype(jnp.bfloat16)
    queries, keyset, valueset = split_join(joined)
    factor = HEAD_DIM ** (-0.5)
    scores = (
        jnp.einsum(
            token_form + "hd," + key_form + "hd->" + score_form,
            queries,
            keyset,
            preferred_element_type=jnp.float32,
        )
        * factor
    )
    totals = jax.nn.logsumexp(scores, axis=-1, keepdims=True)
    weighting = jnp.exp(scores - totals).astype(jnp.bfloat16)
    context = jnp.einsum(
        score_form + "," + key_form + "hd->" + token_form + "hd",
        weighting,
        valueset,
        preferred_element_type=jnp.float32,
    )
    context = context.reshape(normed.shape[:-1] + (D,)).astype(jnp.bfloat16)
    return (joined, totals, context)


def attend_back(joined, totals, back_context, token_form, key_form, score_form):
    queries, keyset, valueset = split_join(joined)
    back_heads = back_context.reshape(back_context.shape[:-1] + (HEADS, HEAD_DIM))
    factor = HEAD_DIM ** (-0.5)
    scores = (
        jnp.einsum(
            token_form + "hd," + key_form + "hd->" + score_form,
            queries,
            keyset,
            preferred_element_type=jnp.float32,
        )
        * factor
    )
    weighting = jnp.exp(scores - totals)
    back_weight = jnp.einsum(
        token_form + "hd," + key_form + "hd->" + score_form,
        back_heads,
        valueset,
        preferred_element_type=jnp.float32,
    )
    back_weight = back_weight.astype(jnp.bfloat16).astype(jnp.float32)
    inner_sum = jnp.sum(weighting * back_weight, axis=-1, keepdims=True)
    back_scores = (weighting * (back_weight - inner_sum)).astype(jnp.bfloat16)
    back_query = (
        jnp.einsum(
            score_form + "," + key_form + "hd->" + token_form + "hd",
            back_scores,
            keyset,
            preferred_element_type=jnp.float32,
        )
        * factor
    )
    back_keys = (
        jnp.einsum(
            score_form + "," + token_form + "hd->" + key_form + "hd",
            back_scores,
            queries,
            preferred_element_type=jnp.float32,
        )
        * factor
    )
    back_values = jnp.einsum(
        score_form + "," + token_form + "hd->" + key_form + "hd",
        weighting.astype(jnp.bfloat16),
        back_heads,
        preferred_element_type=jnp.float32,
    )
    stacked = jnp.stack((back_query, back_keys, back_values), axis=-3)
    return stacked.reshape(back_context.shape[:-1] + (3 * D,)).astype(jnp.bfloat16)


def gelu(values):
    return 0.5 * values * (1.0 + lax.erf(values * (0.5 ** 0.5)))


def to_places(frames_major):
    peers = lax.axis_size("fsdp")
    frames, places, width = frames_major.shape
    blocks = frames_major.reshape(frames, peers, places // peers, width).transpose(1, 0, 2, 3)
    blocks = lax.all_to_all(blocks, "fsdp", split_axis=0, concat_axis=0, tiled=True)
    return blocks.reshape(peers * frames, places // peers, width)


def to_frames(places_major):
    peers = lax.axis_size("fsdp")
    all_frames, places, width = places_major.shape
    blocks = places_major.reshape(peers, all_frames // peers, places, width)
    blocks = lax.all_to_all(blocks, "fsdp", split_axis=0, concat_axis=0, tiled=True)
    return blocks.transpose(1, 0, 2, 3).reshape(all_frames // peers, peers * places, width)


def to_member(array, kind, part, half):
    if kind == "gains":
        gain_part = lax.dynamic_slice_in_dim(array, part * half, half, axis=1).T
        return jnp.pad(gain_part, ((0, 0), (0, GAIN_COLS - gain_part.shape[1])))
    if kind == "grouped":
        rows = lax.dynamic_slice_in_dim(array, part * 4 * half, 4 * half, axis=0)
        return jnp.concatenate([rows[q * half:(q + 1) * half] for q in range(4)], axis=1)
    return lax.dynamic_slice_in_dim(array, part * half, half, axis=0)


def width_of(array, kind):
    return {"gains": GAIN_COLS, "grouped": 4 * D}.get(kind, array.shape[-1])


def from_members(block, kinds, widths, half):
    members = block.shape[0] // half
    outs = []
    offset = 0
    for kind, width in zip(kinds, widths):
        part = block[:, offset:offset + width]
        offset += width
        if kind == "gains":
            outs.append(part[:, :3].T)
        elif kind == "grouped":
            grouped = part.reshape(members, half, 4 * D)
            outs.append(
                jnp.concatenate([grouped[:, :, q * D:(q + 1) * D] for q in range(4)], axis=1).reshape(
                    members * 4 * half, D
                )
            )
        else:
            outs.append(part)
    return outs


def to_members_full(array, kind, members, half):
    array = array.astype(jnp.bfloat16)
    if kind == "gains":
        cols = array.T
        return jnp.pad(cols, ((0, 0), (0, GAIN_COLS - cols.shape[1])))
    if kind == "grouped":
        grouped = array.reshape(members, 4 * half, D)
        return jnp.concatenate(
            [grouped[:, q * half:(q + 1) * half, :] for q in range(4)], axis=2
        ).reshape(members * half, 4 * D)
    return array


def gather_group(arrays, kinds, part, half):
    block = jnp.concatenate([to_member(a, k, part, half) for a, k in zip(arrays, kinds)], axis=1)
    widths = [width_of(a, k) for a, k in zip(arrays, kinds)]
    gathered = lax.all_gather(block, MEMBERS, axis=0, tiled=True)
    return from_members(gathered, kinds, widths, half)


def pair_sum(values, axis):
    if lax.axis_size(axis) == 2:
        return values + lax.ppermute(values, axis, [(0, 1), (1, 0)])
    return lax.psum(values, axis)


def core_gather(values):
    if lax.axis_size("core") == 2:
        other = lax.ppermute(values, "core", [(0, 1), (1, 0)])
        first = lax.axis_index("core") == 0
        return jnp.concatenate(
            [jnp.where(first, values, other), jnp.where(first, other, values)], axis=0
        )
    return lax.all_gather(values, "core", axis=0, tiled=True)


def pack_group(grads, kinds, members, half):
    return jnp.concatenate(
        [to_members_full(g, k, members, half) for g, k in zip(grads, kinds)], axis=1
    )


def reduce_group(packed, grads, kinds, half):
    widths = [width_of(g, k) for g, k in zip(grads, kinds)]
    owned = lax.psum_scatter(packed, MEMBERS, scatter_dimension=0, tiled=True)
    owned = core_gather(pair_sum(owned, "dpo"))
    return [part.astype(jnp.float32) for part in from_members(owned, kinds, widths, half)]


def layer(
    inputs, space_in, space_out, time_in, time_out, hidden_in, hidden_out, norm_gains, cotangent
):
    fsdp_size = lax.axis_size("fsdp")
    core_size = lax.axis_size("core")
    members = fsdp_size * core_size
    half = space_in.shape[0] // core_size
    core = lax.axis_index("core")

    s_in, s_out, gains = gather_group(
        (space_in, space_out, norm_gains), ("plain", "plain", "gains"), core, half
    )
    t_in, t_out = gather_group((time_in, time_out), ("plain", "plain"), core, half)
    h_in, h_out = gather_group((hidden_in, hidden_out), ("plain", "grouped"), core, half)
    gain_rows = gains.astype(jnp.float32)

    micro = inputs.shape[0]
    spatial = ("gl", "gm", "ghlm")
    temporal = ("lg", "mg", "ghlm")

    saved = []
    mixed_twos = []
    for index in range(micro):
        frames_in = inputs[index, 0].astype(jnp.float32)
        normed_one = layer_norm(frames_in, gain_rows[0]).astype(jnp.bfloat16)
        join_space, total_space, context_space = attend_core(normed_one, s_in, *spatial)
        mixed_one = frames_in + flat_dot(context_space, s_out)
        normed_two = layer_norm(mixed_one, gain_rows[1]).astype(jnp.bfloat16)
        placed = to_places(normed_two)
        join_time, total_time, context_placed = attend_core(placed, t_in, *temporal)
        context_time = to_frames(context_placed)
        mixed_two = mixed_one + flat_dot(context_time, t_out)
        saved.append(
            dict(
                frames_in=frames_in,
                normed_one=normed_one,
                join_space=join_space,
                total_space=total_space,
                context_space=context_space,
                mixed_one=mixed_one,
                placed=placed,
                join_time=join_time,
                total_time=total_time,
                context_time=context_time,
            )
        )
        mixed_twos.append(mixed_two)

    mixed_two = jnp.stack(mixed_twos)
    normed_three = layer_norm(mixed_two, gain_rows[2]).astype(jnp.bfloat16)
    hidden = flat_dot(normed_three, h_in)
    activated = gelu(hidden).astype(jnp.bfloat16)
    result = mixed_two + flat_dot(activated, h_out)

    def summed(terms):
        total = terms[0]
        for term in terms[1:]:
            total = total + term
        return total

    gain_two_terms = []
    upstream_all = cotangent[:, 0].astype(jnp.float32)
    rounded = upstream_all.astype(jnp.bfloat16)
    grad_hidden_out = token_sum(activated, rounded)
    back_active = back_dot(rounded, h_out).astype(jnp.bfloat16)
    _, gelu_pull = jax.vjp(gelu, hidden)
    back_hidden = gelu_pull(back_active.astype(jnp.float32))[0].astype(jnp.bfloat16)
    grad_hidden_in = token_sum(normed_three, back_hidden)
    back_three_all = back_dot(back_hidden, h_in).astype(jnp.bfloat16)
    ffn_grads = (grad_hidden_in, grad_hidden_out)
    ffn_kinds = ("plain", "grouped")
    packed_ffn, t_in, t_out = lax.optimization_barrier(
        (pack_group(ffn_grads, ffn_kinds, members, half), t_in, t_out)
    )
    grad_ffn = reduce_group(packed_ffn, ffn_grads, ffn_kinds, half)
    back_threes = [back_three_all[index] for index in range(micro)]
    upstreams = [upstream_all[index] for index in range(micro)]

    back_twos_placed = []
    time_out_terms = []
    time_in_terms = []
    for index in range(micro):
        s = saved[index]
        back_mixed, gain_grad = norm_back(
            mixed_twos[index], gain_rows[2], back_threes[index].astype(jnp.float32)
        )
        gain_two_terms.append(gain_grad)
        upstream = upstreams[index] + back_mixed
        upstreams[index] = upstream
        rounded = upstream.astype(jnp.bfloat16)
        time_out_terms.append(token_sum(s["context_time"], rounded))
        back_context = back_dot(rounded, t_out).astype(jnp.bfloat16)
        back_placed = to_places(back_context)
        back_join = attend_back(s["join_time"], s["total_time"], back_placed, *temporal)
        time_in_terms.append(token_sum(s["placed"], back_join))
        back_twos_placed.append(back_dot(back_join, t_in).astype(jnp.bfloat16))
    time_grads = (summed(time_in_terms), summed(time_out_terms))
    time_kinds = ("plain", "plain")
    packed_time, back_twos_placed[-1] = lax.optimization_barrier(
        (pack_group(time_grads, time_kinds, members, half), back_twos_placed[-1])
    )
    grad_time = reduce_group(packed_time, time_grads, time_kinds, half)

    input_grads = []
    gain_one_terms = []
    back_ones = []
    space_out_terms = []
    space_in_terms = []
    for index in range(micro):
        s = saved[index]
        back_two = to_frames(back_twos_placed[index])
        back_mixed, gain_grad = norm_back(s["mixed_one"], gain_rows[1], back_two.astype(jnp.float32))
        gain_one_terms.append(gain_grad)
        upstream = upstreams[index] + back_mixed
        rounded = upstream.astype(jnp.bfloat16)
        space_out_terms.append(token_sum(s["context_space"], rounded))
        back_context = back_dot(rounded, s_out).astype(jnp.bfloat16)
        back_join = attend_back(s["join_space"], s["total_space"], back_context, *spatial)
        space_in_terms.append(token_sum(s["normed_one"], back_join))
        back_ones.append(back_dot(back_join, s_in).astype(jnp.bfloat16))
        input_grads.append(upstream)
    grad_space_in = summed(space_in_terms)
    grad_space_out = summed(space_out_terms)
    back_mixed, gain_grad_zero = norm_back(
        inputs[:, 0].astype(jnp.float32), gain_rows[0], jnp.stack(back_ones).astype(jnp.float32)
    )
    gain_grad_one = summed(gain_one_terms)
    gain_grad_two = summed(gain_two_terms)
    input_grad = jnp.stack(input_grads) + back_mixed

    gain_grads = jnp.stack((gain_grad_zero, gain_grad_one, gain_grad_two))
    space_grads = (grad_space_in, grad_space_out, gain_grads)
    space_kinds = ("plain", "plain", "gains")
    grad_space = reduce_group(
        pack_group(space_grads, space_kinds, members, half), space_grads, space_kinds, half
    )
    return (
        result[:, None],
        input_grad[:, None],
        grad_space[0],
        grad_space[1],
        grad_time[0],
        grad_time[1],
        grad_ffn[0],
        grad_ffn[1],
        grad_space[2],
    )


def solution(mesh):
    dp_size, fsdp_size = mesh.devices.shape
    split = Mesh(mesh.devices.reshape(dp_size // 2, 2, fsdp_size), ("dpo", "core", "fsdp"))
    tokens = P(None, ("dpo", "core"), "fsdp", None, None)
    rows = P("fsdp", None)
    return jax.shard_map(
        layer,
        mesh=split,
        in_specs=(tokens, rows, rows, rows, rows, rows, rows, P(None, "fsdp"), tokens),
        out_specs=(tokens, tokens, rows, rows, rows, rows, rows, rows, P(None, "fsdp")),
        check_vma=False,
    )
```

```python
import jax
import jax.numpy as jnp
from jax import lax
from jax.sharding import Mesh
from jax.sharding import PartitionSpec as P


D = 768
HEADS = 12
HEAD_DIM = 64
GAIN_COLS = 128

EPS = 1e-06

MEMBERS = ("fsdp", "core")


def layer_norm(values, scales):
    average = jnp.mean(values, axis=-1, keepdims=True)
    centred = values - average
    spread = jnp.mean(centred * centred, axis=-1, keepdims=True)
    return centred * lax.rsqrt(spread + EPS) * scales


def norm_back(values, scales, incoming):
    _, pullback = jax.vjp(layer_norm, values, scales)
    return pullback(incoming)


def flat_dot(left, right):
    flat = left.reshape(-1, left.shape[-1])
    product = jnp.dot(flat, right, preferred_element_type=jnp.float32)
    return product.reshape(left.shape[:-1] + (right.shape[1],))


def back_dot(left, right):
    flat = left.reshape(-1, left.shape[-1])
    product = lax.dot_general(
        flat, right, (((1,), (1,)), ((), ())), preferred_element_type=jnp.float32
    )
    return product.reshape(left.shape[:-1] + (right.shape[0],))


def token_sum(left, right):
    left_rows = left.reshape(-1, left.shape[-1])
    right_rows = right.reshape(-1, right.shape[-1])
    return lax.dot_general(
        left_rows, right_rows, (((0,), (0,)), ((), ())), preferred_element_type=jnp.float32
    )


def split_join(joined):
    split_heads = joined.reshape(joined.shape[:-1] + (3, HEADS, HEAD_DIM))
    return (split_heads[..., 0, :, :], split_heads[..., 1, :, :], split_heads[..., 2, :, :])


def attend_core(normed, weight_in, token_form, key_form, score_form):
    joined = flat_dot(normed, weight_in).astype(jnp.bfloat16)
    queries, keyset, valueset = split_join(joined)
    factor = HEAD_DIM ** (-0.5)
    scores = (
        jnp.einsum(
            token_form + "hd," + key_form + "hd->" + score_form,
            queries,
            keyset,
            preferred_element_type=jnp.float32,
        )
        * factor
    )
    totals = jax.nn.logsumexp(scores, axis=-1, keepdims=True)
    weighting = jnp.exp(scores - totals).astype(jnp.bfloat16)
    context = jnp.einsum(
        score_form + "," + key_form + "hd->" + token_form + "hd",
        weighting,
        valueset,
        preferred_element_type=jnp.float32,
    )
    context = context.reshape(normed.shape[:-1] + (D,)).astype(jnp.bfloat16)
    return (joined, totals, context)


def attend_back(joined, totals, back_context, token_form, key_form, score_form):
    queries, keyset, valueset = split_join(joined)
    back_heads = back_context.reshape(back_context.shape[:-1] + (HEADS, HEAD_DIM))
    factor = HEAD_DIM ** (-0.5)
    scores = (
        jnp.einsum(
            token_form + "hd," + key_form + "hd->" + score_form,
            queries,
            keyset,
            preferred_element_type=jnp.float32,
        )
        * factor
    )
    weighting = jnp.exp(scores - totals)
    back_weight = jnp.einsum(
        token_form + "hd," + key_form + "hd->" + score_form,
        back_heads,
        valueset,
        preferred_element_type=jnp.float32,
    )
    back_weight = back_weight.astype(jnp.bfloat16).astype(jnp.float32)
    inner_sum = jnp.sum(weighting * back_weight, axis=-1, keepdims=True)
    back_scores = (weighting * (back_weight - inner_sum)).astype(jnp.bfloat16)
    back_query = (
        jnp.einsum(
            score_form + "," + key_form + "hd->" + token_form + "hd",
            back_scores,
            keyset,
            preferred_element_type=jnp.float32,
        )
        * factor
    )
    back_keys = (
        jnp.einsum(
            score_form + "," + token_form + "hd->" + key_form + "hd",
            back_scores,
            queries,
            preferred_element_type=jnp.float32,
        )
        * factor
    )
    back_values = jnp.einsum(
        score_form + "," + token_form + "hd->" + key_form + "hd",
        weighting.astype(jnp.bfloat16),
        back_heads,
        preferred_element_type=jnp.float32,
    )
    stacked = jnp.stack((back_query, back_keys, back_values), axis=-3)
    return stacked.reshape(back_context.shape[:-1] + (3 * D,)).astype(jnp.bfloat16)


def gelu(values):
    return 0.5 * values * (1.0 + lax.erf(values * (0.5 ** 0.5)))


def to_places(frames_major):
    peers = lax.axis_size("fsdp")
    frames, places, width = frames_major.shape
    blocks = frames_major.reshape(frames, peers, places // peers, width).transpose(1, 0, 2, 3)
    blocks = lax.all_to_all(blocks, "fsdp", split_axis=0, concat_axis=0, tiled=True)
    return blocks.reshape(peers * frames, places // peers, width)


def to_frames(places_major):
    peers = lax.axis_size("fsdp")
    all_frames, places, width = places_major.shape
    blocks = places_major.reshape(peers, all_frames // peers, places, width)
    blocks = lax.all_to_all(blocks, "fsdp", split_axis=0, concat_axis=0, tiled=True)
    return blocks.transpose(1, 0, 2, 3).reshape(all_frames // peers, peers * places, width)


def to_member(array, kind, part, half):
    if kind == "gains":
        gain_part = lax.dynamic_slice_in_dim(array, part * half, half, axis=1).T
        return jnp.pad(gain_part, ((0, 0), (0, GAIN_COLS - gain_part.shape[1])))
    if kind == "grouped":
        rows = lax.dynamic_slice_in_dim(array, part * 4 * half, 4 * half, axis=0)
        return jnp.concatenate([rows[q * half:(q + 1) * half] for q in range(4)], axis=1)
    return lax.dynamic_slice_in_dim(array, part * half, half, axis=0)


def width_of(array, kind):
    return {"gains": GAIN_COLS, "grouped": 4 * D}.get(kind, array.shape[-1])


def from_members(block, kinds, widths, half):
    members = block.shape[0] // half
    outs = []
    offset = 0
    for kind, width in zip(kinds, widths):
        part = block[:, offset:offset + width]
        offset += width
        if kind == "gains":
            outs.append(part[:, :3].T)
        elif kind == "grouped":
            grouped = part.reshape(members, half, 4 * D)
            outs.append(
                jnp.concatenate([grouped[:, :, q * D:(q + 1) * D] for q in range(4)], axis=1).reshape(
                    members * 4 * half, D
                )
            )
        else:
            outs.append(part)
    return outs


def to_members_full(array, kind, members, half):
    array = array.astype(jnp.bfloat16)
    if kind == "gains":
        cols = array.T
        return jnp.pad(cols, ((0, 0), (0, GAIN_COLS - cols.shape[1])))
    if kind == "grouped":
        grouped = array.reshape(members, 4 * half, D)
        return jnp.concatenate(
            [grouped[:, q * half:(q + 1) * half, :] for q in range(4)], axis=2
        ).reshape(members * half, 4 * D)
    return array


def gather_group(arrays, kinds, part, half):
    block = jnp.concatenate([to_member(a, k, part, half) for a, k in zip(arrays, kinds)], axis=1)
    widths = [width_of(a, k) for a, k in zip(arrays, kinds)]
    gathered = lax.all_gather(block, MEMBERS, axis=0, tiled=True)
    return from_members(gathered, kinds, widths, half)


def pair_sum(values, axis):
    if lax.axis_size(axis) == 2:
        return values + lax.ppermute(values, axis, [(0, 1), (1, 0)])
    return lax.psum(values, axis)


def core_gather(values):
    if lax.axis_size("core") == 2:
        other = lax.ppermute(values, "core", [(0, 1), (1, 0)])
        first = lax.axis_index("core") == 0
        return jnp.concatenate(
            [jnp.where(first, values, other), jnp.where(first, other, values)], axis=0
        )
    return lax.all_gather(values, "core", axis=0, tiled=True)


def pack_group(grads, kinds, members, half):
    return jnp.concatenate(
        [to_members_full(g, k, members, half) for g, k in zip(grads, kinds)], axis=1
    )


def reduce_group(packed, grads, kinds, half):
    widths = [width_of(g, k) for g, k in zip(grads, kinds)]
    owned = lax.psum_scatter(packed, MEMBERS, scatter_dimension=0, tiled=True)
    owned = core_gather(pair_sum(owned, "dpo"))
    return [part.astype(jnp.float32) for part in from_members(owned, kinds, widths, half)]


def layer(
    inputs, space_in, space_out, time_in, time_out, hidden_in, hidden_out, norm_gains, cotangent
):
    fsdp_size = lax.axis_size("fsdp")
    core_size = lax.axis_size("core")
    members = fsdp_size * core_size
    half = space_in.shape[0] // core_size
    core = lax.axis_index("core")

    s_in, s_out, gains = gather_group(
        (space_in, space_out, norm_gains), ("plain", "plain", "gains"), core, half
    )
    t_in, t_out = gather_group((time_in, time_out), ("plain", "plain"), core, half)
    h_in, h_out = gather_group((hidden_in, hidden_out), ("plain", "grouped"), core, half)
    gain_rows = gains.astype(jnp.float32)

    micro = inputs.shape[0]
    spatial = ("gl", "gm", "ghlm")
    temporal = ("lg", "mg", "ghlm")

    saved = []
    mixed_twos = []
    for index in range(micro):
        frames_in = inputs[index, 0].astype(jnp.float32)
        normed_one = layer_norm(frames_in, gain_rows[0]).astype(jnp.bfloat16)
        join_space, total_space, context_space = attend_core(normed_one, s_in, *spatial)
        mixed_one = frames_in + flat_dot(context_space, s_out)
        normed_two = layer_norm(mixed_one, gain_rows[1]).astype(jnp.bfloat16)
        placed = to_places(normed_two)
        join_time, total_time, context_placed = attend_core(placed, t_in, *temporal)
        context_time = to_frames(context_placed)
        mixed_two = mixed_one + flat_dot(context_time, t_out)
        saved.append(
            dict(
                frames_in=frames_in,
                normed_one=normed_one,
                join_space=join_space,
                total_space=total_space,
                context_space=context_space,
                mixed_one=mixed_one,
                placed=placed,
                join_time=join_time,
                total_time=total_time,
                context_time=context_time,
            )
        )
        mixed_twos.append(mixed_two)

    mixed_two = jnp.stack(mixed_twos)
    normed_three = layer_norm(mixed_two, gain_rows[2]).astype(jnp.bfloat16)
    hidden = flat_dot(normed_three, h_in)
    activated = gelu(hidden).astype(jnp.bfloat16)
    result = mixed_two + flat_dot(activated, h_out)

    def pooled(pairs):
        lefts = [left.reshape(-1, left.shape[-1]) for left, _ in pairs]
        rights = [right.reshape(-1, right.shape[-1]) for _, right in pairs]
        return token_sum(jnp.concatenate(lefts, axis=0), jnp.concatenate(rights, axis=0))

    def summed(terms):
        total = terms[0]
        for term in terms[1:]:
            total = total + term
        return total

    gain_two_terms = []
    upstream_all = cotangent[:, 0].astype(jnp.float32)
    rounded = upstream_all.astype(jnp.bfloat16)
    grad_hidden_out = token_sum(activated, rounded)
    back_active = back_dot(rounded, h_out).astype(jnp.bfloat16)
    _, gelu_pull = jax.vjp(gelu, hidden)
    back_hidden = gelu_pull(back_active.astype(jnp.float32))[0].astype(jnp.bfloat16)
    grad_hidden_in = token_sum(normed_three, back_hidden)
    back_three_all = back_dot(back_hidden, h_in).astype(jnp.bfloat16)
    ffn_grads = (grad_hidden_in, grad_hidden_out)
    ffn_kinds = ("plain", "grouped")
    packed_ffn, t_in, t_out = lax.optimization_barrier(
        (pack_group(ffn_grads, ffn_kinds, members, half), t_in, t_out)
    )
    grad_ffn = reduce_group(packed_ffn, ffn_grads, ffn_kinds, half)
    back_threes = [back_three_all[index] for index in range(micro)]
    upstreams = [upstream_all[index] for index in range(micro)]

    back_twos_placed = []
    time_out_terms = []
    time_in_terms = []
    for index in range(micro):
        s = saved[index]
        back_mixed, gain_grad = norm_back(
            mixed_twos[index], gain_rows[2], back_threes[index].astype(jnp.float32)
        )
        gain_two_terms.append(gain_grad)
        upstream = upstreams[index] + back_mixed
        upstreams[index] = upstream
        rounded = upstream.astype(jnp.bfloat16)
        time_out_terms.append((s["context_time"], rounded))
        back_context = back_dot(rounded, t_out).astype(jnp.bfloat16)
        back_placed = to_places(back_context)
        back_join = attend_back(s["join_time"], s["total_time"], back_placed, *temporal)
        time_in_terms.append((s["placed"], back_join))
        back_twos_placed.append(back_dot(back_join, t_in).astype(jnp.bfloat16))
    time_grads = (pooled(time_in_terms), pooled(time_out_terms))
    time_kinds = ("plain", "plain")
    packed_time, back_twos_placed[-1] = lax.optimization_barrier(
        (pack_group(time_grads, time_kinds, members, half), back_twos_placed[-1])
    )
    grad_time = reduce_group(packed_time, time_grads, time_kinds, half)

    input_grads = []
    gain_one_terms = []
    gain_zero_terms = []
    space_out_terms = []
    space_in_terms = []
    for index in range(micro):
        s = saved[index]
        back_two = to_frames(back_twos_placed[index])
        back_mixed, gain_grad = norm_back(s["mixed_one"], gain_rows[1], back_two.astype(jnp.float32))
        gain_one_terms.append(gain_grad)
        upstream = upstreams[index] + back_mixed
        rounded = upstream.astype(jnp.bfloat16)
        space_out_terms.append(token_sum(s["context_space"], rounded))
        back_context = back_dot(rounded, s_out).astype(jnp.bfloat16)
        back_join = attend_back(s["join_space"], s["total_space"], back_context, *spatial)
        space_in_terms.append(token_sum(s["normed_one"], back_join))
        back_one = back_dot(back_join, s_in).astype(jnp.bfloat16)
        back_mixed, gain_grad = norm_back(
            s["frames_in"], gain_rows[0], back_one.astype(jnp.float32)
        )
        gain_zero_terms.append(gain_grad)
        input_grads.append(upstream + back_mixed)
    grad_space_in = summed(space_in_terms)
    grad_space_out = summed(space_out_terms)
    gain_grad_zero = summed(gain_zero_terms)
    gain_grad_one = summed(gain_one_terms)
    gain_grad_two = summed(gain_two_terms)
    input_grad = jnp.stack(input_grads)

    gain_grads = jnp.stack((gain_grad_zero, gain_grad_one, gain_grad_two))
    space_grads = (grad_space_in, grad_space_out, gain_grads)
    space_kinds = ("plain", "plain", "gains")
    grad_space = reduce_group(
        pack_group(space_grads, space_kinds, members, half), space_grads, space_kinds, half
    )
    return (
        result[:, None],
        input_grad[:, None],
        grad_space[0],
        grad_space[1],
        grad_time[0],
        grad_time[1],
        grad_ffn[0],
        grad_ffn[1],
        grad_space[2],
    )


def solution(mesh):
    dp_size, fsdp_size = mesh.devices.shape
    split = Mesh(mesh.devices.reshape(dp_size // 2, 2, fsdp_size), ("dpo", "core", "fsdp"))
    tokens = P(None, ("dpo", "core"), "fsdp", None, None)
    rows = P("fsdp", None)
    return jax.shard_map(
        layer,
        mesh=split,
        in_specs=(tokens, rows, rows, rows, rows, rows, rows, P(None, "fsdp"), tokens),
        out_specs=(tokens, tokens, rows, rows, rows, rows, rows, rows, P(None, "fsdp")),
        check_vma=False,
    )
```
